32 devices in a mesh: gx: 4 (over y, core), gy: 8 (over z, x).
Axes of the slice: x: 2, y: 2, z: 4, core: 2. Of those that a mesh axis runs over, the one named last changes fastest.
Arguments:
- previous: float32 [2, 7, 512, 1024], P(None, None, 'gx', 'gy'), may hold values from -6 to 6
- dissipated: float32 [2, 4, 512, 1024], P(None, None, 'gx', 'gy'), may hold values from 0.05 to 3
- material: int32 [4, 512, 1024], P(None, 'gx', 'gy'), may hold values from 0 to 3
- coolant: int32 [3, 512, 1024], P(None, 'gx', 'gy'), may hold values from 0 to 3
Outputs:
- temperature: float32 [2, 7, 512, 1024], P(None, None, 'gx', 'gy')
The draws below stay inside these ranges and needn't reach their ends.
All inputs are finite; a program needn't handle non-finite values.
Results may differ from the reference program's by a relative error of at most 0.00011.
Values sent between devices are 32-bit elements; how exact they have to be, the bound alone decides.
A program may use at most 64 MiB of HBM per device.

```python
import math
import jax
import jax.numpy as jnp
from jax import lax

TIERS = 4
CHANNELS = 3
LAYERS = 7
SCEN = 2
ITERS = 3
NX = 512
NY = 1024


def set_ends(entries, stream_key, low, largest):
    longest = entries.shape.index(max(entries.shape))
    spots = []
    for shift in (0, 1):
        where = [jax.random.randint(jax.random.fold_in(stream_key, axis), (), 0, length) for axis, length in enumerate(entries.shape)]
        where[longest] = (where[longest] + shift) % entries.shape[longest]
        spots.append(tuple(where))
    return entries.at[spots[0]].set(low).at[spots[1]].set(largest)


def block_scale(key, dims, split, low, largest):
    def one(position, shards_of):
        steps = jax.random.uniform(jax.random.fold_in(jax.random.fold_in(key, 6), position), (shards_of,), jnp.float32, low / len(split), largest / len(split))
        return jnp.repeat(jnp.exp(steps), dims[position] // shards_of).reshape((-1,) + (1,) * (len(dims) - position - 1))

    level = one(*split[0])
    for cut in split[1:]:
        level = level * one(*cut)
    return level


def bell_draw(key, shape, deviation, bound, cuts=(), dtype=jnp.bfloat16):
    result = jax.random.normal(key, shape, jnp.float32) * deviation
    if len(cuts) > 0:
        result = block_scale(key, shape, cuts, -0.22, 0.18) * result
    return jnp.clip(result, min=-bound, max=bound).astype(dtype)


def setup_inputs(seed: int = 0) -> dict:
    streams_of = jax.random.split(jax.random.key(seed), 5)
    previous = bell_draw(streams_of[0], (SCEN, LAYERS, NX, NY), 1.0, 6.0, ((2, 4), (3, 8)), jnp.float32)
    dissipated = jnp.clip(jnp.exp(math.log(3.0) - 4.0943445 * jax.random.uniform(streams_of[1], (SCEN, TIERS, NX, NY), jnp.float32) ** block_scale(streams_of[1], (SCEN, TIERS, NX, NY), ((2, 4), (3, 8)), -0.2, 0.2)), 0.05, 3.0)
    material = set_ends(jax.random.randint(streams_of[2], (TIERS, NX, NY), 0, 4), jax.random.fold_in(streams_of[2], 1), 0, 3).astype(jnp.int32)
    coolant = set_ends(jax.random.randint(streams_of[3], (CHANNELS, NX, NY), 0, 4), jax.random.fold_in(streams_of[3], 1), 0, 3).astype(jnp.int32)
    return dict(previous=previous, dissipated=dissipated, material=material, coolant=coolant)


TIER_K = (1.0, 0.3, 0.12, 2.5)
CHANNEL_K = (1.0, 0.3, 0.25, 0.2)
CHANNEL_SINK = (0.0, 0.15, 0.45, 1.2)
TIER_HEAT = 0.05
CHANNEL_HEAT = 0.2
VERTICAL = 4.0

def lookup(codes, table):
    total = jnp.zeros(codes.shape, jnp.float32)
    for index, value in enumerate(table):
        total = total + jnp.where(codes == index, jnp.float32(value), jnp.float32(0.0))
    return total

def mix(tiers, channels):
    rows = []
    for layer in range(2 * tiers.shape[0] - 1):
        rows.append(tiers[layer // 2] if layer % 2 == 0 else channels[layer // 2])
    return jnp.stack(rows)

def capacity_column(layers):
    return jnp.array([TIER_HEAT if layer % 2 == 0 else CHANNEL_HEAT for layer in range(layers)], jnp.float32)

def couplings(padded_k):
    centre = padded_k[:, 1:-1, 1:-1]
    g_north = jnp.sqrt(centre * padded_k[:, :-2, 1:-1])
    g_south = jnp.sqrt(centre * padded_k[:, 2:, 1:-1])
    g_west = jnp.sqrt(centre * padded_k[:, 1:-1, :-2])
    g_east = jnp.sqrt(centre * padded_k[:, 1:-1, 2:])
    g_vertical = VERTICAL * jnp.sqrt(centre[:-1] * centre[1:])
    return (g_north, g_south, g_west, g_east, g_vertical)

def operate(padded_v, padded_k, sink, capacity):
    g_north, g_south, g_west, g_east, g_vertical = couplings(padded_k)
    centre = padded_v[:, 1:-1, 1:-1]
    lateral = g_north * (centre - padded_v[:, :-2, 1:-1]) + g_south * (centre - padded_v[:, 2:, 1:-1])
    lateral = lateral + g_west * (centre - padded_v[:, 1:-1, :-2]) + g_east * (centre - padded_v[:, 1:-1, 2:])
    flux = g_vertical * (centre[:-1] - centre[1:])
    zero_row = jnp.zeros_like(centre[:1])
    vertical = jnp.concatenate([flux, zero_row], 0) - jnp.concatenate([zero_row, flux], 0)
    return (capacity + sink) * centre + lateral + vertical

def diagonal_terms(padded_k, sink, capacity):
    g_north, g_south, g_west, g_east, g_vertical = couplings(padded_k)
    zero_row = jnp.zeros_like(g_vertical[:1])
    vertical = jnp.concatenate([g_vertical, zero_row], 0) + jnp.concatenate([zero_row, g_vertical], 0)
    return capacity + sink + g_north + g_south + g_west + g_east + vertical

def padded(field):
    return jnp.pad(field, ((0, 0), (1, 1), (1, 1)))

def reference(previous, dissipated, material, coolant):
    tier_k = lookup(material, TIER_K)
    kappa = mix(tier_k, lookup(coolant, CHANNEL_K))
    sink = mix(jnp.zeros_like(tier_k), lookup(coolant, CHANNEL_SINK))
    capacity = capacity_column(kappa.shape[0])[:, None, None]
    padded_k = padded(kappa)
    diagonal = diagonal_terms(padded_k, sink, capacity)

    def solve_one(pair):
        start, heat = pair
        source = capacity * start + mix(heat, jnp.zeros_like(heat[:-1]))
        residual = source - operate(padded(start), padded_k, sink, capacity)
        solution = start
        scaled = residual / diagonal
        norm_now = jnp.sum(residual * scaled)
        direction = scaled
        for iteration in range(ITERS):
            image = operate(padded(direction), padded_k, sink, capacity)
            step_size = norm_now / jnp.sum(direction * image)
            solution = solution + step_size * direction
            residual = residual - step_size * image
            if iteration + 1 < ITERS:
                scaled = residual / diagonal
                norm_next = jnp.sum(residual * scaled)
                direction = scaled + norm_next / norm_now * direction
                norm_now = norm_next
        return solution
    return lax.map(solve_one, (previous, dissipated))
```

```python
import functools
import math

import jax
import jax.numpy as jnp
from jax import lax
from jax.experimental import pallas as pl
from jax.experimental.pallas import tpu as pltpu
from jax.sharding import PartitionSpec as P

ITERS = 3
TIER_K = (1.0, 0.3, 0.12, 2.5)
CHANNEL_K = (1.0, 0.3, 0.25, 0.2)
CHANNEL_SINK = (0.0, 0.15, 0.45, 1.2)
TIER_HEAT = 0.05
CHANNEL_HEAT = 0.2
VERTICAL = 4.0

HALO = 8
STRIP = 4
SLOT = 2 * STRIP
MESH = pl.DeviceIdType.MESH

TIER_ROOT = tuple(math.sqrt(v) for v in TIER_K)
CHANNEL_ROOT = tuple(math.sqrt(v) for v in CHANNEL_K)
TIER_INV = tuple(1.0 / math.sqrt(v) for v in TIER_K)
CHANNEL_INV = tuple(1.0 / math.sqrt(v) for v in CHANNEL_K)


def lookup(codes, table):
    total = jnp.zeros(codes.shape, jnp.float32)
    for index, value in enumerate(table):
        total = jnp.where(codes == index, jnp.float32(value), total)
    return total


def coefficients(nu):
    def inner(a, b):
        total = None
        for i, x in enumerate(a):
            for j, y in enumerate(b):
                term = x * y * nu[i + j]
                total = term if total is None else total + term
        return total

    zero = nu[0] * 0.0
    rho = [zero + 1.0]
    pi = [zero + 1.0]
    norm = nu[0]
    result = [zero] * ITERS
    for iteration in range(ITERS):
        image = [a - b for a, b in zip(pi + [zero], [zero] + pi)]
        step = norm / inner(pi, image)
        for i, a in enumerate(pi):
            result[i] = result[i] + step * a
        if iteration + 1 < ITERS:
            rho = [a - step * b for a, b in zip(rho + [zero], image)]
            following = inner(rho, rho)
            growth = following / norm
            pi = [a + growth * b for a, b in zip(rho, pi + [zero])]
            norm = following
    return result


def kernel(nx, ny, prev, diss, mat, cool, out, vp, vq, vm, vc, own_l, own_r, far_l, far_r,
           edges, root, weight, capac, up, u0, u1, u2, row, rows,
           picks, split, load_sem, send_sem, recv_sem, row_send, row_recv):
    scen, layers, length, width = prev.shape
    tiers = mat.shape[0]
    n = nx * ny
    ext = length + 2 * HALO
    x, y = lax.axis_index("gx"), lax.axis_index("gy")
    me = x * ny + y
    barrier = pltpu.get_barrier_semaphore()

    def other(i):
        k = lax.rem(me + i, n)
        return k // ny, lax.rem(k, ny)

    def greet(i, carry):
        pl.semaphore_signal(barrier, inc=1, device_id=other(i), device_id_type=MESH)
        return carry

    inside = pl.ds(HALO, length)
    loads = [
        pltpu.make_async_copy(prev, vp.at[:, :, inside], load_sem.at[0]),
        pltpu.make_async_copy(diss, vq.at[:, :, inside], load_sem.at[1]),
        pltpu.make_async_copy(mat, vm.at[:, inside], load_sem.at[2]),
        pltpu.make_async_copy(cool, vc.at[:, inside], load_sem.at[3]),
    ]
    for copy in loads:
        copy.start()
    lax.fori_loop(1, n, greet, 0)

    has = {(-1, 0): x > 0, (1, 0): x < nx - 1, (0, -1): y > 0, (0, 1): y < ny - 1}
    for dx in (-1, 1):
        for dy in (-1, 1):
            has[dx, dy] = jnp.logical_and(has[dx, 0], has[0, dy])
    top, bottom = pl.ds(0, HALO), pl.ds(HALO + length, HALO)
    first, last = pl.ds(HALO, HALO), pl.ds(length, HALO)

    def fill(ref):
        ref[...] = jnp.full(ref.shape, -1, ref.dtype)

    for dx, where in ((-1, top), (1, bottom)):
        @pl.when(jnp.logical_not(has[dx, 0]))
        def _(where=where):
            for ref in (vp, vq):
                fill(ref.at[:, :, where])
            for ref in (vm, vc):
                fill(ref.at[:, where])
            fill(own_l.at[where])
            fill(own_r.at[where])
    for dy, ref in ((-1, far_l), (1, far_r)):
        @pl.when(jnp.logical_not(has[0, dy]))
        def _(ref=ref):
            fill(ref.at[inside])
        for dx, where in ((-1, top), (1, bottom)):
            @pl.when(jnp.logical_not(has[dx, dy]))
            def _(ref=ref, where=where):
                fill(ref.at[where])

    for copy in loads:
        copy.wait()

    places = []
    for s in range(scen):
        for layer in range(layers):
            places.append((SLOT * (s * layers + layer), vp, (s, layer)))
    for layer in range(layers):
        ref = vm if layer % 2 == 0 else vc
        places.append((SLOT * layer + STRIP, ref, (layer // 2,)))
    for t in range(tiers):
        places.append((SLOT * (layers + 1 + 2 * t) + STRIP, vq, (0, t)))
        places.append((SLOT * (layers + 2 * t) + STRIP, vq, (1, t)))
    chunk = 4 * HALO

    def pack(step, carry):
        start = pl.multiple_of(HALO + step * chunk, HALO)
        lane = lax.broadcasted_iota(jnp.int32, (chunk, width), 1)
        left = jnp.zeros((chunk, width), jnp.float32)
        right = jnp.zeros((chunk, width), jnp.float32)
        for base, ref, index in places:
            plane = ref[index + (pl.ds(start, chunk),)].astype(jnp.float32)
            turned = pltpu.roll(plane, base, 1) if base else plane
            left = jnp.where((lane >= base) & (lane < base + STRIP), turned, left)
            low = (base - STRIP) % width
            right = jnp.where((lane >= low) & (lane < low + STRIP), turned, right)
        own_l[pl.ds(start, chunk)] = left
        own_r[pl.ds(start, chunk)] = pltpu.roll(right, STRIP, 1)
        return carry

    lax.fori_loop(0, length // chunk, pack, 0)

    def pick(slot, carry):
        near = (2 * width, width)
        source = lax.broadcasted_iota(jnp.int32, near, 0) % width - SLOT * slot
        target = lax.broadcasted_iota(jnp.int32, near, 1)
        west = (source == STRIP - 1) & (target == 0)
        east = (source == STRIP - 2) & (target == width - 1)
        picks[slot] = jnp.where(west | east, 1.0, 0.0).astype(jnp.bfloat16)
        return carry

    lax.fori_loop(0, scen * layers, pick, 0)

    pl.semaphore_wait(barrier, n - 1)

    sends = []
    for dx, source, target in ((-1, first, bottom), (1, last, top)):
        for ref in (vp, vq):
            sends.append((dx, 0, ref.at[:, :, source], ref.at[:, :, target]))
        for ref in (vm, vc):
            sends.append((dx, 0, ref.at[:, source], ref.at[:, target]))
        for ref in (own_l, own_r):
            sends.append((dx, 0, ref.at[source], ref.at[target]))
        sends.append((dx, -1, own_l.at[source], far_r.at[target]))
        sends.append((dx, 1, own_r.at[source], far_l.at[target]))
    sends.append((0, -1, own_l.at[inside], far_r.at[inside]))
    sends.append((0, 1, own_r.at[inside], far_l.at[inside]))
    copies = []
    for i, (dx, dy, source, target) in enumerate(sends):
        copy = pltpu.make_async_remote_copy(
            src_ref=source, dst_ref=target, send_sem=send_sem.at[i], recv_sem=recv_sem.at[i],
            device_id=(x + dx, y + dy), device_id_type=MESH)
        copies.append((dx, dy, copy))
    order = sorted(copies, key=lambda c: 0 if c[0] == 0 else 1 if c[1] == 0 else 2)
    for dx, dy, copy in order:
        @pl.when(has[dx, dy])
        def _(copy=copy):
            copy.start()
    blank = jnp.zeros((ext + 2 * HALO, width), jnp.float32)
    for pad in (0, layers + 1):
        root[pad] = blank
        for s in range(scen):
            for ref in (up, u0, u1, u2):
                ref[s, pad] = blank

    def prepare(begin, count):
        at, to = pl.ds(begin, count), pl.ds(begin + HALO, count)
        for layer in range(layers):
            if layer % 2 == 0:
                s = lookup(vm[layer // 2, at], TIER_ROOT)
                total = jnp.full((count, width), TIER_HEAT, jnp.float32)
            else:
                codes = vc[layer // 2, at]
                s = lookup(codes, CHANNEL_ROOT)
                total = CHANNEL_HEAT + lookup(codes, CHANNEL_SINK)
            root[layer + 1, to] = s
            capac[layer, at] = total
            for k in range(scen):
                up[k, layer + 1, to] = s * vp[k, layer, at]

    prepare(HALO, length)
    body = pl.ds(HALO, ext)

    def stencil(ref, at, layer, edge, slot, start=0, count=ext):
        lane = lax.broadcasted_iota(jnp.int32, (count, width), 1)
        rows_at = pl.ds(HALO + start, count)
        centre = ref[at + (layer + 1, rows_at)]
        west = jnp.where(lane == 0, 0.0, pltpu.roll(centre, 1, 1))
        east = jnp.where(lane == width - 1, 0.0, pltpu.roll(centre, width - 1, 1))
        lateral = west + east + ref[at + (layer + 1, pl.ds(HALO + start - 1, count))]
        lateral = lateral + ref[at + (layer + 1, pl.ds(HALO + start + 1, count))]
        vertical = ref[at + (layer, rows_at)] + ref[at + (layer + 2, rows_at)]
        around = lateral + VERTICAL * vertical
        if edge is not None:
            around = around + border(edge, slot, start, count)
        return centre, around

    def border(edge, slot, start, count):
        return jnp.dot(split[edge, pl.ds(start, count)], picks[slot],
                       preferred_element_type=jnp.float32)

    inner, rest = 2 * HALO, length - 2 * HALO

    def early(layer, carry):
        at = pl.ds(inner, rest)
        weight[layer, at] = stencil(root, (), layer, None, 0, inner, rest)[1]
        for k in range(scen):
            u1[k, layer + 1, at] = stencil(up, (k,), layer, None, 0, inner, rest)[1]
        return carry

    lax.fori_loop(0, layers, early, 0)

    for dx, dy, copy in copies:
        @pl.when(has[-dx, -dy])
        def _(copy=copy):
            copy.wait_recv()

    prepare(0, HALO)
    prepare(HALO + length, HALO)

    shape = (ext, width)
    lane = lax.broadcasted_iota(jnp.int32, shape, 1)
    place = lane // SLOT
    low = lane % SLOT < STRIP
    layer_of = place % layers
    tier = layer_of % 2 == 0
    used = place < scen * layers

    def strip_stencil(u):
        lateral = pltpu.roll(u, 1, 1) + pltpu.roll(u, width - 1, 1)
        lateral = lateral + pltpu.roll(u, 1, 0) + pltpu.roll(u, ext - 1, 0)
        above = jnp.where(layer_of > 0, pltpu.roll(u, SLOT, 1), 0.0)
        below = jnp.where(layer_of < layers - 1, pltpu.roll(u, width - SLOT, 1), 0.0)
        return lateral + VERTICAL * (above + below)

    def strip(field, rest):
        codes = jnp.where(place < layers, rest, pltpu.roll(rest, SLOT * layers, 1))
        codes = jnp.where(used, codes, -1.0)
        power = jnp.where(place < layers, pltpu.roll(rest, width - SLOT * (layers + 1), 1), rest)
        power = jnp.where(tier & used, power, 0.0)
        s = jnp.where(tier, lookup(codes, TIER_ROOT), lookup(codes, CHANNEL_ROOT))
        heat = jnp.where(tier, TIER_HEAT, CHANNEL_HEAT)
        total = heat + jnp.where(tier, 0.0, lookup(codes, CHANNEL_SINK))
        total = total + s * strip_stencil(s)
        inverse = 1.0 / total
        scaled = s * field
        residual = (heat - total) * field + power + s * strip_stencil(scaled)
        w = s * s * inverse
        a = s * residual * inverse
        b = w * strip_stencil(a)
        c = w * strip_stencil(b)
        return s, scaled, a, b, c

    here, there = own_l[...], far_l[...]
    lefts = strip(jnp.where(low, there, pltpu.roll(here, STRIP, 1)),
                  jnp.where(low, pltpu.roll(there, width - STRIP, 1), here))
    for i, value in enumerate(lefts):
        edges[i] = value
    here, there = own_r[...], far_r[...]
    rights = strip(jnp.where(low, here, pltpu.roll(there, STRIP, 1)),
                   jnp.where(low, pltpu.roll(here, width - STRIP, 1), there))
    for i, value in enumerate(rights):
        both = jnp.where(lane % SLOT == STRIP - 1, edges[i], pltpu.roll(value, width - 2, 1))
        high = both.astype(jnp.bfloat16)
        split[i, :, :width] = high
        split[i, :, width:] = (both - high.astype(jnp.float32)).astype(jnp.bfloat16)

    body = pl.ds(HALO, ext)

    def gather(total, value):
        tiles = value[HALO:HALO + length].reshape(length // HALO, HALO, width)
        return total + jnp.sum(tiles, axis=0)

    none = jnp.zeros((HALO, width), jnp.float32)

    def begin(layer, carry):
        is_tier = lax.rem(layer, 2) == 0
        heat = jnp.where(is_tier, jnp.float32(TIER_HEAT), jnp.float32(CHANNEL_HEAT))
        on = jnp.where(is_tier, jnp.float32(1.0), jnp.float32(0.0))
        sums = list(carry)
        for start, count in ((0, inner), (inner, rest), (inner + rest, inner)):
            at = pl.ds(start, count)
            if start == inner:
                s = root[layer + 1, pl.ds(HALO + start, count)]
                around = weight[layer, at] + border(0, layer, start, count)
            else:
                s, around = stencil(root, (), layer, 0, layer, start, count)
            total = capac[layer, at] + s * around
            inverse = 1.0 / total
            weight[layer, at] = s * s * inverse
            for k in range(scen):
                slot = k * layers + layer
                if start == inner:
                    around = u1[k, layer + 1, at] + border(1, slot, start, count)
                else:
                    _, around = stencil(up, (k,), layer, 1, slot, start, count)
                residual = (heat - total) * vp[k, layer, at] + on * vq[k, layer // 2, at]
                residual = residual + s * around
                scaled = residual * inverse
                u0[k, layer + 1, pl.ds(HALO + start, count)] = s * scaled
                own = residual * scaled
                own = own[HALO:] if start == 0 else own[:HALO] if start > inner else own
                sums[k] = sums[k] + jnp.sum(own.reshape(-1, HALO, width), axis=0)
        return tuple(sums)

    def advance(source, target, edge):
        def one(layer, carry):
            sums = []
            for k in range(scen):
                centre, around = stencil(source, (k,), layer, edge, k * layers + layer)
                sums.append(gather(carry[len(sums)], centre * around))
                if target is not None:
                    moved = weight[layer] * around
                    target[k, layer + 1, body] = moved
                    sums.append(gather(carry[len(sums)], moved * around))
            return tuple(sums)

        count = scen * (1 if target is None else 2)
        return lax.fori_loop(0, layers, one, (none,) * count, unroll=True)

    first_sums = lax.fori_loop(0, layers, begin, (none,) * scen, unroll=True)
    second = advance(u0, u1, 2)
    third = advance(u1, u2, 3)
    fourth = advance(u2, None, 4)
    moments = []
    for k in range(scen):
        moments += [first_sums[k], *second[2 * k:2 * k + 2], *third[2 * k:2 * k + 2], fourth[k]]
    count = len(moments)
    flat = jnp.zeros((1, width), jnp.float32)
    line = lax.broadcasted_iota(jnp.int32, (1, width), 1)
    for i, value in enumerate(moments):
        total = jnp.sum(jnp.sum(value, axis=0, keepdims=True), axis=1, keepdims=True)
        flat = jnp.where(line == i, total, flat)
    row[...] = flat
    rows[n - 1] = flat

    def to(i):
        return pltpu.make_async_remote_copy(
            src_ref=row, dst_ref=rows.at[i - 1], send_sem=row_send, recv_sem=row_recv,
            device_id=other(i), device_id_type=MESH)

    def spread(i, carry):
        to(i).start()
        return carry

    lax.fori_loop(1, n, spread, 0)
    for dx, dy, copy in copies:
        @pl.when(has[dx, dy])
        def _(copy=copy):
            copy.wait_send()
    own = pl.ds(2 * HALO, length)
    for layer in range(layers):
        if layer % 2 == 0:
            back = lookup(vm[layer // 2, inside], TIER_INV)
        else:
            back = lookup(vc[layer // 2, inside], CHANNEL_INV)
        for k in range(scen):
            for ref in (u0, u1, u2):
                ref[k, layer + 1, own] = back * ref[k, layer + 1, own]
    arrived = rows.at[pl.ds(0, n - 1)]
    pltpu.make_async_copy(arrived, arrived, row_recv).wait()
    summed = jnp.sum(rows[...], axis=0)
    total = [jnp.sum(jnp.where(line == i, summed, 0.0), axis=1, keepdims=True)
             for i in range(count)]
    each = count // scen
    for k in range(scen):
        c0, c1, c2 = coefficients(total[k * each:(k + 1) * each])
        for layer in range(layers):
            change = c0 * u0[k, layer + 1, own] + c1 * u1[k, layer + 1, own]
            change = change + c2 * u2[k, layer + 1, own]
            out[k, layer] = vp[k, layer, inside] + change
    pltpu.make_async_copy(arrived, arrived, row_send).wait()


def per_device(nx, ny, previous, dissipated, material, coolant):
    scen, layers, length, width = previous.shape
    tiers = material.shape[0]
    ext = length + 2 * HALO
    f32 = jnp.float32
    field = pltpu.VMEM((scen, layers + 2, ext + 2 * HALO, width), f32)
    strip = pltpu.VMEM((ext, width), f32)
    return pl.pallas_call(
        functools.partial(kernel, nx, ny),
        out_shape=pltpu.VMEM(previous.shape, f32),
        in_specs=[pl.BlockSpec(memory_space=pl.ANY)] * 4,
        out_specs=pl.BlockSpec(memory_space=pltpu.VMEM),
        scratch_shapes=[
            pltpu.VMEM((scen, layers, ext, width), f32),
            pltpu.VMEM((scen, tiers, ext, width), f32),
            pltpu.VMEM((tiers, ext, width), jnp.int32),
            pltpu.VMEM((layers - tiers, ext, width), jnp.int32),
            strip, strip, strip, strip,
            pltpu.VMEM((5, ext, width), f32),
            pltpu.VMEM((layers + 2, ext + 2 * HALO, width), f32),
            pltpu.VMEM((layers, ext, width), f32),
            pltpu.VMEM((layers, ext, width), f32),
            field, field, field, field,
            pltpu.VMEM((1, width), f32),
            pltpu.VMEM((nx * ny, 1, width), f32),
            pltpu.VMEM((scen * layers, 2 * width, width), jnp.bfloat16),
            pltpu.VMEM((5, ext, 2 * width), jnp.bfloat16),
            pltpu.SemaphoreType.DMA((4,)),
            pltpu.SemaphoreType.DMA((18,)),
            pltpu.SemaphoreType.DMA((18,)),
            pltpu.SemaphoreType.DMA,
            pltpu.SemaphoreType.DMA,
        ],
        compiler_params=pltpu.CompilerParams(
            collective_id=0, has_side_effects=True, vmem_limit_bytes=60 * 1024 * 1024),
    )(previous, dissipated, material, coolant)


def solution(mesh):
    return jax.shard_map(
        functools.partial(per_device, mesh.shape["gx"], mesh.shape["gy"]),
        mesh=mesh,
        in_specs=(
            P(None, None, "gx", "gy"),
            P(None, None, "gx", "gy"),
            P(None, "gx", "gy"),
            P(None, "gx", "gy"),
        ),
        out_specs=P(None, None, "gx", "gy"),
        check_vma=False,
    )
```

```python
import functools
import math

import jax
import jax.numpy as jnp
from jax import lax
from jax.experimental import pallas as pl
from jax.experimental.pallas import tpu as pltpu
from jax.sharding import PartitionSpec as P

ITERS = 3
TIER_K = (1.0, 0.3, 0.12, 2.5)
CHANNEL_K = (1.0, 0.3, 0.25, 0.2)
CHANNEL_SINK = (0.0, 0.15, 0.45, 1.2)
TIER_HEAT = 0.05
CHANNEL_HEAT = 0.2
VERTICAL = 4.0

HALO = 8
STRIP = 4
SLOT = 2 * STRIP
MESH = pl.DeviceIdType.MESH

TIER_ROOT = tuple(math.sqrt(v) for v in TIER_K)
CHANNEL_ROOT = tuple(math.sqrt(v) for v in CHANNEL_K)
TIER_INV = tuple(1.0 / math.sqrt(v) for v in TIER_K)
CHANNEL_INV = tuple(1.0 / math.sqrt(v) for v in CHANNEL_K)


def lookup(codes, table):
    total = jnp.zeros(codes.shape, jnp.float32)
    for index, value in enumerate(table):
        total = jnp.where(codes == index, jnp.float32(value), total)
    return total


def coefficients(nu):
    def inner(a, b):
        total = None
        for i, x in enumerate(a):
            for j, y in enumerate(b):
                term = x * y * nu[i + j]
                total = term if total is None else total + term
        return total

    zero = nu[0] * 0.0
    rho = [zero + 1.0]
    pi = [zero + 1.0]
    norm = nu[0]
    result = [zero] * ITERS
    for iteration in range(ITERS):
        image = [a - b for a, b in zip(pi + [zero], [zero] + pi)]
        step = norm / inner(pi, image)
        for i, a in enumerate(pi):
            result[i] = result[i] + step * a
        if iteration + 1 < ITERS:
            rho = [a - step * b for a, b in zip(rho + [zero], image)]
            following = inner(rho, rho)
            growth = following / norm
            pi = [a + growth * b for a, b in zip(rho, pi + [zero])]
            norm = following
    return result


def kernel(nx, ny, prev, diss, mat, cool, out, vp, vq, vm, vc, own_l, own_r, far_l, far_r,
           edges, root, weight, capac, up, u0, u1, u2, row, rows,
           along, across, known, load_sem, send_sem, recv_sem, row_send, row_recv):
    scen, layers, length, width = prev.shape
    tiers = mat.shape[0]
    n = nx * ny
    ext = length + 2 * HALO
    x, y = lax.axis_index("gx"), lax.axis_index("gy")
    me = x * ny + y
    barrier = pltpu.get_barrier_semaphore()

    def around_me(reach):
        found = []
        for dx in (-reach, 0, reach):
            for dy in (-reach, 0, reach):
                if (dx or dy) and abs(dx) < nx and abs(dy) < ny:
                    inside_x = jnp.logical_and(x + dx >= 0, x + dx < nx)
                    inside_y = jnp.logical_and(y + dy >= 0, y + dy < ny)
                    found.append((dx, dy, jnp.logical_and(inside_x, inside_y)))
        return found

    def greet(sem, reach):
        for dx, dy, there in around_me(reach):
            @pl.when(there)
            def _(dx=dx, dy=dy):
                pl.semaphore_signal(sem, inc=1, device_id=(x + dx, y + dy), device_id_type=MESH)

    def hear(sem, reach):
        pl.semaphore_wait(sem, sum(there.astype(jnp.int32) for _, _, there in around_me(reach)))

    reaches = [1]
    while 2 * reaches[-1] < max(nx, ny) - 1:
        reaches.append(2 * reaches[-1])
    heard = []

    def know():
        if len(heard) < len(reaches):
            hear(known.at[len(heard)], reaches[len(heard)])
            heard.append(True)
            if len(heard) < len(reaches):
                greet(known.at[len(heard)], reaches[len(heard)])

    inside = pl.ds(HALO, length)
    loads = [
        pltpu.make_async_copy(prev, vp.at[:, :, inside], load_sem.at[0]),
        pltpu.make_async_copy(diss, vq.at[:, :, inside], load_sem.at[1]),
        pltpu.make_async_copy(mat, vm.at[:, inside], load_sem.at[2]),
        pltpu.make_async_copy(cool, vc.at[:, inside], load_sem.at[3]),
    ]
    for copy in reversed(loads):
        copy.start()
    greet(barrier, 1)

    has = {(-1, 0): x > 0, (1, 0): x < nx - 1, (0, -1): y > 0, (0, 1): y < ny - 1}
    for dx in (-1, 1):
        for dy in (-1, 1):
            has[dx, dy] = jnp.logical_and(has[dx, 0], has[0, dy])
    top, bottom = pl.ds(0, HALO), pl.ds(HALO + length, HALO)
    first, last = pl.ds(HALO, HALO), pl.ds(length, HALO)

    def fill(ref):
        ref[...] = jnp.full(ref.shape, -1, ref.dtype)

    for dx, where in ((-1, top), (1, bottom)):
        @pl.when(jnp.logical_not(has[dx, 0]))
        def _(where=where):
            for ref in (vp, vq):
                fill(ref.at[:, :, where])
            for ref in (vm, vc):
                fill(ref.at[:, where])
            fill(own_l.at[where])
            fill(own_r.at[where])
    for dy, ref in ((-1, far_l), (1, far_r)):
        @pl.when(jnp.logical_not(has[0, dy]))
        def _(ref=ref):
            fill(ref.at[inside])
        for dx, where in ((-1, top), (1, bottom)):
            @pl.when(jnp.logical_not(has[dx, dy]))
            def _(ref=ref, where=where):
                fill(ref.at[where])

    first_places, later_places = [], []
    for layer in range(layers):
        ref = vm if layer % 2 == 0 else vc
        first_places.append((SLOT * layer, ref, (layer // 2,)))
    for t in range(tiers):
        first_places.append((SLOT * (layers + 1 + 2 * t), vq, (0, t)))
        first_places.append((SLOT * (layers + 2 * t), vq, (1, t)))
    for s in range(scen):
        for layer in range(layers):
            later_places.append((SLOT * (s * layers + layer), vp, (s, layer)))

    def pack(places):
        lane = lax.broadcasted_iota(jnp.int32, (length, width), 1)
        left = right = opening = None
        for base, ref, index in sorted(places, key=lambda place: place[0]):
            plane = ref[index + (inside,)].astype(jnp.float32)
            if base == 0:
                left = right = opening = plane
            else:
                turned = pltpu.roll(plane, base, 1)
                left = jnp.where(lane >= base, turned, left)
                right = jnp.where(lane >= base - STRIP, turned, right)
        return left, jnp.where(lane >= width - STRIP, opening, right)

    for copy in loads[1:]:
        copy.wait()
    own_l[inside], own_r[inside] = pack(first_places)
    loads[0].wait()
    left, right = pack(later_places)
    low = lax.broadcasted_iota(jnp.int32, (length, width), 1) % SLOT < STRIP
    own_l[inside] = jnp.where(low, left, pltpu.roll(own_l[inside], STRIP, 1))
    low = (lax.broadcasted_iota(jnp.int32, (length, width), 1) + STRIP) % SLOT < STRIP
    own_r[inside] = pltpu.roll(jnp.where(low, right, pltpu.roll(own_r[inside], STRIP, 1)), STRIP, 1)

    hear(barrier, 1)
    greet(known.at[0], 1)

    sends = []
    for dx, source, target in ((-1, first, bottom), (1, last, top)):
        for ref in (vp, vq):
            sends.append((dx, 0, ref.at[:, :, source], ref.at[:, :, target]))
        for ref in (vm, vc):
            sends.append((dx, 0, ref.at[:, source], ref.at[:, target]))
        for ref in (own_l, own_r):
            sends.append((dx, 0, ref.at[source], ref.at[target]))
        sends.append((dx, -1, own_l.at[source], far_r.at[target]))
        sends.append((dx, 1, own_r.at[source], far_l.at[target]))
    sends.append((0, -1, own_l.at[inside], far_r.at[inside]))
    sends.append((0, 1, own_r.at[inside], far_l.at[inside]))
    copies = []
    for i, (dx, dy, source, target) in enumerate(sends):
        copy = pltpu.make_async_remote_copy(
            src_ref=source, dst_ref=target, send_sem=send_sem.at[i], recv_sem=recv_sem.at[i],
            device_id=(x + dx, y + dy), device_id_type=MESH)
        copies.append((dx, dy, copy))
    order = sorted(copies, key=lambda c: 0 if c[0] == 0 else 1 if c[1] == 0 else 2)
    for dx, dy, copy in order:
        @pl.when(has[dx, dy])
        def _(copy=copy):
            copy.start()
    for i in range(2):
        source = lax.broadcasted_iota(jnp.int32, (width, width), 0)
        target = lax.broadcasted_iota(jnp.int32, (width, width), 1)
        apart = target - source
        beside = (apart == 1) | (apart == -1)
        along[pl.ds(i * width, width)] = jnp.where(beside, 1.0, 0.0).astype(jnp.bfloat16)
        spot = target // SLOT
        level = spot % layers
        used = spot < scen * layers
        beside = beside & (source // SLOT == spot) & used
        stacked = (apart == SLOT) & (level > 0) | (apart == -SLOT) & (level < layers - 1)
        weights = jnp.where(stacked & used, VERTICAL, jnp.where(beside, 1.0, 0.0))
        across[pl.ds(i * width, width)] = weights.astype(jnp.bfloat16)
    blank = jnp.zeros((ext + 2 * HALO, width), jnp.float32)
    for pad in (0, layers + 1):
        root[pad] = blank
        for s in range(scen):
            for ref in (up, u0, u1, u2):
                ref[s, pad] = blank

    def prepare(begin, count):
        at, to = pl.ds(begin, count), pl.ds(begin + HALO, count)
        for layer in range(layers):
            if layer % 2 == 0:
                s = lookup(vm[layer // 2, at], TIER_ROOT)
                total = jnp.full((count, width), TIER_HEAT, jnp.float32)
            else:
                codes = vc[layer // 2, at]
                s = lookup(codes, CHANNEL_ROOT)
                total = CHANNEL_HEAT + lookup(codes, CHANNEL_SINK)
            root[layer + 1, to] = s
            capac[layer, at] = total
            for k in range(scen):
                up[k, layer + 1, to] = s * vp[k, layer, at]

    prepare(HALO, length)
    know()
    body = pl.ds(HALO, ext)

    def shifted(value, matrix):
        high = value.astype(jnp.bfloat16)
        low = (value - high.astype(jnp.float32)).astype(jnp.bfloat16)
        return jnp.dot(jnp.concatenate([high, low], axis=1), matrix[...],
                       preferred_element_type=jnp.float32)

    def stencil(ref, at, layer, edge, slot, start=0, count=ext):
        rows_at = pl.ds(HALO + start, count)
        centre = ref[at + (layer + 1, rows_at)]
        lateral = shifted(centre, along) + ref[at + (layer + 1, pl.ds(HALO + start - 1, count))]
        lateral = lateral + ref[at + (layer + 1, pl.ds(HALO + start + 1, count))]
        vertical = ref[at + (layer, rows_at)] + ref[at + (layer + 2, rows_at)]
        around = lateral + VERTICAL * vertical
        if edge is not None:
            around = around + margins(edge, slot, start, count)
        return centre, around

    def border(edge, slot, start, count):
        shift = (width - SLOT * slot - (STRIP - 1)) % width
        return pltpu.roll(edges[edge, pl.ds(start, count)], shift, 1)

    def margins(edge, slot, start, count):
        lane = lax.broadcasted_iota(jnp.int32, (count, width), 1)
        ends = (lane == 0) | (lane == width - 1)
        return jnp.where(ends, border(edge, slot, start, count), 0.0)

    inner, rest = 2 * HALO, length - 2 * HALO

    def early(layer, carry):
        at = pl.ds(inner, rest)
        weight[layer, at] = stencil(root, (), layer, None, 0, inner, rest)[1]
        for k in range(scen):
            u1[k, layer + 1, at] = stencil(up, (k,), layer, None, 0, inner, rest)[1]
        return carry

    lax.fori_loop(0, layers, early, 0)
    know()

    for dx, dy, copy in copies:
        @pl.when(has[-dx, -dy])
        def _(copy=copy):
            copy.wait_recv()

    prepare(0, HALO)
    prepare(HALO + length, HALO)

    shape = (ext, width)
    lane = lax.broadcasted_iota(jnp.int32, shape, 1)
    place = lane // SLOT
    low = lane % SLOT < STRIP
    layer_of = place % layers
    tier = layer_of % 2 == 0
    used = place < scen * layers

    def strip_stencil(u):
        return shifted(u, across) + pltpu.roll(u, 1, 0) + pltpu.roll(u, ext - 1, 0)

    def strip(field, rest):
        codes = jnp.where(place < layers, rest, pltpu.roll(rest, SLOT * layers, 1))
        codes = jnp.where(used, codes, -1.0)
        power = jnp.where(place < layers, pltpu.roll(rest, width - SLOT * (layers + 1), 1), rest)
        power = jnp.where(tier & used, power, 0.0)
        s = jnp.where(tier, lookup(codes, TIER_ROOT), lookup(codes, CHANNEL_ROOT))
        heat = jnp.where(tier, TIER_HEAT, CHANNEL_HEAT)
        total = heat + jnp.where(tier, 0.0, lookup(codes, CHANNEL_SINK))
        total = total + s * strip_stencil(s)
        inverse = 1.0 / total
        scaled = s * field
        residual = (heat - total) * field + power + s * strip_stencil(scaled)
        w = s * s * inverse
        a = s * residual * inverse
        b = w * strip_stencil(a)
        c = w * strip_stencil(b)
        return s, scaled, a, b, c

    here, there = own_l[...], far_l[...]
    lefts = strip(jnp.where(low, there, pltpu.roll(here, STRIP, 1)),
                  jnp.where(low, pltpu.roll(there, width - STRIP, 1), here))
    for i, value in enumerate(lefts):
        edges[i] = value
    here, there = own_r[...], far_r[...]
    rights = strip(jnp.where(low, here, pltpu.roll(there, STRIP, 1)),
                   jnp.where(low, pltpu.roll(here, width - STRIP, 1), there))
    for i, value in enumerate(rights):
        edges[i] = jnp.where(lane % SLOT == STRIP - 1, edges[i], pltpu.roll(value, width - 2, 1))

    body = pl.ds(HALO, ext)

    def gather(total, value):
        tiles = value[HALO:HALO + length].reshape(length // HALO, HALO, width)
        return total + jnp.sum(tiles, axis=0)

    none = jnp.zeros((HALO, width), jnp.float32)

    def begin(layer, carry):
        heat = TIER_HEAT if layer % 2 == 0 else CHANNEL_HEAT
        sums = list(carry)
        for start, count in ((0, inner), (inner, rest), (inner + rest, inner)):
            at = pl.ds(start, count)
            if start == inner:
                s = root[layer + 1, pl.ds(HALO + start, count)]
                around = weight[layer, at] + margins(0, layer, start, count)
            else:
                s, around = stencil(root, (), layer, 0, layer, start, count)
            total = capac[layer, at] + s * around
            inverse = 1.0 / total
            weight[layer, at] = s * s * inverse
            for k in range(scen):
                slot = k * layers + layer
                if start == inner:
                    around = u1[k, layer + 1, at] + margins(1, slot, start, count)
                else:
                    _, around = stencil(up, (k,), layer, 1, slot, start, count)
                residual = (heat - total) * vp[k, layer, at]
                if layer % 2 == 0:
                    residual = residual + vq[k, layer // 2, at]
                residual = residual + s * around
                scaled = residual * inverse
                u0[k, layer + 1, pl.ds(HALO + start, count)] = s * scaled
                own = residual * scaled
                own = own[HALO:] if start == 0 else own[:HALO] if start > inner else own
                sums[k] = sums[k] + jnp.sum(own.reshape(-1, HALO, width), axis=0)
        return tuple(sums)

    def advance(source, target, edge):
        def one(layer, carry):
            sums = []
            for k in range(scen):
                centre, around = stencil(source, (k,), layer, edge, k * layers + layer)
                sums.append(gather(carry[len(sums)], centre * around))
                if target is not None:
                    moved = weight[layer] * around
                    target[k, layer + 1, body] = moved
                    sums.append(gather(carry[len(sums)], moved * around))
            return tuple(sums)

        carry = (none,) * (scen * (1 if target is None else 2))
        for layer in range(layers):
            carry = one(layer, carry)
        return carry

    first_sums = (none,) * scen
    for layer in range(layers):
        first_sums = begin(layer, first_sums)
    second = advance(u0, u1, 2)
    third = advance(u1, u2, 3)
    fourth = advance(u2, None, 4)
    moments = []
    for k in range(scen):
        moments += [first_sums[k], *second[2 * k:2 * k + 2], *third[2 * k:2 * k + 2], fourth[k]]
    count = len(moments)
    flat = jnp.zeros((1, width), jnp.float32)
    line = lax.broadcasted_iota(jnp.int32, (1, width), 1)
    for i, value in enumerate(moments):
        total = jnp.sum(jnp.sum(value, axis=0, keepdims=True), axis=1, keepdims=True)
        flat = jnp.where(line == i, total, flat)
    row[...] = flat
    rows[n - 1] = flat
    while len(heard) < len(reaches):
        know()

    def spread(i, carry):
        k = me + i
        pltpu.make_async_remote_copy(
            src_ref=row, dst_ref=rows.at[i - 1], send_sem=row_send, recv_sem=row_recv,
            device_id=jnp.where(k < n, k, k - n),
            device_id_type=pl.DeviceIdType.LOGICAL).start()
        return carry

    lax.fori_loop(1, n, spread, 0)
    for dx, dy, copy in copies:
        @pl.when(has[dx, dy])
        def _(copy=copy):
            copy.wait_send()
    own = pl.ds(2 * HALO, length)
    for layer in range(layers):
        if layer % 2 == 0:
            back = lookup(vm[layer // 2, inside], TIER_INV)
        else:
            back = lookup(vc[layer // 2, inside], CHANNEL_INV)
        for k in range(scen):
            for ref in (u0, u1, u2):
                ref[k, layer + 1, own] = back * ref[k, layer + 1, own]
    arrived = rows.at[pl.ds(0, n - 1)]
    pltpu.make_async_copy(arrived, arrived, row_recv).wait()
    summed = jnp.sum(rows[...], axis=0)
    total = [jnp.sum(jnp.where(line == i, summed, 0.0), axis=1, keepdims=True)
             for i in range(count)]
    each = count // scen
    for k in range(scen):
        c0, c1, c2 = coefficients(total[k * each:(k + 1) * each])
        for layer in range(layers):
            change = c0 * u0[k, layer + 1, own] + c1 * u1[k, layer + 1, own]
            change = change + c2 * u2[k, layer + 1, own]
            out[k, layer] = vp[k, layer, inside] + change
    pltpu.make_async_copy(arrived, arrived, row_send).wait()


def per_device(nx, ny, previous, dissipated, material, coolant):
    scen, layers, length, width = previous.shape
    tiers = material.shape[0]
    ext = length + 2 * HALO
    f32 = jnp.float32
    field = pltpu.VMEM((scen, layers + 2, ext + 2 * HALO, width), f32)
    strip = pltpu.VMEM((ext, width), f32)
    return pl.pallas_call(
        functools.partial(kernel, nx, ny),
        out_shape=pltpu.VMEM(previous.shape, f32),
        in_specs=[pl.BlockSpec(memory_space=pl.ANY)] * 4,
        out_specs=pl.BlockSpec(memory_space=pltpu.VMEM),
        scratch_shapes=[
            pltpu.VMEM((scen, layers, ext, width), f32),
            pltpu.VMEM((scen, tiers, ext, width), f32),
            pltpu.VMEM((tiers, ext, width), jnp.int32),
            pltpu.VMEM((layers - tiers, ext, width), jnp.int32),
            strip, strip, strip, strip,
            pltpu.VMEM((5, ext, width), f32),
            pltpu.VMEM((layers + 2, ext + 2 * HALO, width), f32),
            pltpu.VMEM((layers, ext, width), f32),
            pltpu.VMEM((layers, ext, width), f32),
            field, field, field, field,
            pltpu.VMEM((1, width), f32),
            pltpu.VMEM((nx * ny, 1, width), f32),
            pltpu.VMEM((2 * width, width), jnp.bfloat16),
            pltpu.VMEM((2 * width, width), jnp.bfloat16),
            pltpu.SemaphoreType.REGULAR((max(nx, ny).bit_length(),)),
            pltpu.SemaphoreType.DMA((4,)),
            pltpu.SemaphoreType.DMA((18,)),
            pltpu.SemaphoreType.DMA((18,)),
            pltpu.SemaphoreType.DMA,
            pltpu.SemaphoreType.DMA,
        ],
        compiler_params=pltpu.CompilerParams(
            collective_id=0, has_side_effects=True, vmem_limit_bytes=60 * 1024 * 1024),
    )(previous, dissipated, material, coolant)


def solution(mesh):
    return jax.shard_map(
        functools.partial(per_device, mesh.shape["gx"], mesh.shape["gy"]),
        mesh=mesh,
        in_specs=(
            P(None, None, "gx", "gy"),
            P(None, None, "gx", "gy"),
            P(None, "gx", "gy"),
            P(None, "gx", "gy"),
        ),
        out_specs=P(None, None, "gx", "gy"),
        check_vma=False,
    )
```

```python
import functools
import math

import jax
import jax.numpy as jnp
from jax import lax
from jax.experimental import pallas as pl
from jax.experimental.pallas import tpu as pltpu
from jax.sharding import PartitionSpec as P

ITERS = 3
TIER_K = (1.0, 0.3, 0.12, 2.5)
CHANNEL_K = (1.0, 0.3, 0.25, 0.2)
CHANNEL_SINK = (0.0, 0.15, 0.45, 1.2)
TIER_HEAT = 0.05
CHANNEL_HEAT = 0.2
VERTICAL = 4.0

HALO = 8
STRIP = 4
PIECE = 32
SPAN = 48
SLOT = 2 * STRIP
MESH = pl.DeviceIdType.MESH

TIER_ROOT = tuple(math.sqrt(v) for v in TIER_K)
CHANNEL_ROOT = tuple(math.sqrt(v) for v in CHANNEL_K)
TIER_INV = tuple(1.0 / math.sqrt(v) for v in TIER_K)
CHANNEL_INV = tuple(1.0 / math.sqrt(v) for v in CHANNEL_K)


def lookup(codes, table):
    total = jnp.zeros(codes.shape, jnp.float32)
    for index, value in enumerate(table):
        total = jnp.where(codes == index, jnp.float32(value), total)
    return total


def coefficients(nu):
    def inner(a, b):
        total = None
        for i, x in enumerate(a):
            for j, y in enumerate(b):
                term = x * y * nu[i + j]
                total = term if total is None else total + term
        return total

    zero = nu[0] * 0.0
    rho = [zero + 1.0]
    pi = [zero + 1.0]
    norm = nu[0]
    result = [zero] * ITERS
    for iteration in range(ITERS):
        image = [a - b for a, b in zip(pi + [zero], [zero] + pi)]
        step = norm / inner(pi, image)
        for i, a in enumerate(pi):
            result[i] = result[i] + step * a
        if iteration + 1 < ITERS:
            rho = [a - step * b for a, b in zip(rho + [zero], image)]
            following = inner(rho, rho)
            growth = following / norm
            pi = [a + growth * b for a, b in zip(rho, pi + [zero])]
            norm = following
    return result


def kernel(nx, ny, prev, diss, mat, cool, sums, vp, f0, f1, f2, vq, vm, vc, own_l, own_r, far_l, far_r,
           edges, root, weight, capac, up, u0, u1, u2, row, rows,
           along, across, known, load_sem, send_sem, recv_sem, row_send, row_recv):
    scen, layers, length, width = prev.shape
    tiers = mat.shape[0]
    n = nx * ny
    ext = length + 2 * HALO
    x, y = lax.axis_index("gx"), lax.axis_index("gy")
    me = x * ny + y
    barrier = pltpu.get_barrier_semaphore()

    def around_me(reach):
        found = []
        for dx in (-reach, 0, reach):
            for dy in (-reach, 0, reach):
                if (dx or dy) and abs(dx) < nx and abs(dy) < ny:
                    inside_x = jnp.logical_and(x + dx >= 0, x + dx < nx)
                    inside_y = jnp.logical_and(y + dy >= 0, y + dy < ny)
                    found.append((dx, dy, jnp.logical_and(inside_x, inside_y)))
        return found

    def greet(sem, reach):
        for dx, dy, there in around_me(reach):
            @pl.when(there)
            def _(dx=dx, dy=dy):
                pl.semaphore_signal(sem, inc=1, device_id=(x + dx, y + dy), device_id_type=MESH)

    def hear(sem, reach):
        pl.semaphore_wait(sem, sum(there.astype(jnp.int32) for _, _, there in around_me(reach)))

    reaches = [1]
    while 2 * reaches[-1] < max(nx, ny) - 1:
        reaches.append(2 * reaches[-1])
    heard = []

    def know():
        if len(heard) < len(reaches):
            hear(known.at[len(heard)], reaches[len(heard)])
            heard.append(True)
            if len(heard) < len(reaches):
                greet(known.at[len(heard)], reaches[len(heard)])

    inside = pl.ds(HALO, length)
    loads = [
        pltpu.make_async_copy(prev, vp.at[:, :, inside], load_sem.at[0]),
        pltpu.make_async_copy(diss, vq.at[:, :, inside], load_sem.at[1]),
        pltpu.make_async_copy(mat, vm.at[:, inside], load_sem.at[2]),
        pltpu.make_async_copy(cool, vc.at[:, inside], load_sem.at[3]),
    ]
    for copy in reversed(loads):
        copy.start()
    greet(barrier, 1)

    has = {(-1, 0): x > 0, (1, 0): x < nx - 1, (0, -1): y > 0, (0, 1): y < ny - 1}
    for dx in (-1, 1):
        for dy in (-1, 1):
            has[dx, dy] = jnp.logical_and(has[dx, 0], has[0, dy])
    top, bottom = pl.ds(0, HALO), pl.ds(HALO + length, HALO)
    first, last = pl.ds(HALO, HALO), pl.ds(length, HALO)

    def fill(ref):
        ref[...] = jnp.full(ref.shape, -1, ref.dtype)

    for dx, where in ((-1, top), (1, bottom)):
        @pl.when(jnp.logical_not(has[dx, 0]))
        def _(where=where):
            for ref in (vp, vq):
                fill(ref.at[:, :, where])
            for ref in (vm, vc):
                fill(ref.at[:, where])
            fill(own_l.at[where])
            fill(own_r.at[where])
    for dy, ref in ((-1, far_l), (1, far_r)):
        @pl.when(jnp.logical_not(has[0, dy]))
        def _(ref=ref):
            fill(ref.at[inside])
        for dx, where in ((-1, top), (1, bottom)):
            @pl.when(jnp.logical_not(has[dx, dy]))
            def _(ref=ref, where=where):
                fill(ref.at[where])

    for i in range(2):
        source = lax.broadcasted_iota(jnp.int32, (width, width), 0)
        target = lax.broadcasted_iota(jnp.int32, (width, width), 1)
        apart = target - source
        beside = (apart == 1) | (apart == -1)
        along[pl.ds(i * width, width)] = jnp.where(beside, 1.0, 0.0).astype(jnp.bfloat16)
        spot = target // SLOT
        level = spot % layers
        used = spot < scen * layers
        beside = beside & (source // SLOT == spot) & used
        stacked = (apart == SLOT) & (level > 0) | (apart == -SLOT) & (level < layers - 1)
        weights = jnp.where(stacked & used, VERTICAL, jnp.where(beside, 1.0, 0.0))
        across[pl.ds(i * width, width)] = weights.astype(jnp.bfloat16)
    blank = jnp.zeros((ext + 3 * HALO, width), jnp.float32)
    for pad in (0, layers + 1):
        root[pad] = blank
        for s in range(scen):
            for ref in (up, u0, u1, u2):
                ref[s, pad] = blank

    first_places, later_places = [], []
    for layer in range(layers):
        ref = vm if layer % 2 == 0 else vc
        first_places.append((SLOT * layer + STRIP, ref, (layer // 2,)))
    for t in range(tiers):
        first_places.append((SLOT * (layers + 1 + 2 * t) + STRIP, vq, (0, t)))
        first_places.append((SLOT * (layers + 2 * t) + STRIP, vq, (1, t)))
    for s in range(scen):
        for layer in range(layers):
            later_places.append((SLOT * (s * layers + layer), vp, (s, layer)))

    def pack(places):
        lane = lax.broadcasted_iota(jnp.int32, (length, width), 1)
        left = right = opening = None
        for base, ref, index in sorted(places, key=lambda place: place[0]):
            plane = ref[index + (inside,)].astype(jnp.float32)
            turned = pltpu.roll(plane, base, 1) if base else plane
            if left is None:
                left = right = turned
                opening = None if base else plane
            else:
                left = jnp.where(lane >= base, turned, left)
                right = jnp.where(lane >= base - STRIP, turned, right)
        if opening is not None:
            right = jnp.where(lane >= width - STRIP, opening, right)
        return left, right

    for copy in loads[1:]:
        copy.wait()
    own_l[inside], own_r[inside] = pack(first_places)
    loads[0].wait()
    left, right = pack(later_places)
    low = lax.broadcasted_iota(jnp.int32, (length, width), 1) % SLOT < STRIP
    own_l[inside] = jnp.where(low, left, own_l[inside])
    own_r[inside] = jnp.where(low, own_r[inside], right)

    hear(barrier, 1)
    greet(known.at[0], 1)

    sends = []
    for dx, source, target in ((-1, first, bottom), (1, last, top)):
        for ref in (vp, vq):
            sends.append((dx, 0, ref.at[:, :, source], ref.at[:, :, target]))
        for ref in (vm, vc):
            sends.append((dx, 0, ref.at[:, source], ref.at[:, target]))
        for ref in (own_l, own_r):
            sends.append((dx, 0, ref.at[source], ref.at[target]))
        sends.append((dx, -1, own_l.at[source], far_r.at[target]))
        sends.append((dx, 1, own_r.at[source], far_l.at[target]))
    sends.append((0, -1, own_l.at[inside], far_r.at[inside]))
    sends.append((0, 1, own_r.at[inside], far_l.at[inside]))
    copies = []
    for i, (dx, dy, source, target) in enumerate(sends):
        copy = pltpu.make_async_remote_copy(
            src_ref=source, dst_ref=target, send_sem=send_sem.at[i], recv_sem=recv_sem.at[i],
            device_id=(x + dx, y + dy), device_id_type=MESH)
        copies.append((dx, dy, copy))
    order = sorted(copies, key=lambda c: 0 if c[0] and c[1] else 1 if c[0] == 0 else 2)
    for dx, dy, copy in order:
        @pl.when(has[dx, dy])
        def _(copy=copy):
            copy.start()
    def prepare(at, to):
        count = at.size
        for layer in range(layers):
            if layer % 2 == 0:
                s = lookup(vm[layer // 2, at], TIER_ROOT)
                total = jnp.full((count, width), TIER_HEAT, jnp.float32)
            else:
                codes = vc[layer // 2, at]
                s = lookup(codes, CHANNEL_ROOT)
                total = CHANNEL_HEAT + lookup(codes, CHANNEL_SINK)
            root[layer + 1, to] = s
            capac[layer, at] = total
            for k in range(scen):
                up[k, layer + 1, to] = s * vp[k, layer, at]

    def in_pieces(step):
        def one(i, carry):
            step(pl.multiple_of(i * PIECE, PIECE))
            return carry

        lax.fori_loop(0, length // PIECE, one, 0)

    in_pieces(lambda start: prepare(pl.ds(HALO + start, PIECE), pl.ds(2 * HALO + start, PIECE)))
    know()

    def shifted(value, matrix):
        high = value.astype(jnp.bfloat16)
        low = (value - high.astype(jnp.float32)).astype(jnp.bfloat16)
        return jnp.dot(jnp.concatenate([high, low], axis=1), matrix[...],
                       preferred_element_type=jnp.float32)

    def spans(start, count):
        pieces = []
        while count > 0:
            piece = min(count, SPAN)
            pieces.append((start, piece))
            start, count = start + piece, count - piece
        return pieces

    def column(ref, at, start, count):
        rows_at = pl.ds(HALO + start, count)
        above, centre = None, ref[at + (1, rows_at)]
        for layer in range(layers):
            below = ref[at + (layer + 2, rows_at)] if layer + 1 < layers else None
            lateral = shifted(centre, along) + ref[at + (layer + 1, pl.ds(HALO + start - 1, count))]
            lateral = lateral + ref[at + (layer + 1, pl.ds(HALO + start + 1, count))]
            vertical = below if above is None else above if below is None else above + below
            around = lateral if vertical is None else lateral + VERTICAL * vertical
            yield layer, centre, around
            above, centre = centre, below

    def margins(edge, slot):
        lane = lax.broadcasted_iota(jnp.int32, edge.shape, 1)
        ends = (lane == 0) | (lane == width - 1)
        shift = (width - SLOT * slot - (STRIP - 1)) % width
        return jnp.where(ends, pltpu.roll(edge, shift, 1), 0.0)

    inner, rest = 2 * HALO, length - 2 * HALO

    for start, count in spans(inner, rest):
        at = pl.ds(start, count)
        for layer, _, around in column(root, (), start, count):
            weight[layer, at] = around
        for k in range(scen):
            for layer, _, around in column(up, (k,), start, count):
                u1[k, layer + 1, at] = around
    know()

    for dx, dy, copy in copies:
        @pl.when(has[-dx, -dy])
        def _(copy=copy):
            copy.wait_recv()

    prepare(pl.ds(0, HALO), pl.ds(HALO, HALO))
    prepare(pl.ds(HALO + length, HALO), pl.ds(2 * HALO + length, HALO))

    shape = (ext, width)
    lane = lax.broadcasted_iota(jnp.int32, shape, 1)
    place = lane // SLOT
    low = lane % SLOT < STRIP
    layer_of = place % layers
    tier = layer_of % 2 == 0
    used = place < scen * layers

    def strip_stencil(u):
        return shifted(u, across) + pltpu.roll(u, 1, 0) + pltpu.roll(u, ext - 1, 0)

    def strip(west, east):
        field = pltpu.roll(jnp.where(low, east, west), STRIP, 1)
        rest = jnp.where(low, west, east)
        codes = jnp.where(place < layers, rest, pltpu.roll(rest, SLOT * layers, 1))
        codes = jnp.where(used, codes, -1.0)
        power = jnp.where(place < layers, pltpu.roll(rest, width - SLOT * (layers + 1), 1), rest)
        power = jnp.where(tier & used, power, 0.0)
        s = jnp.where(tier, lookup(codes, TIER_ROOT), lookup(codes, CHANNEL_ROOT))
        heat = jnp.where(tier, TIER_HEAT, CHANNEL_HEAT)
        total = heat + jnp.where(tier, 0.0, lookup(codes, CHANNEL_SINK))
        total = total + s * strip_stencil(s)
        inverse = 1.0 / total
        scaled = s * field
        residual = (heat - total) * field + power + s * strip_stencil(scaled)
        w = s * s * inverse
        a = s * residual * inverse
        b = w * strip_stencil(a)
        c = w * strip_stencil(b)
        return s, scaled, a, b, c

    for i, value in enumerate(strip(far_l[...], own_l[...])):
        edges[i] = value
    rights = strip(own_r[...], far_r[...])
    for i, value in enumerate(rights):
        edges[i] = jnp.where(lane % SLOT == STRIP - 1, edges[i], pltpu.roll(value, width - 2, 1))
    last_u = rights[-1]
    across_u = last_u * pltpu.roll(last_u, width - 1, 1)
    crossing = []
    for k in range(scen):
        mine = (lane % SLOT == STRIP - 1) & (place // layers == k)
        crossing.append(jnp.where(mine, across_u, 0.0))

    def gather(total, value, start):
        first = max(HALO - start, 0)
        last = min(HALO + length - start, value.shape[0])
        if last <= first:
            return total
        return total + jnp.sum(value[first:last].reshape(-1, HALO, width), axis=0)

    none = jnp.zeros((HALO, width), jnp.float32)

    def begin():
        norms = [none] * scen
        for start, count in ((0, inner), *spans(inner, rest), (inner + rest, inner)):
            at = pl.ds(start, count)
            ahead = inner <= start < inner + rest
            if not ahead:
                for layer, _, around in column(root, (), start, count):
                    weight[layer, at] = around
                for k in range(scen):
                    for layer, _, around in column(up, (k,), start, count):
                        u1[k, layer + 1, at] = around
            coupling, flow = edges[0, at], edges[1, at]
            for layer in range(layers):
                s = root[layer + 1, pl.ds(HALO + start, count)]
                total = capac[layer, at] + s * (weight[layer, at] + margins(coupling, layer))
                inverse = 1.0 / total
                weight[layer, at] = s * s * inverse
                heat = TIER_HEAT if layer % 2 == 0 else CHANNEL_HEAT
                for k in range(scen):
                    around = u1[k, layer + 1, at] + margins(flow, k * layers + layer)
                    residual = (heat - total) * vp[k, layer, at] + s * around
                    if layer % 2 == 0:
                        residual = residual + vq[k, layer // 2, at]
                    scaled = residual * inverse
                    u0[k, layer + 1, pl.ds(HALO + start, count)] = s * scaled
                    norms[k] = gather(norms[k], residual * scaled, start)
        return norms

    def advance(source, target, edge):
        sums = []
        for k in range(scen):
            one = two = none
            for start, count in spans(0, ext):
                at = pl.ds(start, count)
                flow = edges[edge, at]
                for layer, centre, around in column(source, (k,), start, count):
                    around = around + margins(flow, k * layers + layer)
                    one = gather(one, centre * around, start)
                    moved = weight[layer, at] * around
                    target[k, layer + 1, pl.ds(HALO + start, count)] = moved
                    two = gather(two, moved * around, start)
            sums += [one, two]
        return sums

    def finish(source):
        sums = []
        for k in range(scen):
            total = gather(none, crossing[k], 0)
            for start, count in spans(2 * HALO, length):
                lane = lax.broadcasted_iota(jnp.int32, (count, width), 1)
                centre = source[k, 1, pl.ds(start, count)]
                for layer in range(layers):
                    ahead = jnp.where(lane < width - 1, pltpu.roll(centre, width - 1, 1), 0.0)
                    ahead = ahead + source[k, layer + 1, pl.ds(start + 1, count)]
                    below = None
                    if layer + 1 < layers:
                        below = source[k, layer + 2, pl.ds(start, count)]
                        ahead = ahead + VERTICAL * below
                    total = total + jnp.sum((centre * ahead).reshape(-1, HALO, width), axis=0)
                    centre = below
            sums.append(2.0 * total)
        return sums

    first_sums = begin()
    second = advance(u0, u1, 2)
    third = advance(u1, u2, 3)
    fourth = finish(u2)
    moments = []
    for k in range(scen):
        moments += [first_sums[k], *second[2 * k:2 * k + 2], *third[2 * k:2 * k + 2], fourth[k]]
    count = len(moments)
    flat = jnp.zeros((1, width), jnp.float32)
    line = lax.broadcasted_iota(jnp.int32, (1, width), 1)
    for i, value in enumerate(moments):
        total = jnp.sum(jnp.sum(value, axis=0, keepdims=True), axis=1, keepdims=True)
        flat = jnp.where(line == i, total, flat)
    row[...] = flat
    rows[n - 1] = flat
    while len(heard) < len(reaches):
        know()

    def spread(i, carry):
        k = me + i
        pltpu.make_async_remote_copy(
            src_ref=row, dst_ref=rows.at[i - 1], send_sem=row_send, recv_sem=row_recv,
            device_id=jnp.where(k < n, k, k - n),
            device_id_type=pl.DeviceIdType.LOGICAL).start()
        return carry

    lax.fori_loop(1, n, spread, 0)
    for dx, dy, copy in copies:
        @pl.when(has[dx, dy])
        def _(copy=copy):
            copy.wait_send()
    def unscale(start):
        at = pl.ds(HALO + start, PIECE)
        for layer in range(layers):
            if layer % 2 == 0:
                back = lookup(vm[layer // 2, at], TIER_INV)
            else:
                back = lookup(vc[layer // 2, at], CHANNEL_INV)
            for k in range(scen):
                for ref, scaled in ((u0, f0), (u1, f1), (u2, f2)):
                    value = ref[k, layer + 1, pl.ds(2 * HALO + start, PIECE)]
                    scaled[k, layer, pl.ds(start, PIECE)] = back * value

    in_pieces(unscale)
    arrived = rows.at[pl.ds(0, n - 1)]
    pltpu.make_async_copy(arrived, arrived, row_recv).wait()
    sums[...] = jnp.sum(rows[...], axis=0)
    pltpu.make_async_copy(arrived, arrived, row_send).wait()


def combine(sums, vp, f0, f1, f2, out, result, sem):
    scen, layers, length, width = result.shape
    line = lax.broadcasted_iota(jnp.int32, (1, width), 1)
    each = 2 * ITERS
    total = [jnp.sum(jnp.where(line == i, sums[...], 0.0), axis=1, keepdims=True)
             for i in range(scen * each)]
    for k in range(scen):
        c0, c1, c2 = coefficients(total[k * each:(k + 1) * each])
        for layer in range(layers):
            for offset in range(0, length, PIECE):
                at = pl.ds(offset, min(PIECE, length - offset))
                change = c0 * f0[k, layer, at] + c1 * f1[k, layer, at] + c2 * f2[k, layer, at]
                before = vp[k, layer, pl.ds(HALO + offset, min(PIECE, length - offset))]
                result[k, layer, at] = before + change
            pltpu.make_async_copy(result.at[k, layer], out.at[k, layer], sem).start()
    pltpu.make_async_copy(result, out, sem).wait()


def per_device(nx, ny, previous, dissipated, material, coolant):
    scen, layers, length, width = previous.shape
    tiers = material.shape[0]
    ext = length + 2 * HALO
    f32 = jnp.float32
    field = pltpu.VMEM((scen, layers + 2, ext + 3 * HALO, width), f32)
    strip = pltpu.VMEM((ext, width), f32)
    own = pltpu.VMEM(previous.shape, f32)
    shared = pl.pallas_call(
        functools.partial(kernel, nx, ny),
        out_shape=(pltpu.VMEM((1, width), f32), pltpu.VMEM((scen, layers, ext, width), f32), own, own, own),
        in_specs=[pl.BlockSpec(memory_space=pl.ANY)] * 4,
        out_specs=[pl.BlockSpec(memory_space=pltpu.VMEM)] * 5,
        scratch_shapes=[
            pltpu.VMEM((scen, tiers, ext, width), f32),
            pltpu.VMEM((tiers, ext, width), jnp.int32),
            pltpu.VMEM((layers - tiers, ext, width), jnp.int32),
            strip, strip, strip, strip,
            pltpu.VMEM((5, ext, width), f32),
            pltpu.VMEM((layers + 2, ext + 3 * HALO, width), f32),
            pltpu.VMEM((layers, ext, width), f32),
            pltpu.VMEM((layers, ext, width), f32),
            field, field, field, field,
            pltpu.VMEM((1, width), f32),
            pltpu.VMEM((nx * ny, 1, width), f32),
            pltpu.VMEM((2 * width, width), jnp.bfloat16),
            pltpu.VMEM((2 * width, width), jnp.bfloat16),
            pltpu.SemaphoreType.REGULAR((max(nx, ny).bit_length(),)),
            pltpu.SemaphoreType.DMA((4,)),
            pltpu.SemaphoreType.DMA((18,)),
            pltpu.SemaphoreType.DMA((18,)),
            pltpu.SemaphoreType.DMA,
            pltpu.SemaphoreType.DMA,
        ],
        compiler_params=pltpu.CompilerParams(
            collective_id=0, has_side_effects=True, vmem_limit_bytes=48 * 1024 * 1024),
    )(*(pltpu.with_memory_space_constraint(part, pltpu.HBM)
        for part in (previous, dissipated, material, coolant)))
    shared = [pltpu.with_memory_space_constraint(part, pltpu.VMEM) for part in shared]
    return pl.pallas_call(
        combine,
        out_shape=jax.ShapeDtypeStruct(previous.shape, f32),
        in_specs=[pl.BlockSpec(memory_space=pltpu.VMEM)] * 5,
        out_specs=pl.BlockSpec(memory_space=pl.ANY),
        scratch_shapes=[own, pltpu.SemaphoreType.DMA],
        compiler_params=pltpu.CompilerParams(vmem_limit_bytes=16 * 1024 * 1024),
    )(*shared)


def solution(mesh):
    return jax.shard_map(
        functools.partial(per_device, mesh.shape["gx"], mesh.shape["gy"]),
        mesh=mesh,
        in_specs=(
            P(None, None, "gx", "gy"),
            P(None, None, "gx", "gy"),
            P(None, "gx", "gy"),
            P(None, "gx", "gy"),
        ),
        out_specs=P(None, None, "gx", "gy"),
        check_vma=False,
    )
```

```python
import functools
import math

import jax
import jax.numpy as jnp
from jax import lax
from jax.experimental import pallas as pl
from jax.experimental.pallas import tpu as pltpu
from jax.sharding import PartitionSpec as P

ITERS = 3
TIER_K = (1.0, 0.3, 0.12, 2.5)
CHANNEL_K = (1.0, 0.3, 0.25, 0.2)
CHANNEL_SINK = (0.0, 0.15, 0.45, 1.2)
TIER_HEAT = 0.05
CHANNEL_HEAT = 0.2
VERTICAL = 4.0

HALO = 8
STRIP = 4
PIECE = 32
SPAN = 48
SLOT = 4 * STRIP
MESH = pl.DeviceIdType.MESH

TIER_ROOT = tuple(math.sqrt(v) for v in TIER_K)
CHANNEL_ROOT = tuple(math.sqrt(v) for v in CHANNEL_K)
TIER_INV = tuple(1.0 / math.sqrt(v) for v in TIER_K)
CHANNEL_INV = tuple(1.0 / math.sqrt(v) for v in CHANNEL_K)


def lookup(codes, table):
    total = jnp.zeros(codes.shape, jnp.float32)
    for index, value in enumerate(table):
        total = jnp.where(codes == index, jnp.float32(value), total)
    return total


def coefficients(nu):
    def inner(a, b):
        total = None
        for i, x in enumerate(a):
            for j, y in enumerate(b):
                term = x * y * nu[i + j]
                total = term if total is None else total + term
        return total

    zero = nu[0] * 0.0
    rho = [zero + 1.0]
    pi = [zero + 1.0]
    norm = nu[0]
    result = [zero] * ITERS
    for iteration in range(ITERS):
        image = [a - b for a, b in zip(pi + [zero], [zero] + pi)]
        step = norm / inner(pi, image)
        for i, a in enumerate(pi):
            result[i] = result[i] + step * a
        if iteration + 1 < ITERS:
            rho = [a - step * b for a, b in zip(rho + [zero], image)]
            following = inner(rho, rho)
            growth = following / norm
            pi = [a + growth * b for a, b in zip(rho, pi + [zero])]
            norm = following
    return result


def kernel(nx, ny, prev, diss, mat, cool, sums, vp, f0, f1, f2, vq, vm, vc, near, own_l, own_r, far_l, far_r,
           edges, faces, root, weight, capac, slope, up, u0, u1, u2, row, rows,
           along, on_left, on_right, known, load_sem, send_sem, recv_sem, row_send, row_recv):
    scen, layers, length, width = prev.shape
    tiers = mat.shape[0]
    n = nx * ny
    ext = length + 2 * HALO
    x, y = lax.axis_index("gx"), lax.axis_index("gy")
    me = x * ny + y
    barrier = pltpu.get_barrier_semaphore()

    def around_me(reach):
        found = []
        for dx in (-reach, 0, reach):
            for dy in (-reach, 0, reach):
                if (dx or dy) and abs(dx) < nx and abs(dy) < ny:
                    inside_x = jnp.logical_and(x + dx >= 0, x + dx < nx)
                    inside_y = jnp.logical_and(y + dy >= 0, y + dy < ny)
                    found.append((dx, dy, jnp.logical_and(inside_x, inside_y)))
        return found

    def greet(sem, reach):
        for dx, dy, there in around_me(reach):
            @pl.when(there)
            def _(dx=dx, dy=dy):
                pl.semaphore_signal(sem, inc=1, device_id=(x + dx, y + dy), device_id_type=MESH)

    def hear(sem, reach):
        pl.semaphore_wait(sem, sum(there.astype(jnp.int32) for _, _, there in around_me(reach)))

    reaches = [1]
    while 2 * reaches[-1] < max(nx, ny) - 1:
        reaches.append(2 * reaches[-1])
    heard = []

    def know():
        if len(heard) < len(reaches):
            hear(known.at[len(heard)], reaches[len(heard)])
            heard.append(True)
            if len(heard) < len(reaches):
                greet(known.at[len(heard)], reaches[len(heard)])

    inside = pl.ds(HALO, length)
    loads = [
        pltpu.make_async_copy(prev, vp.at[:, :, inside], load_sem.at[0]),
        pltpu.make_async_copy(diss, vq.at[:, :, inside], load_sem.at[1]),
        pltpu.make_async_copy(mat, vm.at[:, inside], load_sem.at[2]),
        pltpu.make_async_copy(cool, vc.at[:, inside], load_sem.at[3]),
    ]
    for copy in reversed(loads):
        copy.start()
    greet(barrier, 1)

    has = {(-1, 0): x > 0, (1, 0): x < nx - 1, (0, -1): y > 0, (0, 1): y < ny - 1}
    for dx in (-1, 1):
        for dy in (-1, 1):
            has[dx, dy] = jnp.logical_and(has[dx, 0], has[0, dy])
    top, bottom = pl.ds(0, HALO), pl.ds(HALO + length, HALO)
    first, last = pl.ds(HALO, HALO), pl.ds(length, HALO)

    def fill(ref):
        ref[...] = jnp.full(ref.shape, -1, ref.dtype)

    for dx, where in ((-1, top), (1, bottom)):
        @pl.when(jnp.logical_not(has[dx, 0]))
        def _(where=where):
            for ref in (vp, vq):
                fill(ref.at[:, :, where])
            for ref in (vm, vc):
                fill(ref.at[:, where])
            fill(near.at[:, where])
    for dy, ref in ((-1, far_l), (1, far_r)):
        @pl.when(jnp.logical_not(has[0, dy]))
        def _(ref=ref):
            fill(ref.at[inside])
        for dx, where in ((-1, top), (1, bottom)):
            @pl.when(jnp.logical_not(has[dx, dy]))
            def _(ref=ref, where=where):
                fill(ref.at[where])

    source = lax.broadcasted_iota(jnp.int32, (width, width), 0)
    target = lax.broadcasted_iota(jnp.int32, (width, width), 1)
    beside = jnp.abs(target - source) == 1
    matrices = [(along, jnp.where(beside, 1.0, 0.0))]
    for ref, shift in ((on_left, 0), (on_right, STRIP)):
        begins, ends = (source + shift) % width, (target + shift) % width
        apart, spot = ends - begins, ends // SLOT
        valid = (spot < layers) & (ends % SLOT < 3 * STRIP) & (begins % SLOT < 3 * STRIP)
        beside = ((apart == 1) | (apart == -1)) & (begins // SLOT == spot)
        stacked = (apart == SLOT) & (spot > 0) | (apart == -SLOT) & (spot < layers - 1)
        weights = jnp.where(stacked, VERTICAL, jnp.where(beside, 1.0, 0.0))
        matrices.append((ref, jnp.where(valid, weights, 0.0)))
    for ref, weights in matrices:
        for i in range(2):
            ref[pl.ds(i * width, width)] = weights.astype(jnp.bfloat16)
    blank = jnp.zeros((ext + 3 * HALO, width), jnp.float32)
    for pad in (0, layers + 1):
        root[pad] = blank
        for k in range(scen):
            for ref in (up, u0, u1, u2):
                ref[k, pad] = blank
    for at in (pl.ds(HALO, HALO), pl.ds(2 * HALO + length, HALO)):
        for layer in range(layers):
            root[layer + 1, at] = blank[:HALO]
            for k in range(scen):
                for ref in (up, u0, u1, u2):
                    ref[k, layer + 1, at] = blank[:HALO]

    def pack(places):
        lane = lax.broadcasted_iota(jnp.int32, (length, width), 1)
        packed = opening = None
        for layer, ref, index in places:
            plane = ref[index + (inside,)].astype(jnp.float32)
            turned = pltpu.roll(plane, SLOT * layer + STRIP, 1)
            if packed is None:
                packed = opening = turned
            else:
                packed = jnp.where(lane >= SLOT * layer - STRIP, turned, packed)
        return jnp.where(lane >= width - STRIP, opening, packed)

    def letter(shifts):
        lane = lax.broadcasted_iota(jnp.int32, (length, width), 1)
        q = lane % SLOT
        parts = []
        for i, shift in enumerate(shifts):
            part = near[i, inside]
            parts.append(pltpu.roll(part, shift, 1) if shift else part)
        power = jnp.where(lane // SLOT % 2 == 0, parts[3], parts[4])
        rest = jnp.where(q < 3 * STRIP, parts[2], power)
        return jnp.where(q < STRIP, parts[0], jnp.where(q < 2 * STRIP, parts[1], rest))

    for copy in loads[1:]:
        copy.wait()
    near[scen, inside] = pack([(layer, vc if layer % 2 else vm, (layer // 2,)) for layer in range(layers)])
    for k in range(scen):
        near[scen + 1 + k, inside] = pack([(2 * t, vq, (k, t)) for t in range(tiers)])
    loads[0].wait()
    for k in range(scen):
        near[k, inside] = pack([(layer, vp, (k, layer)) for layer in range(layers)])
    own_l[...] = letter((width - STRIP, 0, STRIP, 2 * STRIP, 6 * STRIP))
    own_r[...] = letter((0, STRIP, 2 * STRIP, 3 * STRIP, 7 * STRIP))

    hear(barrier, 1)
    greet(known.at[0], 1)

    sends = []
    for dx, source, target in ((-1, first, bottom), (1, last, top)):
        for ref in (vp, vq):
            sends.append((dx, 0, ref.at[:, :, source], ref.at[:, :, target]))
        for ref in (vm, vc):
            sends.append((dx, 0, ref.at[:, source], ref.at[:, target]))
        sends.append((dx, 0, near.at[:, source], near.at[:, target]))
        begins = pl.ds(0 if dx < 0 else length - HALO, HALO)
        sends.append((dx, -1, own_l.at[begins], far_r.at[target]))
        sends.append((dx, 1, own_r.at[begins], far_l.at[target]))
    sends.append((0, -1, own_l, far_r.at[inside]))
    sends.append((0, 1, own_r, far_l.at[inside]))
    copies = []
    for i, (dx, dy, source, target) in enumerate(sends):
        copy = pltpu.make_async_remote_copy(
            src_ref=source, dst_ref=target, send_sem=send_sem.at[i], recv_sem=recv_sem.at[i],
            device_id=(x + dx, y + dy), device_id_type=MESH)
        copies.append((dx, dy, copy))
    order = sorted(copies, key=lambda c: 0 if c[0] and c[1] else 1 if c[0] == 0 else 2)
    for dx, dy, copy in order:
        @pl.when(has[dx, dy])
        def _(copy=copy):
            copy.start()
    def prepare(at, to):
        count = at.size
        for layer in range(layers):
            if layer % 2 == 0:
                s = lookup(vm[layer // 2, at], TIER_ROOT)
                total = jnp.full((count, width), TIER_HEAT, jnp.float32)
            else:
                codes = vc[layer // 2, at]
                s = lookup(codes, CHANNEL_ROOT)
                total = CHANNEL_HEAT + lookup(codes, CHANNEL_SINK)
            root[layer + 1, to] = s
            capac[layer, at] = total
            for k in range(scen):
                up[k, layer + 1, to] = s * vp[k, layer, at]

    def in_pieces(step):
        def one(i, carry):
            step(pl.multiple_of(i * PIECE, PIECE))
            return carry

        lax.fori_loop(0, length // PIECE, one, 0)

    in_pieces(lambda start: prepare(pl.ds(HALO + start, PIECE), pl.ds(2 * HALO + start, PIECE)))

    def shifted(value, matrix):
        high = value.astype(jnp.bfloat16)
        low = (value - high.astype(jnp.float32)).astype(jnp.bfloat16)
        return jnp.dot(jnp.concatenate([high, low], axis=1), matrix[...],
                       preferred_element_type=jnp.float32)

    def spans(start, count):
        pieces = []
        while count > 0:
            piece = min(count, SPAN)
            pieces.append((start, piece))
            start, count = start + piece, count - piece
        return pieces

    def column(ref, at, places):
        centres = []
        for layer in range(layers):
            for start, count in places:
                centres.append(ref[at + (layer + 1, pl.ds(HALO + start, count))])
        lateral = shifted(jnp.concatenate(centres, axis=0), along)
        offset = 0
        for i, centre in enumerate(centres):
            layer, (start, count) = i // len(places), places[i % len(places)]
            around = lateral[offset:offset + count]
            offset += count
            around = around + ref[at + (layer + 1, pl.ds(HALO + start - 1, count))]
            around = around + ref[at + (layer + 1, pl.ds(HALO + start + 1, count))]
            stacked = [centres[j] for j in (i - len(places), i + len(places)) if 0 <= j < len(centres)]
            if stacked:
                around = around + VERTICAL * sum(stacked[1:], stacked[0])
            yield layer, start, count, centre, around

    def margins(edge, layer):
        lane = lax.broadcasted_iota(jnp.int32, edge.shape, 1)
        ends = (lane == 0) | (lane == width - 1)
        shift = (width - SLOT * layer - (STRIP - 1)) % width
        return jnp.where(ends, pltpu.roll(edge, shift, 1), 0.0)

    def patched(value, face, layer):
        lane = lax.broadcasted_iota(jnp.int32, face.shape, 1)
        ends = (lane < STRIP) | (lane >= width - STRIP)
        return jnp.where(ends, pltpu.roll(face, width - SLOT * layer - STRIP, 1), value)

    def gather(total, value, start, low, high):
        first, last = max(low - start, 0), min(high - start, value.shape[0])
        if last <= first:
            return total
        return total + jnp.sum(value[first:last].reshape(-1, HALO, width), axis=0)

    none = jnp.zeros((HALO, width), jnp.float32)
    each = 2 * ITERS

    def begin(sums, places, low, high, edged):
        for layer, start, count, _, around in column(root, (), places):
            at = pl.ds(start, count)
            s = root[layer + 1, pl.ds(HALO + start, count)]
            if edged:
                around = around + margins(edges[0, at], layer)
            total = capac[layer, at] + s * around
            inverse = 1.0 / total
            weight[layer, at] = s * s * inverse
            slope[layer, at] = total
        for k in range(scen):
            for layer, start, count, _, around in column(up, (k,), places):
                at = pl.ds(start, count)
                if edged:
                    around = around + margins(edges[1 + 4 * k, at], layer)
                s = root[layer + 1, pl.ds(HALO + start, count)]
                total = slope[layer, at]
                heat = TIER_HEAT if layer % 2 == 0 else CHANNEL_HEAT
                residual = (heat - total) * vp[k, layer, at] + s * around
                if layer % 2 == 0:
                    residual = residual + vq[k, layer // 2, at]
                scaled = residual / total
                u0[k, layer + 1, pl.ds(HALO + start, count)] = s * scaled
                sums[k][0] = gather(sums[k][0], residual * scaled, start, low, high)

    def advance(sums, source, target, level, places, low, high, edged):
        for k in range(scen):
            for layer, start, count, centre, around in column(source, (k,), places):
                at = pl.ds(start, count)
                if edged:
                    around = around + margins(edges[1 + 4 * k + level, at], layer)
                i = 2 * level - 1
                sums[k][i] = gather(sums[k][i], centre * around, start, low, high)
                if target is not None:
                    moved = weight[layer, at] * around
                    target[k, layer + 1, pl.ds(HALO + start, count)] = moved
                    sums[k][i + 1] = gather(sums[k][i + 1], moved * around, start, low, high)

    core = [[none] * each for _ in range(scen)]
    core_rows = (2 * HALO, length)
    whole = spans(HALO, length)
    for place in whole:
        begin(core, [place], *core_rows, False)
    know()
    for place in whole:
        advance(core, u0, u1, 1, [place], *core_rows, False)
    for place in whole:
        advance(core, u1, u2, 2, [place], *core_rows, False)
    for place in spans(2 * HALO, length - 2 * HALO):
        advance(core, u2, None, 3, [place], *core_rows, False)

    know()
    for dx, dy, copy in copies:
        @pl.when(has[-dx, -dy])
        def _(copy=copy):
            copy.wait_recv()

    prepare(pl.ds(0, HALO), pl.ds(HALO, HALO))
    prepare(pl.ds(HALO + length, HALO), pl.ds(2 * HALO + length, HALO))

    shape = (ext, width)
    lane = lax.broadcasted_iota(jnp.int32, shape, 1)

    def strip(far, shifts, low, high, matrix, shift, sums):
        q = lane % SLOT
        theirs = (q >= low) & (q < high)
        turned = (lane + shift) % width
        valid = (turned // SLOT < layers) & (turned % SLOT < 3 * STRIP)
        tier = turned // SLOT % 2 == 0
        message = far[...]
        parts = []
        for i, turn in enumerate(shifts):
            other = pltpu.roll(message, turn, 1) if turn else message
            parts.append(jnp.where(theirs, other, near[i]))

        def around(u):
            return shifted(u, matrix) + pltpu.roll(u, 1, 0) + pltpu.roll(u, ext - 1, 0)

        def add(k, i, value):
            kept = value[2 * HALO:length].reshape(-1, HALO, width)
            sums[k][i] = sums[k][i] + jnp.sum(kept, axis=0)

        codes = jnp.where(valid, parts[scen], -1.0)
        s = jnp.where(tier, lookup(codes, TIER_ROOT), lookup(codes, CHANNEL_ROOT))
        heat = jnp.where(tier, TIER_HEAT, CHANNEL_HEAT)
        total = heat + jnp.where(tier, 0.0, lookup(codes, CHANNEL_SINK)) + s * around(s)
        inverse = 1.0 / total
        w = s * s * inverse
        found = [s]
        for k in range(scen):
            power = jnp.where(tier & valid, parts[scen + 1 + k], 0.0)
            flow = s * parts[k]
            residual = (heat - total) * parts[k] + power + s * around(flow)
            scaled = residual * inverse
            a = s * scaled
            v = around(a)
            b = w * v
            add(k, 0, residual * scaled)
            add(k, 1, a * v)
            add(k, 2, b * v)
            v = around(b)
            c = w * v
            add(k, 3, b * v)
            add(k, 4, c * v)
            add(k, 5, c * around(c))
            found += [flow, a, b, c]
        return found

    rims = [[[none] * each for _ in range(scen)] for _ in range(2)]
    lefts = strip(far_l, (0, width - STRIP, width - 2 * STRIP, width - 3 * STRIP, width - 7 * STRIP),
                  0, STRIP, on_left, 0, rims[0])
    rights = strip(far_r, (STRIP, 0, width - STRIP, width - 2 * STRIP, width - 6 * STRIP),
                   STRIP, 2 * STRIP, on_right, STRIP, rims[1])
    ends = [(0, 2 * HALO), (ext - 2 * HALO, 2 * HALO)]
    for i, (left, right) in enumerate(zip(lefts, rights)):
        for start, count in ends:
            q = lane[:count] % SLOT
            east = pltpu.roll(right[start:start + count], width - 2, 1)
            edges[i, pl.ds(start, count)] = jnp.where(q == STRIP - 1, left[start:start + count], east)
        if i % 4 != 1 and i > 0:
            faces[i] = jnp.where(lane % SLOT < STRIP, right, left)
    full = [[none] * each for _ in range(scen)]
    full_rows = (HALO, HALO + length)

    def mend(ref, level):
        for start in (2 * HALO, length - HALO):
            at, to = pl.ds(start, HALO), pl.ds(HALO + start, HALO)
            for k in range(scen):
                for layer in range(layers):
                    face = faces[1 + 4 * k + level, at]
                    ref[k, layer + 1, to] = patched(ref[k, layer + 1, to], face, layer)

    begin(full, ends, *full_rows, True)
    mend(u0, 1)
    advance(full, u0, u1, 1, ends, *full_rows, True)
    mend(u1, 2)
    advance(full, u1, u2, 2, ends, *full_rows, True)
    mend(u2, 3)
    advance(full, u2, None, 3, ends, *full_rows, True)
    line = lax.broadcasted_iota(jnp.int32, (HALO, width), 1)
    middle = (line >= STRIP) & (line < width - STRIP)
    moments = []
    for k in range(scen):
        for i in range(each):
            value = full[k][i] + jnp.where(middle, core[k][i], 0.0)
            used = (line < SLOT * layers) & (line % SLOT >= STRIP) & (line % SLOT < 2 * STRIP)
            value = value + jnp.where(used, rims[0][k][i], 0.0)
            used = (line < SLOT * layers) & (line % SLOT < STRIP)
            moments.append(value + jnp.where(used, rims[1][k][i], 0.0))
    flat = jnp.zeros((1, width), jnp.float32)
    line = lax.broadcasted_iota(jnp.int32, (1, width), 1)
    for i, value in enumerate(moments):
        total = jnp.sum(jnp.sum(value, axis=0, keepdims=True), axis=1, keepdims=True)
        flat = jnp.where(line == i, total, flat)
    row[...] = flat
    rows[n - 1] = flat
    while len(heard) < len(reaches):
        know()

    def spread(i, carry):
        k = me + i
        pltpu.make_async_remote_copy(
            src_ref=row, dst_ref=rows.at[i - 1], send_sem=row_send, recv_sem=row_recv,
            device_id=jnp.where(k < n, k, k - n),
            device_id_type=pl.DeviceIdType.LOGICAL).start()
        return carry

    lax.fori_loop(1, n, spread, 0)
    for dx, dy, copy in copies:
        @pl.when(has[dx, dy])
        def _(copy=copy):
            copy.wait_send()
    def unscale(start):
        at = pl.ds(HALO + start, PIECE)
        for layer in range(layers):
            if layer % 2 == 0:
                back = lookup(vm[layer // 2, at], TIER_INV)
            else:
                back = lookup(vc[layer // 2, at], CHANNEL_INV)
            for k in range(scen):
                for level, (ref, scaled) in enumerate(((u0, f0), (u1, f1), (u2, f2))):
                    value = ref[k, layer + 1, pl.ds(2 * HALO + start, PIECE)]
                    value = patched(value, faces[2 + 4 * k + level, at], layer)
                    scaled[k, layer, pl.ds(start, PIECE)] = back * value

    in_pieces(unscale)
    arrived = rows.at[pl.ds(0, n - 1)]
    pltpu.make_async_copy(arrived, arrived, row_recv).wait()
    sums[...] = jnp.sum(rows[...], axis=0)
    pltpu.make_async_copy(arrived, arrived, row_send).wait()


def combine(sums, vp, f0, f1, f2, out, result, sem):
    scen, layers, length, width = result.shape
    line = lax.broadcasted_iota(jnp.int32, (1, width), 1)
    each = 2 * ITERS
    total = [jnp.sum(jnp.where(line == i, sums[...], 0.0), axis=1, keepdims=True)
             for i in range(scen * each)]
    for k in range(scen):
        c0, c1, c2 = coefficients(total[k * each:(k + 1) * each])
        for layer in range(layers):
            for offset in range(0, length, PIECE):
                at = pl.ds(offset, min(PIECE, length - offset))
                change = c0 * f0[k, layer, at] + c1 * f1[k, layer, at] + c2 * f2[k, layer, at]
                before = vp[k, layer, pl.ds(HALO + offset, min(PIECE, length - offset))]
                result[k, layer, at] = before + change
            pltpu.make_async_copy(result.at[k, layer], out.at[k, layer], sem).start()
    pltpu.make_async_copy(result, out, sem).wait()


def per_device(nx, ny, previous, dissipated, material, coolant):
    scen, layers, length, width = previous.shape
    tiers = material.shape[0]
    ext = length + 2 * HALO
    f32 = jnp.float32
    field = pltpu.VMEM((scen, layers + 2, ext + 3 * HALO, width), f32)
    strip = pltpu.VMEM((ext, width), f32)
    letter = pltpu.VMEM((length, width), f32)
    own = pltpu.VMEM(previous.shape, f32)
    matrix = pltpu.VMEM((2 * width, width), jnp.bfloat16)
    shared = pl.pallas_call(
        functools.partial(kernel, nx, ny),
        out_shape=(pltpu.VMEM((1, width), f32), pltpu.VMEM((scen, layers, ext, width), f32), own, own, own),
        in_specs=[pl.BlockSpec(memory_space=pl.ANY)] * 4,
        out_specs=[pl.BlockSpec(memory_space=pltpu.VMEM)] * 5,
        scratch_shapes=[
            pltpu.VMEM((scen, tiers, ext, width), f32),
            pltpu.VMEM((tiers, ext, width), jnp.int32),
            pltpu.VMEM((layers - tiers, ext, width), jnp.int32),
            pltpu.VMEM((2 * scen + 1, ext, width), f32),
            letter, letter, strip, strip,
            pltpu.VMEM((4 * scen + 1, ext, width), f32),
            pltpu.VMEM((4 * scen + 1, ext, width), f32),
            pltpu.VMEM((layers + 2, ext + 3 * HALO, width), f32),
            pltpu.VMEM((layers, ext, width), f32),
            pltpu.VMEM((layers, ext, width), f32),
            pltpu.VMEM((layers, ext, width), f32),
            field, field, field, field,
            pltpu.VMEM((1, width), f32),
            pltpu.VMEM((nx * ny, 1, width), f32),
            matrix, matrix, matrix,
            pltpu.SemaphoreType.REGULAR((max(nx, ny).bit_length(),)),
            pltpu.SemaphoreType.DMA((4,)),
            pltpu.SemaphoreType.DMA((16,)),
            pltpu.SemaphoreType.DMA((16,)),
            pltpu.SemaphoreType.DMA,
            pltpu.SemaphoreType.DMA,
        ],
        compiler_params=pltpu.CompilerParams(
            collective_id=0, has_side_effects=True, vmem_limit_bytes=48 * 1024 * 1024),
    )(*(pltpu.with_memory_space_constraint(part, pltpu.HBM)
        for part in (previous, dissipated, material, coolant)))
    shared = [pltpu.with_memory_space_constraint(part, pltpu.VMEM) for part in shared]
    return pl.pallas_call(
        combine,
        out_shape=jax.ShapeDtypeStruct(previous.shape, f32),
        in_specs=[pl.BlockSpec(memory_space=pltpu.VMEM)] * 5,
        out_specs=pl.BlockSpec(memory_space=pl.ANY),
        scratch_shapes=[own, pltpu.SemaphoreType.DMA],
        compiler_params=pltpu.CompilerParams(vmem_limit_bytes=16 * 1024 * 1024),
    )(*shared)


def solution(mesh):
    return jax.shard_map(
        functools.partial(per_device, mesh.shape["gx"], mesh.shape["gy"]),
        mesh=mesh,
        in_specs=(
            P(None, None, "gx", "gy"),
            P(None, None, "gx", "gy"),
            P(None, "gx", "gy"),
            P(None, "gx", "gy"),
        ),
        out_specs=P(None, None, "gx", "gy"),
        check_vma=False,
    )
```

```python
import functools
import math

import jax
import jax.numpy as jnp
from jax import lax
from jax.experimental import pallas as pl
from jax.experimental.pallas import tpu as pltpu
from jax.sharding import PartitionSpec as P

ITERS = 3
TIER_K = (1.0, 0.3, 0.12, 2.5)
CHANNEL_K = (1.0, 0.3, 0.25, 0.2)
CHANNEL_SINK = (0.0, 0.15, 0.45, 1.2)
TIER_HEAT = 0.05
CHANNEL_HEAT = 0.2
VERTICAL = 4.0

HALO = 8
STRIP = 4
PIECE = 32
SPAN = 48
SLOT = 4 * STRIP
MESH = pl.DeviceIdType.MESH

TIER_ROOT = tuple(math.sqrt(v) for v in TIER_K)
CHANNEL_ROOT = tuple(math.sqrt(v) for v in CHANNEL_K)
TIER_INV = tuple(1.0 / math.sqrt(v) for v in TIER_K)
CHANNEL_INV = tuple(1.0 / math.sqrt(v) for v in CHANNEL_K)


def lookup(codes, table):
    total = jnp.zeros(codes.shape, jnp.float32)
    for index, value in enumerate(table):
        total = jnp.where(codes == index, jnp.float32(value), total)
    return total


def coefficients(nu):
    def inner(a, b):
        total = None
        for i, x in enumerate(a):
            for j, y in enumerate(b):
                term = x * y * nu[i + j]
                total = term if total is None else total + term
        return total

    zero = nu[0] * 0.0
    rho = [zero + 1.0]
    pi = [zero + 1.0]
    norm = nu[0]
    result = [zero] * ITERS
    for iteration in range(ITERS):
        image = [a - b for a, b in zip(pi + [zero], [zero] + pi)]
        step = norm / inner(pi, image)
        for i, a in enumerate(pi):
            result[i] = result[i] + step * a
        if iteration + 1 < ITERS:
            rho = [a - step * b for a, b in zip(rho + [zero], image)]
            following = inner(rho, rho)
            growth = following / norm
            pi = [a + growth * b for a, b in zip(rho, pi + [zero])]
            norm = following
    return result


def kernel(nx, ny, prev, diss, mat, cool, sums, vp, f0, f1, f2, vq, vm, vc, near, own_l, own_r, far_l, far_r,
           edges, faces, slabs, root, weight, capac, slope, up, u0, u1, u2, row, rows,
           along, on_left, on_right, known, load_sem, send_sem, recv_sem, row_send, row_recv):
    scen, layers, length, width = prev.shape
    tiers = mat.shape[0]
    n = nx * ny
    ext = length + 2 * HALO
    x, y = lax.axis_index("gx"), lax.axis_index("gy")
    me = x * ny + y
    barrier = pltpu.get_barrier_semaphore()

    def around_me(reach):
        found = []
        for dx in (-reach, 0, reach):
            for dy in (-reach, 0, reach):
                if (dx or dy) and abs(dx) < nx and abs(dy) < ny:
                    inside_x = jnp.logical_and(x + dx >= 0, x + dx < nx)
                    inside_y = jnp.logical_and(y + dy >= 0, y + dy < ny)
                    found.append((dx, dy, jnp.logical_and(inside_x, inside_y)))
        return found

    def greet(sem, reach):
        for dx, dy, there in around_me(reach):
            @pl.when(there)
            def _(dx=dx, dy=dy):
                pl.semaphore_signal(sem, inc=1, device_id=(x + dx, y + dy), device_id_type=MESH)

    def hear(sem, reach):
        pl.semaphore_wait(sem, sum(there.astype(jnp.int32) for _, _, there in around_me(reach)))

    reaches = [1]
    while 2 * reaches[-1] < max(nx, ny) - 1:
        reaches.append(2 * reaches[-1])
    heard = []

    def know():
        if len(heard) < len(reaches):
            hear(known.at[len(heard)], reaches[len(heard)])
            heard.append(True)
            if len(heard) < len(reaches):
                greet(known.at[len(heard)], reaches[len(heard)])

    inside = pl.ds(HALO, length)
    loads = [
        pltpu.make_async_copy(prev, vp.at[:, :, inside], load_sem.at[0]),
        pltpu.make_async_copy(diss, vq.at[:, :, inside], load_sem.at[1]),
        pltpu.make_async_copy(mat, vm.at[:, inside], load_sem.at[2]),
        pltpu.make_async_copy(cool, vc.at[:, inside], load_sem.at[3]),
    ]
    for copy in reversed(loads):
        copy.start()
    greet(barrier, 1)

    has = {(-1, 0): x > 0, (1, 0): x < nx - 1, (0, -1): y > 0, (0, 1): y < ny - 1}
    for dx in (-1, 1):
        for dy in (-1, 1):
            has[dx, dy] = jnp.logical_and(has[dx, 0], has[0, dy])
    top, bottom = pl.ds(0, HALO), pl.ds(HALO + length, HALO)
    first, last = pl.ds(HALO, HALO), pl.ds(length, HALO)

    def fill(ref):
        ref[...] = jnp.full(ref.shape, -1, ref.dtype)

    for dx, where in ((-1, top), (1, bottom)):
        @pl.when(jnp.logical_not(has[dx, 0]))
        def _(where=where):
            for ref in (vp, vq):
                fill(ref.at[:, :, where])
            for ref in (vm, vc):
                fill(ref.at[:, where])
            fill(near.at[:, where])
    for dy, ref in ((-1, far_l), (1, far_r)):
        @pl.when(jnp.logical_not(has[0, dy]))
        def _(ref=ref):
            fill(ref.at[inside])
        for dx, where in ((-1, top), (1, bottom)):
            @pl.when(jnp.logical_not(has[dx, dy]))
            def _(ref=ref, where=where):
                fill(ref.at[where])

    source = lax.broadcasted_iota(jnp.int32, (width, width), 0)
    target = lax.broadcasted_iota(jnp.int32, (width, width), 1)
    beside = jnp.abs(target - source) == 1
    matrices = [(along, jnp.where(beside, 1.0, 0.0))]
    for ref, shift in ((on_left, 0), (on_right, STRIP)):
        begins, ends = (source + shift) % width, (target + shift) % width
        apart, spot = ends - begins, ends // SLOT
        valid = (spot < layers) & (ends % SLOT < 3 * STRIP) & (begins % SLOT < 3 * STRIP)
        beside = ((apart == 1) | (apart == -1)) & (begins // SLOT == spot)
        stacked = (apart == SLOT) & (spot > 0) | (apart == -SLOT) & (spot < layers - 1)
        weights = jnp.where(stacked, VERTICAL, jnp.where(beside, 1.0, 0.0))
        matrices.append((ref, jnp.where(valid, weights, 0.0)))
    for ref, weights in matrices:
        for i in range(2):
            ref[pl.ds(i * width, width)] = weights.astype(jnp.bfloat16)
    blank = jnp.zeros((ext + 3 * HALO, width), jnp.float32)
    for pad in (0, layers + 1):
        root[pad] = blank
        for k in range(scen):
            for ref in (up, u0, u1, u2):
                ref[k, pad] = blank
    for i in range(slabs.shape[0]):
        for at in (pl.ds(0, HALO), pl.ds(HALO + ext, HALO)):
            slabs[i, at] = blank[:HALO]
    for at in (pl.ds(HALO, HALO), pl.ds(2 * HALO + length, HALO)):
        for layer in range(layers):
            root[layer + 1, at] = blank[:HALO]
            for k in range(scen):
                for ref in (up, u0, u1, u2):
                    ref[k, layer + 1, at] = blank[:HALO]

    def pack(places):
        lane = lax.broadcasted_iota(jnp.int32, (length, width), 1)
        packed = opening = None
        for layer, ref, index in places:
            plane = ref[index + (inside,)].astype(jnp.float32)
            turned = pltpu.roll(plane, SLOT * layer + STRIP, 1)
            if packed is None:
                packed = opening = turned
            else:
                packed = jnp.where(lane >= SLOT * layer - STRIP, turned, packed)
        return jnp.where(lane >= width - STRIP, opening, packed)

    def letter(shifts):
        lane = lax.broadcasted_iota(jnp.int32, (length, width), 1)
        q = lane % SLOT
        parts = []
        for i, shift in enumerate(shifts):
            part = near[i, inside]
            parts.append(pltpu.roll(part, shift, 1) if shift else part)
        power = jnp.where(lane // SLOT % 2 == 0, parts[3], parts[4])
        rest = jnp.where(q < 3 * STRIP, parts[2], power)
        return jnp.where(q < STRIP, parts[0], jnp.where(q < 2 * STRIP, parts[1], rest))

    for copy in loads[1:]:
        copy.wait()
    near[scen, inside] = pack([(layer, vc if layer % 2 else vm, (layer // 2,)) for layer in range(layers)])
    for k in range(scen):
        near[scen + 1 + k, inside] = pack([(2 * t, vq, (k, t)) for t in range(tiers)])
    loads[0].wait()
    for k in range(scen):
        near[k, inside] = pack([(layer, vp, (k, layer)) for layer in range(layers)])
    own_l[...] = letter((width - STRIP, 0, STRIP, 2 * STRIP, 6 * STRIP))
    own_r[...] = letter((0, STRIP, 2 * STRIP, 3 * STRIP, 7 * STRIP))

    hear(barrier, 1)
    greet(known.at[0], 1)

    sends = []
    for dx, source, target in ((-1, first, bottom), (1, last, top)):
        for ref in (vp, vq):
            sends.append((dx, 0, ref.at[:, :, source], ref.at[:, :, target]))
        for ref in (vm, vc):
            sends.append((dx, 0, ref.at[:, source], ref.at[:, target]))
        sends.append((dx, 0, near.at[:, source], near.at[:, target]))
        begins = pl.ds(0 if dx < 0 else length - HALO, HALO)
        sends.append((dx, -1, own_l.at[begins], far_r.at[target]))
        sends.append((dx, 1, own_r.at[begins], far_l.at[target]))
    sends.append((0, -1, own_l, far_r.at[inside]))
    sends.append((0, 1, own_r, far_l.at[inside]))
    copies = []
    for i, (dx, dy, source, target) in enumerate(sends):
        copy = pltpu.make_async_remote_copy(
            src_ref=source, dst_ref=target, send_sem=send_sem.at[i], recv_sem=recv_sem.at[i],
            device_id=(x + dx, y + dy), device_id_type=MESH)
        copies.append((dx, dy, copy))
    order = sorted(copies, key=lambda c: 0 if c[0] and c[1] else 1 if c[0] == 0 else 2)
    for dx, dy, copy in order:
        @pl.when(has[dx, dy])
        def _(copy=copy):
            copy.start()
    def prepare(at, to):
        count = at.size
        for layer in range(layers):
            if layer % 2 == 0:
                s = lookup(vm[layer // 2, at], TIER_ROOT)
                total = jnp.full((count, width), TIER_HEAT, jnp.float32)
            else:
                codes = vc[layer // 2, at]
                s = lookup(codes, CHANNEL_ROOT)
                total = CHANNEL_HEAT + lookup(codes, CHANNEL_SINK)
            root[layer + 1, to] = s
            capac[layer, at] = total
            for k in range(scen):
                up[k, layer + 1, to] = s * vp[k, layer, at]

    def in_pieces(step):
        def one(i, carry):
            step(pl.multiple_of(i * PIECE, PIECE))
            return carry

        lax.fori_loop(0, length // PIECE, one, 0)

    in_pieces(lambda start: prepare(pl.ds(HALO + start, PIECE), pl.ds(2 * HALO + start, PIECE)))

    def shifted(value, matrix):
        high = value.astype(jnp.bfloat16)
        low = (value - high.astype(jnp.float32)).astype(jnp.bfloat16)
        return jnp.dot(jnp.concatenate([high, low], axis=1), matrix[...],
                       preferred_element_type=jnp.float32)

    def spans(start, count):
        pieces = []
        while count > 0:
            piece = min(count, SPAN)
            pieces.append((start, piece))
            start, count = start + piece, count - piece
        return pieces

    def column(ref, at, places):
        centres = []
        for layer in range(layers):
            for start, count in places:
                centres.append(ref[at + (layer + 1, pl.ds(HALO + start, count))])
        lateral = shifted(jnp.concatenate(centres, axis=0), along)
        offset = 0
        for i, centre in enumerate(centres):
            layer, (start, count) = i // len(places), places[i % len(places)]
            around = lateral[offset:offset + count]
            offset += count
            around = around + ref[at + (layer + 1, pl.ds(HALO + start - 1, count))]
            around = around + ref[at + (layer + 1, pl.ds(HALO + start + 1, count))]
            stacked = [centres[j] for j in (i - len(places), i + len(places)) if 0 <= j < len(centres)]
            if stacked:
                around = around + VERTICAL * sum(stacked[1:], stacked[0])
            yield layer, start, count, centre, around

    def margins(edge, layer):
        lane = lax.broadcasted_iota(jnp.int32, edge.shape, 1)
        ends = (lane == 0) | (lane == width - 1)
        shift = (width - SLOT * layer - (STRIP - 1)) % width
        return jnp.where(ends, pltpu.roll(edge, shift, 1), 0.0)

    def patched(value, face, layer):
        lane = lax.broadcasted_iota(jnp.int32, face.shape, 1)
        ends = (lane < STRIP) | (lane >= width - STRIP)
        return jnp.where(ends, pltpu.roll(face, width - SLOT * layer - STRIP, 1), value)

    def gather(total, value, start, low, high):
        first, last = max(low - start, 0), min(high - start, value.shape[0])
        if last <= first:
            return total
        return total + jnp.sum(value[first:last].reshape(-1, HALO, width), axis=0)

    none = jnp.zeros((HALO, width), jnp.float32)
    each = 2 * ITERS

    def begin(sums, places, low, high, edged):
        for layer, start, count, _, around in column(root, (), places):
            at = pl.ds(start, count)
            s = root[layer + 1, pl.ds(HALO + start, count)]
            if edged:
                around = around + margins(edges[0, at], layer)
            total = capac[layer, at] + s * around
            inverse = 1.0 / total
            weight[layer, at] = s * s * inverse
            slope[layer, at] = total
        for k in range(scen):
            for layer, start, count, _, around in column(up, (k,), places):
                at = pl.ds(start, count)
                if edged:
                    around = around + margins(edges[1 + 4 * k, at], layer)
                s = root[layer + 1, pl.ds(HALO + start, count)]
                total = slope[layer, at]
                heat = TIER_HEAT if layer % 2 == 0 else CHANNEL_HEAT
                residual = (heat - total) * vp[k, layer, at] + s * around
                if layer % 2 == 0:
                    residual = residual + vq[k, layer // 2, at]
                scaled = residual / total
                u0[k, layer + 1, pl.ds(HALO + start, count)] = s * scaled
                sums[k][0] = gather(sums[k][0], residual * scaled, start, low, high)

    def advance(sums, source, target, level, places, low, high, edged):
        for k in range(scen):
            for layer, start, count, centre, around in column(source, (k,), places):
                at = pl.ds(start, count)
                if edged:
                    around = around + margins(edges[1 + 4 * k + level, at], layer)
                i = 2 * level - 1
                sums[k][i] = gather(sums[k][i], centre * around, start, low, high)
                if target is not None:
                    moved = weight[layer, at] * around
                    target[k, layer + 1, pl.ds(HALO + start, count)] = moved
                    sums[k][i + 1] = gather(sums[k][i + 1], moved * around, start, low, high)

    core = [[none] * each for _ in range(scen)]
    core_rows = (2 * HALO, length)
    whole = spans(HALO, length)
    for place in whole:
        begin(core, [place], *core_rows, False)
    know()
    for place in whole:
        advance(core, u0, u1, 1, [place], *core_rows, False)
    for place in whole:
        advance(core, u1, u2, 2, [place], *core_rows, False)
    for place in spans(2 * HALO, length - 2 * HALO):
        advance(core, u2, None, 3, [place], *core_rows, False)

    know()
    for dx, dy, copy in copies:
        @pl.when(has[-dx, -dy])
        def _(copy=copy):
            copy.wait_recv()

    prepare(pl.ds(0, HALO), pl.ds(HALO, HALO))
    prepare(pl.ds(HALO + length, HALO), pl.ds(2 * HALO + length, HALO))

    shape = (ext, width)
    lane = lax.broadcasted_iota(jnp.int32, shape, 1)

    taken = []

    def arounds(values):
        joined = jnp.concatenate(values, axis=0)
        high = joined.astype(jnp.bfloat16)
        below = (joined - high.astype(jnp.float32)).astype(jnp.bfloat16)
        joined = jnp.concatenate([high, below], axis=1)
        half = joined.shape[0] // 2
        moved = [jnp.dot(joined[:half], on_left[...], preferred_element_type=jnp.float32),
                 jnp.dot(joined[half:], on_right[...], preferred_element_type=jnp.float32)]
        results = []
        for i, value in enumerate(values):
            slab = slabs.at[len(taken)]
            taken.append(True)
            slab[pl.ds(HALO, ext)] = value
            side, at = divmod(i * ext, half)
            result = moved[side][at:at + ext] + slab[pl.ds(HALO - 1, ext)]
            results.append(result + slab[pl.ds(HALO + 1, ext)])
        return results

    q = lane % SLOT
    tiers_of, heats, fields, powers, roots, totals = [], [], [], [], [], []
    for far, shifts, low, shift in (
            (far_l, (0, width - STRIP, width - 2 * STRIP, width - 3 * STRIP, width - 7 * STRIP), 0, 0),
            (far_r, (STRIP, 0, width - STRIP, width - 2 * STRIP, width - 6 * STRIP), STRIP, STRIP)):
        theirs = (q >= low) & (q < low + STRIP)
        turned = (lane + shift) % width
        valid = (turned // SLOT < layers) & (turned % SLOT < 3 * STRIP)
        tier = turned // SLOT % 2 == 0
        message = far[...]
        parts = []
        for i, turn in enumerate(shifts):
            other = pltpu.roll(message, turn, 1) if turn else message
            parts.append(jnp.where(theirs, other, near[i]))
        codes = jnp.where(valid, parts[scen], -1.0)
        heat = jnp.where(tier, TIER_HEAT, CHANNEL_HEAT)
        s, total = jnp.zeros(shape, jnp.float32), heat
        for code, values in enumerate(zip(TIER_ROOT, CHANNEL_ROOT, CHANNEL_SINK)):
            found = codes == code
            s = jnp.where(found, jnp.where(tier, values[0], values[1]), s)
            if values[2]:
                total = jnp.where(found, heat + jnp.where(tier, 0.0, values[2]), total)
        heats.append(heat)
        fields.append(parts[:scen])
        powers.append([jnp.where(tier & valid, part, 0.0) for part in parts[scen + 1:]])
        roots.append(s)
        totals.append(total)
    rims = [[[none] * each for _ in range(scen)] for _ in range(2)]

    def add(side, k, i, value):
        kept = value[2 * HALO:length].reshape(-1, HALO, width)
        rims[side][k][i] = rims[side][k][i] + jnp.sum(kept, axis=0)

    pairs = [(side, k) for side in range(2) for k in range(scen)]
    flows = [[roots[side] * field for field in fields[side]] for side in range(2)]
    spread = arounds([roots[0], *flows[0], roots[1], *flows[1]])
    found = [[s] for s in roots]
    currents, weights = [], []
    for side in range(2):
        s = roots[side]
        total = totals[side] + s * spread[side * (scen + 1)]
        inverse = 1.0 / total
        weights.append(s * s * inverse)
        for k in range(scen):
            residual = (heats[side] - total) * fields[side][k] + powers[side][k]
            residual = residual + s * spread[side * (scen + 1) + 1 + k]
            scaled = residual * inverse
            add(side, k, 0, residual * scaled)
            currents.append(s * scaled)
    chains = [[flows[side][k], current] for (side, k), current in zip(pairs, currents)]
    for level in range(1, ITERS + 1):
        spread = arounds(currents)
        for i, (side, k) in enumerate(pairs):
            add(side, k, 2 * level - 1, currents[i] * spread[i])
            if level < ITERS:
                moved = weights[side] * spread[i]
                add(side, k, 2 * level, moved * spread[i])
                currents[i] = moved
                chains[i].append(moved)
    lefts = [roots[0]] + [value for i in range(scen) for value in chains[i]]
    rights = [roots[1]] + [value for i in range(scen) for value in chains[scen + i]]
    ends = [(0, 2 * HALO), (ext - 2 * HALO, 2 * HALO)]
    for i, (left, right) in enumerate(zip(lefts, rights)):
        for start, count in ends:
            q = lane[:count] % SLOT
            east = pltpu.roll(right[start:start + count], width - 2, 1)
            edges[i, pl.ds(start, count)] = jnp.where(q == STRIP - 1, left[start:start + count], east)
        if i % 4 != 1 and i > 0:
            faces[i] = jnp.where(lane % SLOT < STRIP, right, left)
    full = [[none] * each for _ in range(scen)]
    full_rows = (HALO, HALO + length)

    def mend(ref, level):
        for start in (2 * HALO, length - HALO):
            at, to = pl.ds(start, HALO), pl.ds(HALO + start, HALO)
            for k in range(scen):
                for layer in range(layers):
                    face = faces[1 + 4 * k + level, at]
                    ref[k, layer + 1, to] = patched(ref[k, layer + 1, to], face, layer)

    begin(full, ends, *full_rows, True)
    mend(u0, 1)
    advance(full, u0, u1, 1, ends, *full_rows, True)
    mend(u1, 2)
    advance(full, u1, u2, 2, ends, *full_rows, True)
    mend(u2, 3)
    advance(full, u2, None, 3, ends, *full_rows, True)
    line = lax.broadcasted_iota(jnp.int32, (HALO, width), 1)
    middle = (line >= STRIP) & (line < width - STRIP)
    moments = []
    for k in range(scen):
        for i in range(each):
            value = full[k][i] + jnp.where(middle, core[k][i], 0.0)
            used = (line < SLOT * layers) & (line % SLOT >= STRIP) & (line % SLOT < 2 * STRIP)
            value = value + jnp.where(used, rims[0][k][i], 0.0)
            used = (line < SLOT * layers) & (line % SLOT < STRIP)
            moments.append(value + jnp.where(used, rims[1][k][i], 0.0))
    flat = jnp.zeros((1, width), jnp.float32)
    line = lax.broadcasted_iota(jnp.int32, (1, width), 1)
    for i, value in enumerate(moments):
        total = jnp.sum(jnp.sum(value, axis=0, keepdims=True), axis=1, keepdims=True)
        flat = jnp.where(line == i, total, flat)
    row[...] = flat
    rows[n - 1] = flat
    while len(heard) < len(reaches):
        know()

    def spread(i, carry):
        k = me + i
        pltpu.make_async_remote_copy(
            src_ref=row, dst_ref=rows.at[i - 1], send_sem=row_send, recv_sem=row_recv,
            device_id=jnp.where(k < n, k, k - n),
            device_id_type=pl.DeviceIdType.LOGICAL).start()
        return carry

    lax.fori_loop(1, n, spread, 0)
    for dx, dy, copy in copies:
        @pl.when(has[dx, dy])
        def _(copy=copy):
            copy.wait_send()
    def unscale(start):
        at = pl.ds(HALO + start, PIECE)
        for layer in range(layers):
            if layer % 2 == 0:
                back = lookup(vm[layer // 2, at], TIER_INV)
            else:
                back = lookup(vc[layer // 2, at], CHANNEL_INV)
            for k in range(scen):
                for level, (ref, scaled) in enumerate(((u0, f0), (u1, f1), (u2, f2))):
                    value = ref[k, layer + 1, pl.ds(2 * HALO + start, PIECE)]
                    value = patched(value, faces[2 + 4 * k + level, at], layer)
                    scaled[k, layer, pl.ds(start, PIECE)] = back * value

    in_pieces(unscale)
    arrived = rows.at[pl.ds(0, n - 1)]
    pltpu.make_async_copy(arrived, arrived, row_recv).wait()
    sums[...] = jnp.sum(rows[...], axis=0)
    pltpu.make_async_copy(arrived, arrived, row_send).wait()


def combine(sums, vp, f0, f1, f2, out, result, sem):
    scen, layers, length, width = result.shape
    line = lax.broadcasted_iota(jnp.int32, (1, width), 1)
    each = 2 * ITERS
    total = [jnp.sum(jnp.where(line == i, sums[...], 0.0), axis=1, keepdims=True)
             for i in range(scen * each)]
    for k in range(scen):
        c0, c1, c2 = coefficients(total[k * each:(k + 1) * each])
        for layer in range(layers):
            for offset in range(0, length, PIECE):
                at = pl.ds(offset, min(PIECE, length - offset))
                change = c0 * f0[k, layer, at] + c1 * f1[k, layer, at] + c2 * f2[k, layer, at]
                before = vp[k, layer, pl.ds(HALO + offset, min(PIECE, length - offset))]
                result[k, layer, at] = before + change
            pltpu.make_async_copy(result.at[k, layer], out.at[k, layer], sem).start()
    pltpu.make_async_copy(result, out, sem).wait()


def per_device(nx, ny, previous, dissipated, material, coolant):
    scen, layers, length, width = previous.shape
    tiers = material.shape[0]
    ext = length + 2 * HALO
    f32 = jnp.float32
    field = pltpu.VMEM((scen, layers + 2, ext + 3 * HALO, width), f32)
    strip = pltpu.VMEM((ext, width), f32)
    letter = pltpu.VMEM((length, width), f32)
    own = pltpu.VMEM(previous.shape, f32)
    matrix = pltpu.VMEM((2 * width, width), jnp.bfloat16)
    shared = pl.pallas_call(
        functools.partial(kernel, nx, ny),
        out_shape=(pltpu.VMEM((1, width), f32), pltpu.VMEM((scen, layers, ext, width), f32), own, own, own),
        in_specs=[pl.BlockSpec(memory_space=pl.ANY)] * 4,
        out_specs=[pl.BlockSpec(memory_space=pltpu.VMEM)] * 5,
        scratch_shapes=[
            pltpu.VMEM((scen, tiers, ext, width), f32),
            pltpu.VMEM((tiers, ext, width), jnp.int32),
            pltpu.VMEM((layers - tiers, ext, width), jnp.int32),
            pltpu.VMEM((2 * scen + 1, ext, width), f32),
            letter, letter, strip, strip,
            pltpu.VMEM((4 * scen + 1, ext, width), f32),
            pltpu.VMEM((4 * scen + 1, ext, width), f32),
            pltpu.VMEM((8 * scen + 2, ext + 2 * HALO, width), f32),
            pltpu.VMEM((layers + 2, ext + 3 * HALO, width), f32),
            pltpu.VMEM((layers, ext, width), f32),
            pltpu.VMEM((layers, ext, width), f32),
            pltpu.VMEM((layers, ext, width), f32),
            field, field, field, field,
            pltpu.VMEM((1, width), f32),
            pltpu.VMEM((nx * ny, 1, width), f32),
            matrix, matrix, matrix,
            pltpu.SemaphoreType.REGULAR((max(nx, ny).bit_length(),)),
            pltpu.SemaphoreType.DMA((4,)),
            pltpu.SemaphoreType.DMA((16,)),
            pltpu.SemaphoreType.DMA((16,)),
            pltpu.SemaphoreType.DMA,
            pltpu.SemaphoreType.DMA,
        ],
        compiler_params=pltpu.CompilerParams(
            collective_id=0, has_side_effects=True, vmem_limit_bytes=48 * 1024 * 1024),
    )(*(pltpu.with_memory_space_constraint(part, pltpu.HBM)
        for part in (previous, dissipated, material, coolant)))
    shared = [pltpu.with_memory_space_constraint(part, pltpu.VMEM) for part in shared]
    return pl.pallas_call(
        combine,
        out_shape=jax.ShapeDtypeStruct(previous.shape, f32),
        in_specs=[pl.BlockSpec(memory_space=pltpu.VMEM)] * 5,
        out_specs=pl.BlockSpec(memory_space=pl.ANY),
        scratch_shapes=[own, pltpu.SemaphoreType.DMA],
        compiler_params=pltpu.CompilerParams(vmem_limit_bytes=16 * 1024 * 1024),
    )(*shared)


def solution(mesh):
    return jax.shard_map(
        functools.partial(per_device, mesh.shape["gx"], mesh.shape["gy"]),
        mesh=mesh,
        in_specs=(
            P(None, None, "gx", "gy"),
            P(None, None, "gx", "gy"),
            P(None, "gx", "gy"),
            P(None, "gx", "gy"),
        ),
        out_specs=P(None, None, "gx", "gy"),
        check_vma=False,
    )
```

```python
import functools
import math

import jax
import jax.numpy as jnp
from jax import lax
from jax.experimental import pallas as pl
from jax.experimental.pallas import tpu as pltpu
from jax.sharding import PartitionSpec as P

ITERS = 3
TIER_K = (1.0, 0.3, 0.12, 2.5)
CHANNEL_K = (1.0, 0.3, 0.25, 0.2)
CHANNEL_SINK = (0.0, 0.15, 0.45, 1.2)
TIER_HEAT = 0.05
CHANNEL_HEAT = 0.2
VERTICAL = 4.0

HALO = 8
STRIP = 4
PIECE = 32
SPAN = 48
SLOT = 4 * STRIP
MESH = pl.DeviceIdType.MESH

TIER_ROOT = tuple(math.sqrt(v) for v in TIER_K)
CHANNEL_ROOT = tuple(math.sqrt(v) for v in CHANNEL_K)
TIER_INV = tuple(1.0 / math.sqrt(v) for v in TIER_K)
CHANNEL_INV = tuple(1.0 / math.sqrt(v) for v in CHANNEL_K)


def lookup(codes, table):
    total = jnp.zeros(codes.shape, jnp.float32)
    for index, value in enumerate(table):
        total = jnp.where(codes == index, jnp.float32(value), total)
    return total


def coefficients(nu):
    def inner(a, b):
        total = None
        for i, x in enumerate(a):
            for j, y in enumerate(b):
                term = x * y * nu[i + j]
                total = term if total is None else total + term
        return total

    zero = nu[0] * 0.0
    rho = [zero + 1.0]
    pi = [zero + 1.0]
    norm = nu[0]
    result = [zero] * ITERS
    for iteration in range(ITERS):
        image = [a - b for a, b in zip(pi + [zero], [zero] + pi)]
        step = norm / inner(pi, image)
        for i, a in enumerate(pi):
            result[i] = result[i] + step * a
        if iteration + 1 < ITERS:
            rho = [a - step * b for a, b in zip(rho + [zero], image)]
            following = inner(rho, rho)
            growth = following / norm
            pi = [a + growth * b for a, b in zip(rho, pi + [zero])]
            norm = following
    return result


def kernel(nx, ny, prev, diss, mat, cool, sums, vp, f0, f1, f2, vq, vm, vc, near, own_l, own_r, far_l, far_r,
           edges, faces, slabs, root, weight, capac, slope, recip, up, u0, u1, u2, row, rows,
           along, on_left, on_right, known, load_sem, send_sem, recv_sem, row_send, row_recv):
    scen, layers, length, width = prev.shape
    tiers = mat.shape[0]
    n = nx * ny
    ext = length + 2 * HALO
    x, y = lax.axis_index("gx"), lax.axis_index("gy")
    me = x * ny + y
    barrier = pltpu.get_barrier_semaphore()

    def around_me(reach):
        found = []
        for dx in (-reach, 0, reach):
            for dy in (-reach, 0, reach):
                if (dx or dy) and abs(dx) < nx and abs(dy) < ny:
                    inside_x = jnp.logical_and(x + dx >= 0, x + dx < nx)
                    inside_y = jnp.logical_and(y + dy >= 0, y + dy < ny)
                    found.append((dx, dy, jnp.logical_and(inside_x, inside_y)))
        return found

    def greet(sem, reach):
        for dx, dy, there in around_me(reach):
            @pl.when(there)
            def _(dx=dx, dy=dy):
                pl.semaphore_signal(sem, inc=1, device_id=(x + dx, y + dy), device_id_type=MESH)

    def hear(sem, reach):
        pl.semaphore_wait(sem, sum(there.astype(jnp.int32) for _, _, there in around_me(reach)))

    reaches = [1]
    while 2 * reaches[-1] < max(nx, ny) - 1:
        reaches.append(2 * reaches[-1])
    heard = []

    def know():
        if len(heard) < len(reaches):
            hear(known.at[len(heard)], reaches[len(heard)])
            heard.append(True)
            if len(heard) < len(reaches):
                greet(known.at[len(heard)], reaches[len(heard)])

    inside = pl.ds(HALO, length)
    loads = [
        pltpu.make_async_copy(prev.at[0], vp.at[0, :, inside], load_sem.at[0]),
        pltpu.make_async_copy(prev.at[1], vp.at[1, :, inside], load_sem.at[1]),
        pltpu.make_async_copy(diss, vq.at[:, :, inside], load_sem.at[2]),
        pltpu.make_async_copy(mat, vm.at[:, inside], load_sem.at[3]),
        pltpu.make_async_copy(cool, vc.at[:, inside], load_sem.at[4]),
    ]
    for copy in loads:
        copy.start()
    greet(barrier, 1)

    has = {(-1, 0): x > 0, (1, 0): x < nx - 1, (0, -1): y > 0, (0, 1): y < ny - 1}
    for dx in (-1, 1):
        for dy in (-1, 1):
            has[dx, dy] = jnp.logical_and(has[dx, 0], has[0, dy])
    top, bottom = pl.ds(0, HALO), pl.ds(HALO + length, HALO)
    first, last = pl.ds(HALO, HALO), pl.ds(length, HALO)

    def fill(ref):
        ref[...] = jnp.full(ref.shape, -1, ref.dtype)

    for dx, where in ((-1, top), (1, bottom)):
        @pl.when(jnp.logical_not(has[dx, 0]))
        def _(where=where):
            for ref in (vp, vq):
                fill(ref.at[:, :, where])
            for ref in (vm, vc):
                fill(ref.at[:, where])
            fill(near.at[:, where])
    for dy, ref in ((-1, far_l), (1, far_r)):
        @pl.when(jnp.logical_not(has[0, dy]))
        def _(ref=ref):
            fill(ref.at[inside])
        for dx, where in ((-1, top), (1, bottom)):
            @pl.when(jnp.logical_not(has[dx, dy]))
            def _(ref=ref, where=where):
                fill(ref.at[where])

    source = lax.broadcasted_iota(jnp.int32, (width, width), 0)
    target = lax.broadcasted_iota(jnp.int32, (width, width), 1)
    beside = jnp.abs(target - source) == 1
    matrices = [(along, jnp.where(beside, 1.0, 0.0))]
    for ref, shift in ((on_left, 0), (on_right, STRIP)):
        begins, ends = (source + shift) % width, (target + shift) % width
        apart, spot = ends - begins, ends // SLOT
        valid = (spot < layers) & (ends % SLOT < 3 * STRIP) & (begins % SLOT < 3 * STRIP)
        beside = ((apart == 1) | (apart == -1)) & (begins // SLOT == spot)
        stacked = (apart == SLOT) & (spot > 0) | (apart == -SLOT) & (spot < layers - 1)
        weights = jnp.where(stacked, VERTICAL, jnp.where(beside, 1.0, 0.0))
        matrices.append((ref, jnp.where(valid, weights, 0.0)))
    for ref, weights in matrices:
        for i in range(2):
            ref[pl.ds(i * width, width)] = weights.astype(jnp.bfloat16)
    blank = jnp.zeros((ext + 3 * HALO, width), jnp.float32)
    for pad in (0, layers + 1):
        root[pad] = blank
        for k in range(scen):
            for ref in (up, u0, u1, u2):
                ref[k, pad] = blank
    for i in range(slabs.shape[0]):
        for at in (pl.ds(0, HALO), pl.ds(HALO + ext, HALO)):
            slabs[i, at] = blank[:HALO]
    for at in (pl.ds(HALO, HALO), pl.ds(2 * HALO + length, HALO)):
        for layer in range(layers):
            root[layer + 1, at] = blank[:HALO]
            for k in range(scen):
                for ref in (up, u0, u1, u2):
                    ref[k, layer + 1, at] = blank[:HALO]

    def pack(places):
        lane = lax.broadcasted_iota(jnp.int32, (length, width), 1)
        packed = opening = None
        for layer, ref, index in places:
            plane = ref[index + (inside,)].astype(jnp.float32)
            turned = pltpu.roll(plane, SLOT * layer + STRIP, 1)
            if packed is None:
                packed = opening = turned
            else:
                packed = jnp.where(lane >= SLOT * layer - STRIP, turned, packed)
        return jnp.where(lane >= width - STRIP, opening, packed)

    def write(part, places):
        lane = lax.broadcasted_iota(jnp.int32, (length, width), 1)
        left = right = opening = None
        for slot, ref, index in places:
            base = SLOT * slot + STRIP * part
            plane = ref[index + (inside,)].astype(jnp.float32)
            turned = pltpu.roll(plane, base, 1) if base else plane
            if left is None:
                left = right = opening = turned
            else:
                left = jnp.where(lane >= base, turned, left)
                right = jnp.where(lane >= base - STRIP, turned, right)
        if part == 0:
            right = jnp.where(lane >= width - STRIP, opening, right)
        if written:
            left = jnp.where(lane % SLOT // STRIP == part, left, own_l[...])
            right = jnp.where((lane + STRIP) % SLOT // STRIP == part, right, own_r[...])
        own_l[...], own_r[...] = left, right
        written.append(part)

    written = []
    for k in range(scen):
        loads[k].wait()
        write(k, [(layer, vp, (k, layer)) for layer in range(layers)])
    loads[2].wait()
    write(scen + 1, [(2 * t + k, vq, (k, t)) for t in range(tiers) for k in range(scen)])
    for copy in loads[3:]:
        copy.wait()
    write(scen, [(layer, vc if layer % 2 else vm, (layer // 2,)) for layer in range(layers)])

    hear(barrier, 1)
    greet(known.at[0], 1)

    sends = []
    for dx, source, target in ((-1, first, bottom), (1, last, top)):
        for ref in (vp, vq):
            sends.append((dx, 0, ref.at[:, :, source], ref.at[:, :, target]))
        for ref in (vm, vc):
            sends.append((dx, 0, ref.at[:, source], ref.at[:, target]))
        begins = pl.ds(0 if dx < 0 else length - HALO, HALO)
        sends.append((dx, -1, own_l.at[begins], far_r.at[target]))
        sends.append((dx, 1, own_r.at[begins], far_l.at[target]))
    sends.append((0, -1, own_l, far_r.at[inside]))
    sends.append((0, 1, own_r, far_l.at[inside]))
    for dx, source, target in ((-1, first, bottom), (1, last, top)):
        sends.append((dx, 0, near.at[:, source], near.at[:, target]))
    copies = []
    for i, (dx, dy, source, target) in enumerate(sends):
        copy = pltpu.make_async_remote_copy(
            src_ref=source, dst_ref=target, send_sem=send_sem.at[i], recv_sem=recv_sem.at[i],
            device_id=(x + dx, y + dy), device_id_type=MESH)
        copies.append((dx, dy, copy))
    order = sorted(copies[:-2], key=lambda c: 0 if c[0] and c[1] else 1 if c[0] == 0 else 2)

    def begin_sends(order):
        for dx, dy, copy in order:
            @pl.when(has[dx, dy])
            def _(copy=copy):
                copy.start()

    begin_sends(order)
    for k in range(scen):
        near[k, inside] = pack([(layer, vp, (k, layer)) for layer in range(layers)])
        near[scen + 1 + k, inside] = pack([(2 * t, vq, (k, t)) for t in range(tiers)])
    near[scen, inside] = pack([(layer, vc if layer % 2 else vm, (layer // 2,)) for layer in range(layers)])
    begin_sends(copies[-2:])

    def prepare(at, to):
        count = at.size
        for layer in range(layers):
            if layer % 2 == 0:
                s = lookup(vm[layer // 2, at], TIER_ROOT)
                total = jnp.full((count, width), TIER_HEAT, jnp.float32)
            else:
                codes = vc[layer // 2, at]
                s = lookup(codes, CHANNEL_ROOT)
                total = CHANNEL_HEAT + lookup(codes, CHANNEL_SINK)
            root[layer + 1, to] = s
            capac[layer, at] = total
            for k in range(scen):
                up[k, layer + 1, to] = s * vp[k, layer, at]

    def in_pieces(step):
        def one(i, carry):
            step(pl.multiple_of(i * PIECE, PIECE))
            return carry

        lax.fori_loop(0, length // PIECE, one, 0)

    in_pieces(lambda start: prepare(pl.ds(HALO + start, PIECE), pl.ds(2 * HALO + start, PIECE)))

    def shifted(value, matrix):
        high = value.astype(jnp.bfloat16)
        low = (value - high.astype(jnp.float32)).astype(jnp.bfloat16)
        return jnp.dot(jnp.concatenate([high, low], axis=1), matrix[...],
                       preferred_element_type=jnp.float32)

    def spans(start, count):
        pieces = []
        while count > 0:
            piece = min(count, SPAN)
            pieces.append((start, piece))
            start, count = start + piece, count - piece
        return pieces

    def columns(refs, places):
        centres = []
        for ref, at in refs:
            for layer in range(layers):
                for start, count in places:
                    centres.append(ref[at + (layer + 1, pl.ds(HALO + start, count))])
        lateral = shifted(jnp.concatenate(centres, axis=0), along)
        many, offset = layers * len(places), 0
        for i, centre in enumerate(centres):
            ref, at = refs[i // many]
            layer, (start, count) = i % many // len(places), places[i % len(places)]
            around = lateral[offset:offset + count]
            offset += count
            around = around + ref[at + (layer + 1, pl.ds(HALO + start - 1, count))]
            around = around + ref[at + (layer + 1, pl.ds(HALO + start + 1, count))]
            stacked = []
            if layer > 0:
                stacked.append(centres[i - len(places)])
            if layer < layers - 1:
                stacked.append(centres[i + len(places)])
            if stacked:
                around = around + VERTICAL * sum(stacked[1:], stacked[0])
            yield i // many, layer, start, count, centre, around

    def margins(edge, layer):
        lane = lax.broadcasted_iota(jnp.int32, edge.shape, 1)
        ends = (lane == 0) | (lane == width - 1)
        shift = (width - SLOT * layer - (STRIP - 1)) % width
        return jnp.where(ends, pltpu.roll(edge, shift, 1), 0.0)

    def patched(value, face, layer):
        lane = lax.broadcasted_iota(jnp.int32, face.shape, 1)
        ends = (lane < STRIP) | (lane >= width - STRIP)
        return jnp.where(ends, pltpu.roll(face, width - SLOT * layer - STRIP, 1), value)

    def gather(total, value, start, low, high):
        first, last = max(low - start, 0), min(high - start, value.shape[0])
        if last <= first:
            return total
        return total + jnp.sum(value[first:last].reshape(-1, HALO, width), axis=0)

    none = jnp.zeros((HALO, width), jnp.float32)
    each = 2 * ITERS

    def begin(sums, places, low, high, edged):
        for k, layer, start, count, _, around in columns(
                [(root, ())] + [(up, (k,)) for k in range(scen)], places):
            at = pl.ds(start, count)
            s = root[layer + 1, pl.ds(HALO + start, count)]
            if edged:
                around = around + margins(edges[4 * k - 3 if k else 0, at], layer)
            if k == 0:
                total = capac[layer, at] + s * around
                inverse = 1.0 / total
                weight[layer, at] = s * s * inverse
                slope[layer, at] = total
                recip[layer, at] = inverse
                continue
            k = k - 1
            total = slope[layer, at]
            heat = TIER_HEAT if layer % 2 == 0 else CHANNEL_HEAT
            residual = (heat - total) * vp[k, layer, at] + s * around
            if layer % 2 == 0:
                residual = residual + vq[k, layer // 2, at]
            scaled = residual * recip[layer, at]
            u0[k, layer + 1, pl.ds(HALO + start, count)] = s * scaled
            sums[k][0] = gather(sums[k][0], residual * scaled, start, low, high)

    def advance(sums, source, target, level, places, low, high, edged):
        for k, layer, start, count, centre, around in columns(
                [(source, (k,)) for k in range(scen)], places):
            at = pl.ds(start, count)
            if edged:
                around = around + margins(edges[1 + 4 * k + level, at], layer)
            i = 2 * level - 1
            sums[k][i] = gather(sums[k][i], centre * around, start, low, high)
            if target is not None:
                moved = weight[layer, at] * around
                target[k, layer + 1, pl.ds(HALO + start, count)] = moved
                sums[k][i + 1] = gather(sums[k][i + 1], moved * around, start, low, high)

    core = [[none] * each for _ in range(scen)]
    core_rows = (2 * HALO, length)
    whole = spans(HALO, length)
    for place in whole:
        begin(core, [place], *core_rows, False)
    know()
    for place in whole:
        advance(core, u0, u1, 1, [place], *core_rows, False)
    for place in whole:
        advance(core, u1, u2, 2, [place], *core_rows, False)
    for place in spans(2 * HALO, length - 2 * HALO):
        advance(core, u2, None, 3, [place], *core_rows, False)

    know()
    for dx, dy, copy in copies:
        @pl.when(has[-dx, -dy])
        def _(copy=copy):
            copy.wait_recv()

    prepare(pl.ds(0, HALO), pl.ds(HALO, HALO))
    prepare(pl.ds(HALO + length, HALO), pl.ds(2 * HALO + length, HALO))

    shape = (ext, width)
    lane = lax.broadcasted_iota(jnp.int32, shape, 1)

    taken = []

    def arounds(values):
        joined = jnp.concatenate(values, axis=0)
        high = joined.astype(jnp.bfloat16)
        below = (joined - high.astype(jnp.float32)).astype(jnp.bfloat16)
        joined = jnp.concatenate([high, below], axis=1)
        half = joined.shape[0] // 2
        moved = [jnp.dot(joined[:half], on_left[...], preferred_element_type=jnp.float32),
                 jnp.dot(joined[half:], on_right[...], preferred_element_type=jnp.float32)]
        results = []
        for i, value in enumerate(values):
            slab = slabs.at[len(taken)]
            taken.append(True)
            slab[pl.ds(HALO, ext)] = value
            side, at = divmod(i * ext, half)
            result = moved[side][at:at + ext] + slab[pl.ds(HALO - 1, ext)]
            results.append(result + slab[pl.ds(HALO + 1, ext)])
        return results

    q = lane % SLOT
    tiers_of, heats, fields, powers, roots, totals = [], [], [], [], [], []
    for far, shifts, low, shift in (
            (far_l, (STRIP, 0, width - STRIP, width - 2 * STRIP, width - 6 * STRIP), 0, 0),
            (far_r, (STRIP, 0, width - STRIP, width - 2 * STRIP, width - 6 * STRIP), STRIP, STRIP)):
        theirs = (q >= low) & (q < low + STRIP)
        turned = (lane + shift) % width
        valid = (turned // SLOT < layers) & (turned % SLOT < 3 * STRIP)
        tier = turned // SLOT % 2 == 0
        message = far[...]
        parts = []
        for i, turn in enumerate(shifts):
            other = pltpu.roll(message, turn, 1) if turn else message
            parts.append(jnp.where(theirs, other, near[i]))
        codes = jnp.where(valid, parts[scen], -1.0)
        heat = jnp.where(tier, TIER_HEAT, CHANNEL_HEAT)
        s, total = jnp.zeros(shape, jnp.float32), heat
        for code, values in enumerate(zip(TIER_ROOT, CHANNEL_ROOT, CHANNEL_SINK)):
            found = codes == code
            s = jnp.where(found, jnp.where(tier, values[0], values[1]), s)
            if values[2]:
                total = jnp.where(found, heat + jnp.where(tier, 0.0, values[2]), total)
        heats.append(heat)
        fields.append(parts[:scen])
        powers.append([jnp.where(tier & valid, part, 0.0) for part in parts[scen + 1:]])
        roots.append(s)
        totals.append(total)
    rims = [[[none] * each for _ in range(scen)] for _ in range(2)]

    def add(side, k, i, value):
        kept = value[2 * HALO:length].reshape(-1, HALO, width)
        rims[side][k][i] = rims[side][k][i] + jnp.sum(kept, axis=0)

    ends = [(0, 2 * HALO), (ext - 2 * HALO, 2 * HALO)]
    full = [[none] * each for _ in range(scen)]
    full_rows = (HALO, HALO + length)

    def border(i, left, right, faced):
        for start, count in ends:
            east = pltpu.roll(right[start:start + count], width - 2, 1)
            here = left[start:start + count]
            edges[i, pl.ds(start, count)] = jnp.where(q[:count] == STRIP - 1, here, east)
        if faced:
            faces[i] = jnp.where(q < STRIP, right, left)

    def mend(ref, level):
        for start in (2 * HALO, length - HALO):
            at, to = pl.ds(start, HALO), pl.ds(HALO + start, HALO)
            for k in range(scen):
                for layer in range(layers):
                    face = faces[1 + 4 * k + level, at]
                    ref[k, layer + 1, to] = patched(ref[k, layer + 1, to], face, layer)

    pairs = [(side, k) for side in range(2) for k in range(scen)]
    flows = [[roots[side] * field for field in fields[side]] for side in range(2)]
    border(0, *roots, False)
    for k in range(scen):
        border(1 + 4 * k, flows[0][k], flows[1][k], False)
    spread = arounds([roots[0], *flows[0], roots[1], *flows[1]])
    begin(full, ends, *full_rows, True)
    currents, weights = [], []
    for side in range(2):
        s = roots[side]
        total = totals[side] + s * spread[side * (scen + 1)]
        inverse = 1.0 / total
        weights.append(s * s * inverse)
        for k in range(scen):
            residual = (heats[side] - total) * fields[side][k] + powers[side][k]
            residual = residual + s * spread[side * (scen + 1) + 1 + k]
            scaled = residual * inverse
            add(side, k, 0, residual * scaled)
            currents.append(s * scaled)
    iterates = (u0, u1, u2, None)
    for level in range(1, ITERS + 1):
        for k in range(scen):
            border(1 + 4 * k + level, currents[k], currents[scen + k], True)
        mend(iterates[level - 1], level)
        spread = arounds(currents)
        advance(full, iterates[level - 1], iterates[level], level, ends, *full_rows, True)
        for i, (side, k) in enumerate(pairs):
            add(side, k, 2 * level - 1, currents[i] * spread[i])
            if level < ITERS:
                moved = weights[side] * spread[i]
                add(side, k, 2 * level, moved * spread[i])
                currents[i] = moved
    line = lax.broadcasted_iota(jnp.int32, (HALO, width), 1)
    middle = (line >= STRIP) & (line < width - STRIP)
    moments = []
    for k in range(scen):
        for i in range(each):
            value = full[k][i] + jnp.where(middle, core[k][i], 0.0)
            used = (line < SLOT * layers) & (line % SLOT >= STRIP) & (line % SLOT < 2 * STRIP)
            value = value + jnp.where(used, rims[0][k][i], 0.0)
            used = (line < SLOT * layers) & (line % SLOT < STRIP)
            moments.append(value + jnp.where(used, rims[1][k][i], 0.0))
    flat = jnp.zeros((1, width), jnp.float32)
    line = lax.broadcasted_iota(jnp.int32, (1, width), 1)
    for i, value in enumerate(moments):
        total = jnp.sum(jnp.sum(value, axis=0, keepdims=True), axis=1, keepdims=True)
        flat = jnp.where(line == i, total, flat)
    row[...] = flat
    rows[n - 1] = flat
    while len(heard) < len(reaches):
        know()

    def spread(i, carry):
        k = me + i
        pltpu.make_async_remote_copy(
            src_ref=row, dst_ref=rows.at[i - 1], send_sem=row_send, recv_sem=row_recv,
            device_id=jnp.where(k < n, k, k - n),
            device_id_type=pl.DeviceIdType.LOGICAL).start()
        return carry

    lax.fori_loop(1, n, spread, 0)
    for dx, dy, copy in copies:
        @pl.when(has[dx, dy])
        def _(copy=copy):
            copy.wait_send()
    def unscale(start):
        at = pl.ds(HALO + start, PIECE)
        for layer in range(layers):
            if layer % 2 == 0:
                back = lookup(vm[layer // 2, at], TIER_INV)
            else:
                back = lookup(vc[layer // 2, at], CHANNEL_INV)
            for k in range(scen):
                for level, (ref, scaled) in enumerate(((u0, f0), (u1, f1), (u2, f2))):
                    value = ref[k, layer + 1, pl.ds(2 * HALO + start, PIECE)]
                    value = patched(value, faces[2 + 4 * k + level, at], layer)
                    scaled[k, layer, pl.ds(start, PIECE)] = back * value

    in_pieces(unscale)
    arrived = rows.at[pl.ds(0, n - 1)]
    pltpu.make_async_copy(arrived, arrived, row_recv).wait()
    sums[...] = jnp.sum(rows[...], axis=0)
    pltpu.make_async_copy(arrived, arrived, row_send).wait()


def combine(sums, vp, f0, f1, f2, out, result, sem):
    scen, layers, length, width = result.shape
    line = lax.broadcasted_iota(jnp.int32, (1, width), 1)
    each = 2 * ITERS
    total = [jnp.sum(jnp.where(line == i, sums[...], 0.0), axis=1, keepdims=True)
             for i in range(scen * each)]
    for k in range(scen):
        c0, c1, c2 = coefficients(total[k * each:(k + 1) * each])
        for layer in range(layers):
            for offset in range(0, length, PIECE):
                at = pl.ds(offset, min(PIECE, length - offset))
                change = c0 * f0[k, layer, at] + c1 * f1[k, layer, at] + c2 * f2[k, layer, at]
                before = vp[k, layer, pl.ds(HALO + offset, min(PIECE, length - offset))]
                result[k, layer, at] = before + change
            pltpu.make_async_copy(result.at[k, layer], out.at[k, layer], sem).start()
    pltpu.make_async_copy(result, out, sem).wait()


def per_device(nx, ny, previous, dissipated, material, coolant):
    scen, layers, length, width = previous.shape
    tiers = material.shape[0]
    ext = length + 2 * HALO
    f32 = jnp.float32
    field = pltpu.VMEM((scen, layers + 2, ext + 3 * HALO, width), f32)
    strip = pltpu.VMEM((ext, width), f32)
    letter = pltpu.VMEM((length, width), f32)
    own = pltpu.VMEM(previous.shape, f32)
    matrix = pltpu.VMEM((2 * width, width), jnp.bfloat16)
    shared = pl.pallas_call(
        functools.partial(kernel, nx, ny),
        out_shape=(pltpu.VMEM((1, width), f32), pltpu.VMEM((scen, layers, ext, width), f32), own, own, own),
        in_specs=[pl.BlockSpec(memory_space=pl.ANY)] * 4,
        out_specs=[pl.BlockSpec(memory_space=pltpu.VMEM)] * 5,
        scratch_shapes=[
            pltpu.VMEM((scen, tiers, ext, width), f32),
            pltpu.VMEM((tiers, ext, width), jnp.int32),
            pltpu.VMEM((layers - tiers, ext, width), jnp.int32),
            pltpu.VMEM((2 * scen + 1, ext, width), f32),
            letter, letter, strip, strip,
            pltpu.VMEM((4 * scen + 1, ext, width), f32),
            pltpu.VMEM((4 * scen + 1, ext, width), f32),
            pltpu.VMEM((8 * scen + 2, ext + 2 * HALO, width), f32),
            pltpu.VMEM((layers + 2, ext + 3 * HALO, width), f32),
            pltpu.VMEM((layers, ext, width), f32),
            pltpu.VMEM((layers, ext, width), f32),
            pltpu.VMEM((layers, ext, width), f32),
            pltpu.VMEM((layers, ext, width), f32),
            field, field, field, field,
            pltpu.VMEM((1, width), f32),
            pltpu.VMEM((nx * ny, 1, width), f32),
            matrix, matrix, matrix,
            pltpu.SemaphoreType.REGULAR((max(nx, ny).bit_length(),)),
            pltpu.SemaphoreType.DMA((5,)),
            pltpu.SemaphoreType.DMA((16,)),
            pltpu.SemaphoreType.DMA((16,)),
            pltpu.SemaphoreType.DMA,
            pltpu.SemaphoreType.DMA,
        ],
        compiler_params=pltpu.CompilerParams(
            collective_id=0, has_side_effects=True, vmem_limit_bytes=48 * 1024 * 1024),
    )(*(pltpu.with_memory_space_constraint(part, pltpu.HBM)
        for part in (previous, dissipated, material, coolant)))
    shared = [pltpu.with_memory_space_constraint(part, pltpu.VMEM) for part in shared]
    return pl.pallas_call(
        combine,
        out_shape=jax.ShapeDtypeStruct(previous.shape, f32),
        in_specs=[pl.BlockSpec(memory_space=pltpu.VMEM)] * 5,
        out_specs=pl.BlockSpec(memory_space=pl.ANY),
        scratch_shapes=[own, pltpu.SemaphoreType.DMA],
        compiler_params=pltpu.CompilerParams(vmem_limit_bytes=16 * 1024 * 1024),
    )(*shared)


def solution(mesh):
    return jax.shard_map(
        functools.partial(per_device, mesh.shape["gx"], mesh.shape["gy"]),
        mesh=mesh,
        in_specs=(
            P(None, None, "gx", "gy"),
            P(None, None, "gx", "gy"),
            P(None, "gx", "gy"),
            P(None, "gx", "gy"),
        ),
        out_specs=P(None, None, "gx", "gy"),
        check_vma=False,
    )
```

```python
import functools
import math

import jax
import jax.numpy as jnp
from jax import lax
from jax.experimental import pallas as pl
from jax.experimental.pallas import tpu as pltpu
from jax.sharding import PartitionSpec as P

ITERS = 3
TIER_K = (1.0, 0.3, 0.12, 2.5)
CHANNEL_K = (1.0, 0.3, 0.25, 0.2)
CHANNEL_SINK = (0.0, 0.15, 0.45, 1.2)
TIER_HEAT = 0.05
CHANNEL_HEAT = 0.2
VERTICAL = 4.0

HALO = 8
STRIP = 4
PIECE = 32
SPAN = 48
SLOT = 4 * STRIP
MESH = pl.DeviceIdType.MESH

TIER_ROOT = tuple(math.sqrt(v) for v in TIER_K)
CHANNEL_ROOT = tuple(math.sqrt(v) for v in CHANNEL_K)
TIER_INV = tuple(1.0 / math.sqrt(v) for v in TIER_K)
CHANNEL_INV = tuple(1.0 / math.sqrt(v) for v in CHANNEL_K)


def lookup(codes, table):
    total = jnp.zeros(codes.shape, jnp.float32)
    for index, value in enumerate(table):
        total = jnp.where(codes == index, jnp.float32(value), total)
    return total


def coefficients(nu):
    def inner(a, b):
        total = None
        for i, x in enumerate(a):
            for j, y in enumerate(b):
                term = x * y * nu[i + j]
                total = term if total is None else total + term
        return total

    zero = nu[0] * 0.0
    rho = [zero + 1.0]
    pi = [zero + 1.0]
    norm = nu[0]
    result = [zero] * ITERS
    for iteration in range(ITERS):
        image = [a - b for a, b in zip(pi + [zero], [zero] + pi)]
        step = norm / inner(pi, image)
        for i, a in enumerate(pi):
            result[i] = result[i] + step * a
        if iteration + 1 < ITERS:
            rho = [a - step * b for a, b in zip(rho + [zero], image)]
            following = inner(rho, rho)
            growth = following / norm
            pi = [a + growth * b for a, b in zip(rho, pi + [zero])]
            norm = following
    return result


def kernel(nx, ny, prev, diss, mat, cool, sums, vp, f0, f1, f2, vq, vm, vc, near, own_l, own_r, far_l, far_r,
           edges, faces, slabs, root, weight, capac, slope, recip, up, u0, u1, u2, row, rows,
           along, on_left, on_right, known, load_sem, send_sem, recv_sem, row_send, row_recv):
    scen, layers, length, width = prev.shape
    tiers = mat.shape[0]
    n = nx * ny
    ext = length + 2 * HALO
    x, y = lax.axis_index("gx"), lax.axis_index("gy")
    me = x * ny + y
    barrier = pltpu.get_barrier_semaphore()

    def around_me(reach):
        found = []
        for dx in (-reach, 0, reach):
            for dy in (-reach, 0, reach):
                if (dx or dy) and abs(dx) < nx and abs(dy) < ny:
                    inside_x = jnp.logical_and(x + dx >= 0, x + dx < nx)
                    inside_y = jnp.logical_and(y + dy >= 0, y + dy < ny)
                    found.append((dx, dy, jnp.logical_and(inside_x, inside_y)))
        return found

    def greet(sem, reach):
        for dx, dy, there in around_me(reach):
            @pl.when(there)
            def _(dx=dx, dy=dy):
                pl.semaphore_signal(sem, inc=1, device_id=(x + dx, y + dy), device_id_type=MESH)

    def hear(sem, reach):
        pl.semaphore_wait(sem, sum(there.astype(jnp.int32) for _, _, there in around_me(reach)))

    reaches = [1]
    while 2 * reaches[-1] < max(nx, ny) - 1:
        reaches.append(2 * reaches[-1])
    heard = []

    def know():
        if len(heard) < len(reaches):
            hear(known.at[len(heard)], reaches[len(heard)])
            heard.append(True)
            if len(heard) < len(reaches):
                greet(known.at[len(heard)], reaches[len(heard)])

    inside = pl.ds(HALO, length)
    loads = [
        pltpu.make_async_copy(prev.at[0], vp.at[0, :, inside], load_sem.at[0]),
        pltpu.make_async_copy(prev.at[1], vp.at[1, :, inside], load_sem.at[1]),
        pltpu.make_async_copy(diss, vq.at[:, :, inside], load_sem.at[2]),
        pltpu.make_async_copy(mat, vm.at[:, inside], load_sem.at[3]),
        pltpu.make_async_copy(cool, vc.at[:, inside], load_sem.at[4]),
    ]
    for copy in loads:
        copy.start()
    greet(barrier, 1)

    has = {(-1, 0): x > 0, (1, 0): x < nx - 1, (0, -1): y > 0, (0, 1): y < ny - 1}
    for dx in (-1, 1):
        for dy in (-1, 1):
            has[dx, dy] = jnp.logical_and(has[dx, 0], has[0, dy])
    top, bottom = pl.ds(0, HALO), pl.ds(HALO + length, HALO)
    first, last = pl.ds(HALO, HALO), pl.ds(length, HALO)

    def fill(ref):
        ref[...] = jnp.full(ref.shape, -1, ref.dtype)

    for dx, where in ((-1, top), (1, bottom)):
        @pl.when(jnp.logical_not(has[dx, 0]))
        def _(where=where):
            for ref in (vp, vq):
                fill(ref.at[:, :, where])
            for ref in (vm, vc):
                fill(ref.at[:, where])
            fill(near.at[:, where])
    for dy, ref in ((-1, far_l), (1, far_r)):
        @pl.when(jnp.logical_not(has[0, dy]))
        def _(ref=ref):
            fill(ref.at[inside])
        for dx, where in ((-1, top), (1, bottom)):
            @pl.when(jnp.logical_not(has[dx, dy]))
            def _(ref=ref, where=where):
                fill(ref.at[where])

    source = lax.broadcasted_iota(jnp.int32, (width, width), 0)
    target = lax.broadcasted_iota(jnp.int32, (width, width), 1)
    beside = jnp.abs(target - source) == 1
    matrices = [(along, jnp.where(beside, 1.0, 0.0))]
    for ref, shift in ((on_left, 0), (on_right, STRIP)):
        begins, ends = (source + shift) % width, (target + shift) % width
        apart, spot = ends - begins, ends // SLOT
        valid = (spot < layers) & (ends % SLOT < 3 * STRIP) & (begins % SLOT < 3 * STRIP)
        beside = ((apart == 1) | (apart == -1)) & (begins // SLOT == spot)
        stacked = (apart == SLOT) & (spot > 0) | (apart == -SLOT) & (spot < layers - 1)
        weights = jnp.where(stacked, VERTICAL, jnp.where(beside, 1.0, 0.0))
        matrices.append((ref, jnp.where(valid, weights, 0.0)))
    for ref, weights in matrices:
        for i in range(2):
            ref[pl.ds(i * width, width)] = weights.astype(jnp.bfloat16)
    blank = jnp.zeros((ext + 3 * HALO, width), jnp.float32)
    for pad in (0, layers + 1):
        root[pad] = blank
        for k in range(scen):
            for ref in (up, u0, u1, u2):
                ref[k, pad] = blank
    for i in range(slabs.shape[0]):
        for at in (pl.ds(0, HALO), pl.ds(HALO + ext, HALO)):
            slabs[i, at] = blank[:HALO]
    for at in (pl.ds(HALO, HALO), pl.ds(2 * HALO + length, HALO)):
        for layer in range(layers):
            root[layer + 1, at] = blank[:HALO]
            for k in range(scen):
                for ref in (up, u0, u1, u2):
                    ref[k, layer + 1, at] = blank[:HALO]

    def pack(places):
        lane = lax.broadcasted_iota(jnp.int32, (length, width), 1)
        packed = opening = None
        for layer, ref, index in places:
            plane = ref[index + (inside,)].astype(jnp.float32)
            turned = pltpu.roll(plane, SLOT * layer + STRIP, 1)
            if packed is None:
                packed = opening = turned
            else:
                packed = jnp.where(lane >= SLOT * layer - STRIP, turned, packed)
        return jnp.where(lane >= width - STRIP, opening, packed)

    def write(part, places):
        lane = lax.broadcasted_iota(jnp.int32, (length, width), 1)
        left = right = opening = None
        for slot, ref, index in places:
            base = SLOT * slot + STRIP * part
            plane = ref[index + (inside,)].astype(jnp.float32)
            turned = pltpu.roll(plane, base, 1) if base else plane
            if left is None:
                left = right = opening = turned
            else:
                left = jnp.where(lane >= base, turned, left)
                right = jnp.where(lane >= base - STRIP, turned, right)
        if part == 0:
            right = jnp.where(lane >= width - STRIP, opening, right)
        if written:
            left = jnp.where(lane % SLOT // STRIP == part, left, own_l[...])
            right = jnp.where((lane + STRIP) % SLOT // STRIP == part, right, own_r[...])
        own_l[...], own_r[...] = left, right
        written.append(part)

    written = []
    for k in range(scen):
        loads[k].wait()
        write(k, [(layer, vp, (k, layer)) for layer in range(layers)])
    loads[2].wait()
    write(scen + 1, [(2 * t + k, vq, (k, t)) for t in range(tiers) for k in range(scen)])
    for copy in loads[3:]:
        copy.wait()
    write(scen, [(layer, vc if layer % 2 else vm, (layer // 2,)) for layer in range(layers)])

    hear(barrier, 1)
    greet(known.at[0], 1)

    sends = []
    for dx, source, target in ((-1, first, bottom), (1, last, top)):
        for ref in (vp, vq):
            sends.append((dx, 0, ref.at[:, :, source], ref.at[:, :, target]))
        for ref in (vm, vc):
            sends.append((dx, 0, ref.at[:, source], ref.at[:, target]))
        begins = pl.ds(0 if dx < 0 else length - HALO, HALO)
        sends.append((dx, -1, own_l.at[begins], far_r.at[target]))
        sends.append((dx, 1, own_r.at[begins], far_l.at[target]))
    sends.append((0, -1, own_l, far_r.at[inside]))
    sends.append((0, 1, own_r, far_l.at[inside]))
    for dx, source, target in ((-1, first, bottom), (1, last, top)):
        sends.append((dx, 0, near.at[:, source], near.at[:, target]))
    copies = []
    for i, (dx, dy, source, target) in enumerate(sends):
        copy = pltpu.make_async_remote_copy(
            src_ref=source, dst_ref=target, send_sem=send_sem.at[i], recv_sem=recv_sem.at[i],
            device_id=(x + dx, y + dy), device_id_type=MESH)
        copies.append((dx, dy, copy))
    order = sorted(copies[:-2], key=lambda c: 0 if c[0] and c[1] else 1 if c[0] == 0 else 2)

    def begin_sends(order):
        for dx, dy, copy in order:
            @pl.when(has[dx, dy])
            def _(copy=copy):
                copy.start()

    begin_sends(order)
    for k in range(scen):
        near[k, inside] = pack([(layer, vp, (k, layer)) for layer in range(layers)])
        near[scen + 1 + k, inside] = pack([(2 * t, vq, (k, t)) for t in range(tiers)])
    near[scen, inside] = pack([(layer, vc if layer % 2 else vm, (layer // 2,)) for layer in range(layers)])
    begin_sends(copies[-2:])

    def prepare(at, to):
        count = at.size
        for layer in range(layers):
            if layer % 2 == 0:
                s = lookup(vm[layer // 2, at], TIER_ROOT)
                total = jnp.full((count, width), TIER_HEAT, jnp.float32)
            else:
                codes = vc[layer // 2, at]
                s = lookup(codes, CHANNEL_ROOT)
                total = CHANNEL_HEAT + lookup(codes, CHANNEL_SINK)
            root[layer + 1, to] = s
            capac[layer, at] = total
            for k in range(scen):
                up[k, layer + 1, to] = s * vp[k, layer, at]

    def in_pieces(step):
        def one(i, carry):
            step(pl.multiple_of(i * PIECE, PIECE))
            return carry

        lax.fori_loop(0, length // PIECE, one, 0)

    in_pieces(lambda start: prepare(pl.ds(HALO + start, PIECE), pl.ds(2 * HALO + start, PIECE)))

    def shifted(value, matrix):
        high = value.astype(jnp.bfloat16)
        low = (value - high.astype(jnp.float32)).astype(jnp.bfloat16)
        return jnp.dot(jnp.concatenate([high, low], axis=1), matrix[...],
                       preferred_element_type=jnp.float32)

    def spans(start, count):
        pieces = []
        while count > 0:
            piece = min(count, SPAN)
            pieces.append((start, piece))
            start, count = start + piece, count - piece
        return pieces

    def columns(refs, places):
        centres = []
        for ref, at in refs:
            for layer in range(layers):
                for start, count in places:
                    centres.append(ref[at + (layer + 1, pl.ds(HALO + start, count))])
        lateral = shifted(jnp.concatenate(centres, axis=0), along)
        many, offset = layers * len(places), 0
        for i, centre in enumerate(centres):
            ref, at = refs[i // many]
            layer, (start, count) = i % many // len(places), places[i % len(places)]
            around = lateral[offset:offset + count]
            offset += count
            around = around + ref[at + (layer + 1, pl.ds(HALO + start - 1, count))]
            around = around + ref[at + (layer + 1, pl.ds(HALO + start + 1, count))]
            stacked = []
            if layer > 0:
                stacked.append(centres[i - len(places)])
            if layer < layers - 1:
                stacked.append(centres[i + len(places)])
            if stacked:
                around = around + VERTICAL * sum(stacked[1:], stacked[0])
            yield i // many, layer, start, count, centre, around

    def margins(edge, layer):
        lane = lax.broadcasted_iota(jnp.int32, edge.shape, 1)
        ends = (lane == 0) | (lane == width - 1)
        shift = (width - SLOT * layer - (STRIP - 1)) % width
        return jnp.where(ends, pltpu.roll(edge, shift, 1), 0.0)

    def patched(value, face, layer):
        lane = lax.broadcasted_iota(jnp.int32, face.shape, 1)
        ends = (lane < STRIP) | (lane >= width - STRIP)
        return jnp.where(ends, pltpu.roll(face, width - SLOT * layer - STRIP, 1), value)

    def gather(total, value, start, low, high):
        first, last = max(low - start, 0), min(high - start, value.shape[0])
        if last <= first:
            return total
        return total + jnp.sum(value[first:last].reshape(-1, HALO, width), axis=0)

    none = jnp.zeros((HALO, width), jnp.float32)
    each = 2 * ITERS

    def begin(sums, places, low, high, edged):
        for k, layer, start, count, _, around in columns(
                [(root, ())] + [(up, (k,)) for k in range(scen)], places):
            at = pl.ds(start, count)
            s = root[layer + 1, pl.ds(HALO + start, count)]
            if edged:
                around = around + margins(edges[4 * k - 3 if k else 0, at], layer)
            if k == 0:
                total = capac[layer, at] + s * around
                inverse = 1.0 / total
                weight[layer, at] = s * s * inverse
                slope[layer, at] = total
                recip[layer, at] = inverse
                continue
            k = k - 1
            total = slope[layer, at]
            heat = TIER_HEAT if layer % 2 == 0 else CHANNEL_HEAT
            residual = (heat - total) * vp[k, layer, at] + s * around
            if layer % 2 == 0:
                residual = residual + vq[k, layer // 2, at]
            scaled = residual * recip[layer, at]
            u0[k, layer + 1, pl.ds(HALO + start, count)] = s * scaled
            sums[k][0] = gather(sums[k][0], residual * scaled, start, low, high)

    def advance(sums, source, target, level, places, low, high, edged):
        for k, layer, start, count, centre, around in columns(
                [(source, (k,)) for k in range(scen)], places):
            at = pl.ds(start, count)
            if edged:
                around = around + margins(edges[1 + 4 * k + level, at], layer)
            i = 2 * level - 1
            sums[k][i] = gather(sums[k][i], centre * around, start, low, high)
            if target is not None:
                moved = weight[layer, at] * around
                target[k, layer + 1, pl.ds(HALO + start, count)] = moved
                sums[k][i + 1] = gather(sums[k][i + 1], moved * around, start, low, high)

    core = [[none] * each for _ in range(scen)]
    core_rows = (2 * HALO, length)
    whole = spans(HALO, length)
    for place in whole:
        begin(core, [place], *core_rows, False)
    know()
    for place in whole:
        advance(core, u0, u1, 1, [place], *core_rows, False)
    for place in whole:
        advance(core, u1, u2, 2, [place], *core_rows, False)
    for place in spans(2 * HALO, length - 2 * HALO):
        advance(core, u2, None, 3, [place], *core_rows, False)

    know()
    def arrive(chosen):
        for dx, dy, copy in chosen:
            @pl.when(has[-dx, -dy])
            def _(copy=copy):
                copy.wait_recv()

    arrive(copy for copy in copies if copy[:2] != (0, -1))

    prepare(pl.ds(0, HALO), pl.ds(HALO, HALO))
    prepare(pl.ds(HALO + length, HALO), pl.ds(2 * HALO + length, HALO))

    shape = (ext, width)
    lane = lax.broadcasted_iota(jnp.int32, shape, 1)

    taken = []

    def arounds(values, matrix, first=0, count=ext):
        moved = shifted(jnp.concatenate([value[first:first + count] for value in values], axis=0), matrix)
        results = []
        for i, value in enumerate(values):
            slab = slabs.at[len(taken)]
            taken.append(True)
            slab[pl.ds(HALO, ext)] = value
            result = moved[i * count:(i + 1) * count] + slab[pl.ds(HALO + first - 1, count)]
            results.append(result + slab[pl.ds(HALO + first + 1, count)])
        return results

    q = lane % SLOT
    rims = [[[none] * each for _ in range(scen)] for _ in range(2)]

    def add(side, k, i, value):
        kept = value if value.shape[0] < ext else value[2 * HALO:length]
        kept = kept.reshape(-1, HALO, width)
        rims[side][k][i] = rims[side][k][i] + jnp.sum(kept, axis=0)

    def side_of(side, far, shifts, low, shift, matrix, between):
        theirs = (q >= low) & (q < low + STRIP)
        turned = (lane + shift) % width
        valid = (turned // SLOT < layers) & (turned % SLOT < 3 * STRIP)
        tier = turned // SLOT % 2 == 0
        message = far[...]
        parts = []
        for i, turn in enumerate(shifts):
            other = pltpu.roll(message, turn, 1) if turn else message
            parts.append(jnp.where(theirs, other, near[i]))
        codes = jnp.where(valid, parts[scen], -1.0)
        heat = jnp.where(tier, TIER_HEAT, CHANNEL_HEAT)
        s, total = jnp.zeros(shape, jnp.float32), heat
        for code, values in enumerate(zip(TIER_ROOT, CHANNEL_ROOT, CHANNEL_SINK)):
            found = codes == code
            s = jnp.where(found, jnp.where(tier, values[0], values[1]), s)
            if values[2]:
                total = jnp.where(found, heat + jnp.where(tier, 0.0, values[2]), total)
        currents = [s] + [s * parts[k] for k in range(scen)]
        between(0, currents, False)
        spread = arounds(currents, matrix)
        between(0, currents, True)
        total = total + s * spread[0]
        inverse = 1.0 / total
        w = s * s * inverse
        currents = []
        for k in range(scen):
            power = jnp.where(tier & valid, parts[scen + 1 + k], 0.0)
            residual = (heat - total) * parts[k] + power + s * spread[1 + k]
            scaled = residual * inverse
            add(side, k, 0, residual * scaled)
            currents.append(s * scaled)
        for level in range(1, ITERS + 1):
            between(level, currents, False)
            kept = (0, ext) if level < ITERS else (2 * HALO, length - 2 * HALO)
            spread = arounds(currents, matrix, *kept)
            between(level, currents, True)
            for k in range(scen):
                add(side, k, 2 * level - 1, currents[k][kept[0]:kept[0] + kept[1]] * spread[k])
                if level < ITERS:
                    moved = w * spread[k]
                    add(side, k, 2 * level, moved * spread[k])
                    currents[k] = moved

    ends = [(0, 2 * HALO), (ext - 2 * HALO, 2 * HALO)]
    full = [[none] * each for _ in range(scen)]
    full_rows = (HALO, HALO + length)

    def border(i, left, right, faced):
        for start, count in ends:
            east = pltpu.roll(right[start:start + count], width - 2, 1)
            here = slabs[left, pl.ds(HALO + start, count)]
            edges[i, pl.ds(start, count)] = jnp.where(q[:count] == STRIP - 1, here, east)
        if faced:
            faces[i] = jnp.where(q < STRIP, right, slabs[left, pl.ds(HALO, ext)])

    def mend(ref, level):
        for start in (2 * HALO, length - HALO):
            at, to = pl.ds(start, HALO), pl.ds(HALO + start, HALO)
            for k in range(scen):
                for layer in range(layers):
                    face = faces[1 + 4 * k + level, at]
                    ref[k, layer + 1, to] = patched(ref[k, layer + 1, to], face, layer)

    iterates = (u0, u1, u2, None)

    def alone(level, currents, after):
        pass

    def beside_rows(level, currents, after):
        if after and level:
            advance(full, iterates[level - 1], iterates[level], level, ends, *full_rows, True)
        elif after:
            begin(full, ends, *full_rows, True)
        elif level:
            for k in range(scen):
                border(1 + 4 * k + level, scen * level + 1 + k, currents[k], True)
            mend(iterates[level - 1], level)
        else:
            border(0, 0, currents[0], False)
            for k in range(scen):
                border(1 + 4 * k, 1 + k, currents[1 + k], False)

    turns = (STRIP, 0, width - STRIP, width - 2 * STRIP, width - 6 * STRIP)
    side_of(0, far_l, turns, 0, 0, on_left, alone)
    arrive(copy for copy in copies if copy[:2] == (0, -1))
    side_of(1, far_r, turns, STRIP, STRIP, on_right, beside_rows)
    line = lax.broadcasted_iota(jnp.int32, (HALO, width), 1)
    middle = (line >= STRIP) & (line < width - STRIP)
    moments = []
    for k in range(scen):
        for i in range(each):
            value = full[k][i] + jnp.where(middle, core[k][i], 0.0)
            used = (line < SLOT * layers) & (line % SLOT >= STRIP) & (line % SLOT < 2 * STRIP)
            value = value + jnp.where(used, rims[0][k][i], 0.0)
            used = (line < SLOT * layers) & (line % SLOT < STRIP)
            moments.append(value + jnp.where(used, rims[1][k][i], 0.0))
    flat = jnp.zeros((1, width), jnp.float32)
    line = lax.broadcasted_iota(jnp.int32, (1, width), 1)
    for i, value in enumerate(moments):
        total = jnp.sum(jnp.sum(value, axis=0, keepdims=True), axis=1, keepdims=True)
        flat = jnp.where(line == i, total, flat)
    row[...] = flat
    rows[n - 1] = flat
    while len(heard) < len(reaches):
        know()

    def spread(i, carry):
        k = jnp.where(i < me, i, i + 1)
        slot = jnp.where(i < me, i - me + n - 1, i - me)
        pltpu.make_async_remote_copy(
            src_ref=row, dst_ref=rows.at[slot], send_sem=row_send, recv_sem=row_recv,
            device_id=k, device_id_type=pl.DeviceIdType.LOGICAL).start()
        return carry

    lax.fori_loop(0, n - 1, spread, 0)
    for dx, dy, copy in copies:
        @pl.when(has[dx, dy])
        def _(copy=copy):
            copy.wait_send()
    def unscale(start):
        at = pl.ds(HALO + start, PIECE)
        for layer in range(layers):
            if layer % 2 == 0:
                back = lookup(vm[layer // 2, at], TIER_INV)
            else:
                back = lookup(vc[layer // 2, at], CHANNEL_INV)
            for k in range(scen):
                for level, (ref, scaled) in enumerate(((u0, f0), (u1, f1), (u2, f2))):
                    value = ref[k, layer + 1, pl.ds(2 * HALO + start, PIECE)]
                    value = patched(value, faces[2 + 4 * k + level, at], layer)
                    scaled[k, layer, pl.ds(start, PIECE)] = back * value

    in_pieces(unscale)
    arrived = rows.at[pl.ds(0, n - 1)]
    pltpu.make_async_copy(arrived, arrived, row_recv).wait()
    sums[...] = jnp.sum(rows[...], axis=0)
    pltpu.make_async_copy(arrived, arrived, row_send).wait()


def combine(sums, vp, f0, f1, f2, out, result, sem):
    scen, layers, length, width = result.shape
    line = lax.broadcasted_iota(jnp.int32, (1, width), 1)
    each = 2 * ITERS
    total = [jnp.sum(jnp.where(line == i, sums[...], 0.0), axis=1, keepdims=True)
             for i in range(scen * each)]
    for k in range(scen):
        c0, c1, c2 = coefficients(total[k * each:(k + 1) * each])
        for layer in range(layers):
            for offset in range(0, length, PIECE):
                at = pl.ds(offset, min(PIECE, length - offset))
                change = c0 * f0[k, layer, at] + c1 * f1[k, layer, at] + c2 * f2[k, layer, at]
                before = vp[k, layer, pl.ds(HALO + offset, min(PIECE, length - offset))]
                result[k, layer, at] = before + change
            pltpu.make_async_copy(result.at[k, layer], out.at[k, layer], sem).start()
    pltpu.make_async_copy(result, out, sem).wait()


def per_device(nx, ny, previous, dissipated, material, coolant):
    scen, layers, length, width = previous.shape
    tiers = material.shape[0]
    ext = length + 2 * HALO
    f32 = jnp.float32
    field = pltpu.VMEM((scen, layers + 2, ext + 3 * HALO, width), f32)
    strip = pltpu.VMEM((ext, width), f32)
    letter = pltpu.VMEM((length, width), f32)
    own = pltpu.VMEM(previous.shape, f32)
    matrix = pltpu.VMEM((2 * width, width), jnp.bfloat16)
    shared = pl.pallas_call(
        functools.partial(kernel, nx, ny),
        out_shape=(pltpu.VMEM((1, width), f32), pltpu.VMEM((scen, layers, ext, width), f32), own, own, own),
        in_specs=[pl.BlockSpec(memory_space=pl.ANY)] * 4,
        out_specs=[pl.BlockSpec(memory_space=pltpu.VMEM)] * 5,
        scratch_shapes=[
            pltpu.VMEM((scen, tiers, ext, width), f32),
            pltpu.VMEM((tiers, ext, width), jnp.int32),
            pltpu.VMEM((layers - tiers, ext, width), jnp.int32),
            pltpu.VMEM((2 * scen + 1, ext, width), f32),
            letter, letter, strip, strip,
            pltpu.VMEM((4 * scen + 1, ext, width), f32),
            pltpu.VMEM((4 * scen + 1, ext, width), f32),
            pltpu.VMEM((8 * scen + 2, ext + 2 * HALO, width), f32),
            pltpu.VMEM((layers + 2, ext + 3 * HALO, width), f32),
            pltpu.VMEM((layers, ext, width), f32),
            pltpu.VMEM((layers, ext, width), f32),
            pltpu.VMEM((layers, ext, width), f32),
            pltpu.VMEM((layers, ext, width), f32),
            field, field, field, field,
            pltpu.VMEM((1, width), f32),
            pltpu.VMEM((nx * ny, 1, width), f32),
            matrix, matrix, matrix,
            pltpu.SemaphoreType.REGULAR((max(nx, ny).bit_length(),)),
            pltpu.SemaphoreType.DMA((5,)),
            pltpu.SemaphoreType.DMA((16,)),
            pltpu.SemaphoreType.DMA((16,)),
            pltpu.SemaphoreType.DMA,
            pltpu.SemaphoreType.DMA,
        ],
        compiler_params=pltpu.CompilerParams(
            collective_id=0, has_side_effects=True, vmem_limit_bytes=48 * 1024 * 1024),
    )(*(pltpu.with_memory_space_constraint(part, pltpu.HBM)
        for part in (previous, dissipated, material, coolant)))
    shared = [pltpu.with_memory_space_constraint(part, pltpu.VMEM) for part in shared]
    return pl.pallas_call(
        combine,
        out_shape=jax.ShapeDtypeStruct(previous.shape, f32),
        in_specs=[pl.BlockSpec(memory_space=pltpu.VMEM)] * 5,
        out_specs=pl.BlockSpec(memory_space=pl.ANY),
        scratch_shapes=[own, pltpu.SemaphoreType.DMA],
        compiler_params=pltpu.CompilerParams(vmem_limit_bytes=16 * 1024 * 1024),
    )(*shared)


def solution(mesh):
    return jax.shard_map(
        functools.partial(per_device, mesh.shape["gx"], mesh.shape["gy"]),
        mesh=mesh,
        in_specs=(
            P(None, None, "gx", "gy"),
            P(None, None, "gx", "gy"),
            P(None, "gx", "gy"),
            P(None, "gx", "gy"),
        ),
        out_specs=P(None, None, "gx", "gy"),
        check_vma=False,
    )
```

```python
import functools
import math

import jax
import jax.numpy as jnp
from jax import lax
from jax.experimental import pallas as pl
from jax.experimental.pallas import tpu as pltpu
from jax.sharding import PartitionSpec as P

ITERS = 3
TIER_K = (1.0, 0.3, 0.12, 2.5)
CHANNEL_K = (1.0, 0.3, 0.25, 0.2)
CHANNEL_SINK = (0.0, 0.15, 0.45, 1.2)
TIER_HEAT = 0.05
CHANNEL_HEAT = 0.2
VERTICAL = 4.0

HALO = 8
STRIP = 4
PIECE = 32
SPAN = 48
SLOT = 4 * STRIP
MESH = pl.DeviceIdType.MESH

TIER_ROOT = tuple(math.sqrt(v) for v in TIER_K)
CHANNEL_ROOT = tuple(math.sqrt(v) for v in CHANNEL_K)
TIER_INV = tuple(1.0 / math.sqrt(v) for v in TIER_K)
CHANNEL_INV = tuple(1.0 / math.sqrt(v) for v in CHANNEL_K)


def lookup(codes, table):
    total = jnp.zeros(codes.shape, jnp.float32)
    for index, value in enumerate(table):
        total = jnp.where(codes == index, jnp.float32(value), total)
    return total


def coefficients(nu):
    def inner(a, b):
        total = None
        for i, x in enumerate(a):
            for j, y in enumerate(b):
                term = x * y * nu[i + j]
                total = term if total is None else total + term
        return total

    zero = nu[0] * 0.0
    rho = [zero + 1.0]
    pi = [zero + 1.0]
    norm = nu[0]
    result = [zero] * ITERS
    for iteration in range(ITERS):
        image = [a - b for a, b in zip(pi + [zero], [zero] + pi)]
        step = norm / inner(pi, image)
        for i, a in enumerate(pi):
            result[i] = result[i] + step * a
        if iteration + 1 < ITERS:
            rho = [a - step * b for a, b in zip(rho + [zero], image)]
            following = inner(rho, rho)
            growth = following / norm
            pi = [a + growth * b for a, b in zip(rho, pi + [zero])]
            norm = following
    return result


def kernel(nx, ny, prev, diss, mat, cool, sums, vp, f0, f1, f2, vq, vm, vc, near, own_l, own_r, far_l, far_r,
           edges, faces, slabs, root, weight, capac, slope, recip, up, u0, u1, u2, row, rows,
           along, on_left, on_right, known, load_sem, send_sem, recv_sem, row_send, row_recv):
    scen, layers, length, width = prev.shape
    tiers = mat.shape[0]
    n = nx * ny
    ext = length + 2 * HALO
    x, y = lax.axis_index("gx"), lax.axis_index("gy")
    me = x * ny + y
    barrier = pltpu.get_barrier_semaphore()

    def around_me(reach):
        found = []
        for dx in (-reach, 0, reach):
            for dy in (-reach, 0, reach):
                if (dx or dy) and abs(dx) < nx and abs(dy) < ny:
                    inside_x = jnp.logical_and(x + dx >= 0, x + dx < nx)
                    inside_y = jnp.logical_and(y + dy >= 0, y + dy < ny)
                    found.append((dx, dy, jnp.logical_and(inside_x, inside_y)))
        return found

    def greet(sem, reach):
        for dx, dy, there in around_me(reach):
            @pl.when(there)
            def _(dx=dx, dy=dy):
                pl.semaphore_signal(sem, inc=1, device_id=(x + dx, y + dy), device_id_type=MESH)

    def hear(sem, reach):
        pl.semaphore_wait(sem, sum(there.astype(jnp.int32) for _, _, there in around_me(reach)))

    reaches = [1]
    while 2 * reaches[-1] < max(nx, ny) - 1:
        reaches.append(2 * reaches[-1])
    heard = []

    def know():
        if len(heard) < len(reaches):
            hear(known.at[len(heard)], reaches[len(heard)])
            heard.append(True)
            if len(heard) < len(reaches):
                greet(known.at[len(heard)], reaches[len(heard)])

    inside = pl.ds(HALO, length)
    loads = [
        pltpu.make_async_copy(prev.at[0], vp.at[0, :, inside], load_sem.at[0]),
        pltpu.make_async_copy(prev.at[1], vp.at[1, :, inside], load_sem.at[1]),
        pltpu.make_async_copy(diss, vq.at[:, :, inside], load_sem.at[2]),
        pltpu.make_async_copy(mat, vm.at[:, inside], load_sem.at[3]),
        pltpu.make_async_copy(cool, vc.at[:, inside], load_sem.at[4]),
    ]
    for copy in loads:
        copy.start()
    greet(barrier, 1)

    has = {(-1, 0): x > 0, (1, 0): x < nx - 1, (0, -1): y > 0, (0, 1): y < ny - 1}
    for dx in (-1, 1):
        for dy in (-1, 1):
            has[dx, dy] = jnp.logical_and(has[dx, 0], has[0, dy])
    top, bottom = pl.ds(0, HALO), pl.ds(HALO + length, HALO)
    first, last = pl.ds(HALO, HALO), pl.ds(length, HALO)

    def fill(ref):
        ref[...] = jnp.full(ref.shape, -1, ref.dtype)

    for dx, where in ((-1, top), (1, bottom)):
        @pl.when(jnp.logical_not(has[dx, 0]))
        def _(where=where):
            for ref in (vp, vq):
                fill(ref.at[:, :, where])
            for ref in (vm, vc):
                fill(ref.at[:, where])
            fill(near.at[:, where])
    for dy, ref in ((-1, far_l), (1, far_r)):
        @pl.when(jnp.logical_not(has[0, dy]))
        def _(ref=ref):
            fill(ref.at[inside])
        for dx, where in ((-1, top), (1, bottom)):
            @pl.when(jnp.logical_not(has[dx, dy]))
            def _(ref=ref, where=where):
                fill(ref.at[where])

    source = lax.broadcasted_iota(jnp.int32, (width, width), 0)
    target = lax.broadcasted_iota(jnp.int32, (width, width), 1)
    beside = jnp.abs(target - source) == 1
    matrices = [(along, jnp.where(beside, 1.0, 0.0))]
    for ref, shift in ((on_left, 0), (on_right, STRIP)):
        begins, ends = (source + shift) % width, (target + shift) % width
        apart, spot = ends - begins, ends // SLOT
        valid = (spot < layers) & (ends % SLOT < 3 * STRIP) & (begins % SLOT < 3 * STRIP)
        beside = ((apart == 1) | (apart == -1)) & (begins // SLOT == spot)
        stacked = (apart == SLOT) & (spot > 0) | (apart == -SLOT) & (spot < layers - 1)
        weights = jnp.where(stacked, VERTICAL, jnp.where(beside, 1.0, 0.0))
        matrices.append((ref, jnp.where(valid, weights, 0.0)))
    for ref, weights in matrices:
        for i in range(2):
            ref[pl.ds(i * width, width)] = weights.astype(jnp.bfloat16)
    blank = jnp.zeros((ext + 3 * HALO, width), jnp.float32)
    for pad in (0, layers + 1):
        root[pad] = blank
        for k in range(scen):
            for ref in (up, u0, u1, u2):
                ref[k, pad] = blank
    for i in range(slabs.shape[0]):
        for at in (pl.ds(0, HALO), pl.ds(HALO + ext, HALO)):
            slabs[i, at] = blank[:HALO]
    for at in (pl.ds(HALO, HALO), pl.ds(2 * HALO + length, HALO)):
        for layer in range(layers):
            root[layer + 1, at] = blank[:HALO]
            for k in range(scen):
                for ref in (up, u0, u1, u2):
                    ref[k, layer + 1, at] = blank[:HALO]

    def pack(places):
        lane = lax.broadcasted_iota(jnp.int32, (length, width), 1)
        packed = opening = None
        for layer, ref, index in places:
            plane = ref[index + (inside,)].astype(jnp.float32)
            turned = pltpu.roll(plane, SLOT * layer + STRIP, 1)
            if packed is None:
                packed = opening = turned
            else:
                packed = jnp.where(lane >= SLOT * layer - STRIP, turned, packed)
        return jnp.where(lane >= width - STRIP, opening, packed)

    def write(part, places):
        lane = lax.broadcasted_iota(jnp.int32, (length, width), 1)
        left = right = opening = None
        for slot, ref, index in places:
            base = SLOT * slot + STRIP * part
            plane = ref[index + (inside,)].astype(jnp.float32)
            turned = pltpu.roll(plane, base, 1) if base else plane
            if left is None:
                left = right = opening = turned
            else:
                left = jnp.where(lane >= base, turned, left)
                right = jnp.where(lane >= base - STRIP, turned, right)
        if part == 0:
            right = jnp.where(lane >= width - STRIP, opening, right)
        if written:
            left = jnp.where(lane % SLOT // STRIP == part, left, own_l[...])
            right = jnp.where((lane + STRIP) % SLOT // STRIP == part, right, own_r[...])
        own_l[...], own_r[...] = left, right
        written.append(part)

    written = []
    for k in range(scen):
        loads[k].wait()
        write(k, [(layer, vp, (k, layer)) for layer in range(layers)])
    loads[2].wait()
    write(scen + 1, [(2 * t + k, vq, (k, t)) for t in range(tiers) for k in range(scen)])
    for copy in loads[3:]:
        copy.wait()
    write(scen, [(layer, vc if layer % 2 else vm, (layer // 2,)) for layer in range(layers)])

    hear(barrier, 1)
    greet(known.at[0], 1)

    sends = []
    for dx, source, target in ((-1, first, bottom), (1, last, top)):
        for ref in (vp, vq):
            sends.append((dx, 0, ref.at[:, :, source], ref.at[:, :, target]))
        for ref in (vm, vc):
            sends.append((dx, 0, ref.at[:, source], ref.at[:, target]))
        begins = pl.ds(0 if dx < 0 else length - HALO, HALO)
        sends.append((dx, -1, own_l.at[begins], far_r.at[target]))
        sends.append((dx, 1, own_r.at[begins], far_l.at[target]))
    sends.append((0, -1, own_l, far_r.at[inside]))
    sends.append((0, 1, own_r, far_l.at[inside]))
    for dx, source, target in ((-1, first, bottom), (1, last, top)):
        sends.append((dx, 0, near.at[:, source], near.at[:, target]))
    copies = []
    for i, (dx, dy, source, target) in enumerate(sends):
        copy = pltpu.make_async_remote_copy(
            src_ref=source, dst_ref=target, send_sem=send_sem.at[i], recv_sem=recv_sem.at[i],
            device_id=(x + dx, y + dy), device_id_type=MESH)
        copies.append((dx, dy, copy))
    order = sorted(copies[:-2], key=lambda c: 0 if c[0] and c[1] else 2 - c[1] if c[0] == 0 else 4)

    def begin_sends(order):
        for dx, dy, copy in order:
            @pl.when(has[dx, dy])
            def _(copy=copy):
                copy.start()

    begin_sends(order)
    for k in range(scen):
        near[k, inside] = pack([(layer, vp, (k, layer)) for layer in range(layers)])
        near[scen + 1 + k, inside] = pack([(2 * t, vq, (k, t)) for t in range(tiers)])
    near[scen, inside] = pack([(layer, vc if layer % 2 else vm, (layer // 2,)) for layer in range(layers)])
    begin_sends(copies[-2:])

    def prepare(at, to):
        count = at.size
        for layer in range(layers):
            if layer % 2 == 0:
                s = lookup(vm[layer // 2, at], TIER_ROOT)
                total = jnp.full((count, width), TIER_HEAT, jnp.float32)
            else:
                codes = vc[layer // 2, at]
                s = lookup(codes, CHANNEL_ROOT)
                total = CHANNEL_HEAT + lookup(codes, CHANNEL_SINK)
            root[layer + 1, to] = s
            capac[layer, at] = total
            for k in range(scen):
                up[k, layer + 1, to] = s * vp[k, layer, at]

    def in_pieces(step):
        def one(i, carry):
            step(pl.multiple_of(i * PIECE, PIECE))
            return carry

        lax.fori_loop(0, length // PIECE, one, 0)

    in_pieces(lambda start: prepare(pl.ds(HALO + start, PIECE), pl.ds(2 * HALO + start, PIECE)))

    def shifted(value, matrix):
        high = value.astype(jnp.bfloat16)
        low = (value - high.astype(jnp.float32)).astype(jnp.bfloat16)
        return jnp.dot(jnp.concatenate([high, low], axis=1), matrix[...],
                       preferred_element_type=jnp.float32)

    def spans(start, count):
        pieces = []
        while count > 0:
            piece = min(count, SPAN)
            pieces.append((start, piece))
            start, count = start + piece, count - piece
        return pieces

    def columns(refs, places):
        centres = []
        for ref, at in refs:
            for layer in range(layers):
                for start, count in places:
                    centres.append(ref[at + (layer + 1, pl.ds(HALO + start, count))])
        lateral = shifted(jnp.concatenate(centres, axis=0), along)
        many, offset = layers * len(places), 0
        for i, centre in enumerate(centres):
            ref, at = refs[i // many]
            layer, (start, count) = i % many // len(places), places[i % len(places)]
            around = lateral[offset:offset + count]
            offset += count
            around = around + ref[at + (layer + 1, pl.ds(HALO + start - 1, count))]
            around = around + ref[at + (layer + 1, pl.ds(HALO + start + 1, count))]
            stacked = []
            if layer > 0:
                stacked.append(centres[i - len(places)])
            if layer < layers - 1:
                stacked.append(centres[i + len(places)])
            if stacked:
                around = around + VERTICAL * sum(stacked[1:], stacked[0])
            yield i // many, layer, start, count, centre, around

    def margins(edge, layer):
        lane = lax.broadcasted_iota(jnp.int32, edge.shape, 1)
        ends = (lane == 0) | (lane == width - 1)
        shift = (width - SLOT * layer - (STRIP - 1)) % width
        return jnp.where(ends, pltpu.roll(edge, shift, 1), 0.0)

    def patched(value, face, layer):
        lane = lax.broadcasted_iota(jnp.int32, face.shape, 1)
        ends = (lane < STRIP) | (lane >= width - STRIP)
        return jnp.where(ends, pltpu.roll(face, width - SLOT * layer - STRIP, 1), value)

    def gather(total, value, start, low, high):
        first, last = max(low - start, 0), min(high - start, value.shape[0])
        if last <= first:
            return total
        return total + jnp.sum(value[first:last].reshape(-1, HALO, width), axis=0)

    none = jnp.zeros((HALO, width), jnp.float32)
    each = 2 * ITERS

    def begin(sums, places, low, high, edged):
        for k, layer, start, count, _, around in columns(
                [(root, ())] + [(up, (k,)) for k in range(scen)], places):
            at = pl.ds(start, count)
            s = root[layer + 1, pl.ds(HALO + start, count)]
            if edged:
                around = around + margins(edges[4 * k - 3 if k else 0, at], layer)
            if k == 0:
                total = capac[layer, at] + s * around
                inverse = 1.0 / total
                weight[layer, at] = s * s * inverse
                slope[layer, at] = total
                recip[layer, at] = inverse
                continue
            k = k - 1
            total = slope[layer, at]
            heat = TIER_HEAT if layer % 2 == 0 else CHANNEL_HEAT
            residual = (heat - total) * vp[k, layer, at] + s * around
            if layer % 2 == 0:
                residual = residual + vq[k, layer // 2, at]
            scaled = residual * recip[layer, at]
            u0[k, layer + 1, pl.ds(HALO + start, count)] = s * scaled
            sums[k][0] = gather(sums[k][0], residual * scaled, start, low, high)

    def advance(sums, source, target, level, places, low, high, edged):
        for k, layer, start, count, centre, around in columns(
                [(source, (k,)) for k in range(scen)], places):
            at = pl.ds(start, count)
            if edged:
                around = around + margins(edges[1 + 4 * k + level, at], layer)
            i = 2 * level - 1
            sums[k][i] = gather(sums[k][i], centre * around, start, low, high)
            if target is not None:
                moved = weight[layer, at] * around
                target[k, layer + 1, pl.ds(HALO + start, count)] = moved
                sums[k][i + 1] = gather(sums[k][i + 1], moved * around, start, low, high)

    core = [[none] * each for _ in range(scen)]
    core_rows = (2 * HALO, length)
    whole = spans(HALO, length)
    for place in whole:
        begin(core, [place], *core_rows, False)
    know()
    for place in whole:
        advance(core, u0, u1, 1, [place], *core_rows, False)
    for place in whole:
        advance(core, u1, u2, 2, [place], *core_rows, False)
    for place in spans(2 * HALO, length - 2 * HALO):
        advance(core, u2, None, 3, [place], *core_rows, False)

    know()
    def arrive(chosen):
        for dx, dy, copy in chosen:
            @pl.when(has[-dx, -dy])
            def _(copy=copy):
                copy.wait_recv()

    arrive(copy for copy in copies if copy[:2] != (0, -1))

    prepare(pl.ds(0, HALO), pl.ds(HALO, HALO))
    prepare(pl.ds(HALO + length, HALO), pl.ds(2 * HALO + length, HALO))

    shape = (ext, width)
    lane = lax.broadcasted_iota(jnp.int32, shape, 1)

    taken = []

    def arounds(values, matrix, first=0, count=ext):
        moved = shifted(jnp.concatenate([value[first:first + count] for value in values], axis=0), matrix)
        results = []
        for i, value in enumerate(values):
            slab = slabs.at[len(taken)]
            taken.append(True)
            slab[pl.ds(HALO, ext)] = value
            result = moved[i * count:(i + 1) * count] + slab[pl.ds(HALO + first - 1, count)]
            results.append(result + slab[pl.ds(HALO + first + 1, count)])
        return results

    q = lane % SLOT
    rims = [[[none] * each for _ in range(scen)] for _ in range(2)]

    def add(side, k, i, value):
        kept = value if value.shape[0] < ext else value[2 * HALO:length]
        kept = kept.reshape(-1, HALO, width)
        rims[side][k][i] = rims[side][k][i] + jnp.sum(kept, axis=0)

    def side_of(side, far, shifts, low, shift, matrix, between):
        theirs = (q >= low) & (q < low + STRIP)
        turned = (lane + shift) % width
        valid = (turned // SLOT < layers) & (turned % SLOT < 3 * STRIP)
        tier = turned // SLOT % 2 == 0
        message = far[...]
        parts = []
        for i, turn in enumerate(shifts):
            other = pltpu.roll(message, turn, 1) if turn else message
            parts.append(jnp.where(theirs, other, near[i]))
        codes = jnp.where(valid, parts[scen], -1.0)
        heat = jnp.where(tier, TIER_HEAT, CHANNEL_HEAT)
        s, total = jnp.zeros(shape, jnp.float32), heat
        for code, values in enumerate(zip(TIER_ROOT, CHANNEL_ROOT, CHANNEL_SINK)):
            found = codes == code
            s = jnp.where(found, jnp.where(tier, values[0], values[1]), s)
            if values[2]:
                total = jnp.where(found, heat + jnp.where(tier, 0.0, values[2]), total)
        currents = [s] + [s * parts[k] for k in range(scen)]
        between(0, currents, False)
        spread = arounds(currents, matrix)
        between(0, currents, True)
        total = total + s * spread[0]
        inverse = 1.0 / total
        w = s * s * inverse
        currents = []
        for k in range(scen):
            power = jnp.where(tier & valid, parts[scen + 1 + k], 0.0)
            residual = (heat - total) * parts[k] + power + s * spread[1 + k]
            scaled = residual * inverse
            add(side, k, 0, residual * scaled)
            currents.append(s * scaled)
        for level in range(1, ITERS + 1):
            between(level, currents, False)
            kept = (0, ext) if level < ITERS else (2 * HALO, length - 2 * HALO)
            spread = arounds(currents, matrix, *kept)
            between(level, currents, True)
            for k in range(scen):
                add(side, k, 2 * level - 1, currents[k][kept[0]:kept[0] + kept[1]] * spread[k])
                if level < ITERS:
                    moved = w * spread[k]
                    add(side, k, 2 * level, moved * spread[k])
                    currents[k] = moved

    ends = [(0, 2 * HALO), (ext - 2 * HALO, 2 * HALO)]
    full = [[none] * each for _ in range(scen)]
    full_rows = (HALO, HALO + length)

    def border(i, left, right, faced):
        for start, count in ends:
            east = pltpu.roll(right[start:start + count], width - 2, 1)
            here = slabs[left, pl.ds(HALO + start, count)]
            edges[i, pl.ds(start, count)] = jnp.where(q[:count] == STRIP - 1, here, east)
        if faced:
            faces[i] = jnp.where(q < STRIP, right, slabs[left, pl.ds(HALO, ext)])

    def mend(ref, level):
        for start in (2 * HALO, length - HALO):
            at, to = pl.ds(start, HALO), pl.ds(HALO + start, HALO)
            for k in range(scen):
                for layer in range(layers):
                    face = faces[1 + 4 * k + level, at]
                    ref[k, layer + 1, to] = patched(ref[k, layer + 1, to], face, layer)

    iterates = (u0, u1, u2, None)

    def alone(level, currents, after):
        pass

    def beside_rows(level, currents, after):
        if after and level:
            advance(full, iterates[level - 1], iterates[level], level, ends, *full_rows, True)
        elif after:
            begin(full, ends, *full_rows, True)
        elif level:
            for k in range(scen):
                border(1 + 4 * k + level, scen * level + 1 + k, currents[k], True)
            mend(iterates[level - 1], level)
        else:
            border(0, 0, currents[0], False)
            for k in range(scen):
                border(1 + 4 * k, 1 + k, currents[1 + k], False)

    turns = (STRIP, 0, width - STRIP, width - 2 * STRIP, width - 6 * STRIP)
    side_of(0, far_l, turns, 0, 0, on_left, alone)
    arrive(copy for copy in copies if copy[:2] == (0, -1))
    side_of(1, far_r, turns, STRIP, STRIP, on_right, beside_rows)
    line = lax.broadcasted_iota(jnp.int32, (HALO, width), 1)
    middle = (line >= STRIP) & (line < width - STRIP)
    moments = []
    for k in range(scen):
        for i in range(each):
            value = full[k][i] + jnp.where(middle, core[k][i], 0.0)
            used = (line < SLOT * layers) & (line % SLOT >= STRIP) & (line % SLOT < 2 * STRIP)
            value = value + jnp.where(used, rims[0][k][i], 0.0)
            used = (line < SLOT * layers) & (line % SLOT < STRIP)
            moments.append(value + jnp.where(used, rims[1][k][i], 0.0))
    flat = jnp.zeros((1, width), jnp.float32)
    line = lax.broadcasted_iota(jnp.int32, (1, width), 1)
    for i, value in enumerate(moments):
        total = jnp.sum(jnp.sum(value, axis=0, keepdims=True), axis=1, keepdims=True)
        flat = jnp.where(line == i, total, flat)
    row[...] = flat
    rows[n - 1] = flat
    while len(heard) < len(reaches):
        know()

    def spread(i, carry):
        k = jnp.where(i < me, i, i + 1)
        slot = jnp.where(i < me, i - me + n - 1, i - me)
        pltpu.make_async_remote_copy(
            src_ref=row, dst_ref=rows.at[slot], send_sem=row_send, recv_sem=row_recv,
            device_id=k, device_id_type=pl.DeviceIdType.LOGICAL).start()
        return carry

    lax.fori_loop(0, n - 1, spread, 0)
    for dx, dy, copy in copies:
        @pl.when(has[dx, dy])
        def _(copy=copy):
            copy.wait_send()
    def unscale(start):
        at = pl.ds(HALO + start, PIECE)
        for layer in range(layers):
            if layer % 2 == 0:
                back = lookup(vm[layer // 2, at], TIER_INV)
            else:
                back = lookup(vc[layer // 2, at], CHANNEL_INV)
            for k in range(scen):
                for level, (ref, scaled) in enumerate(((u0, f0), (u1, f1), (u2, f2))):
                    value = ref[k, layer + 1, pl.ds(2 * HALO + start, PIECE)]
                    value = patched(value, faces[2 + 4 * k + level, at], layer)
                    scaled[k, layer, pl.ds(start, PIECE)] = back * value

    in_pieces(unscale)
    arrived = rows.at[pl.ds(0, n - 1)]
    pltpu.make_async_copy(arrived, arrived, row_recv).wait()
    sums[...] = jnp.sum(rows[...], axis=0)
    pltpu.make_async_copy(arrived, arrived, row_send).wait()


def combine(sums, vp, f0, f1, f2, out, result, sem):
    scen, layers, length, width = result.shape
    line = lax.broadcasted_iota(jnp.int32, (1, width), 1)
    each = 2 * ITERS
    total = [jnp.sum(jnp.where(line == i, sums[...], 0.0), axis=1, keepdims=True)
             for i in range(scen * each)]
    for k in range(scen):
        c0, c1, c2 = coefficients(total[k * each:(k + 1) * each])
        for layer in range(layers):
            for offset in range(0, length, PIECE):
                at = pl.ds(offset, min(PIECE, length - offset))
                change = c0 * f0[k, layer, at] + c1 * f1[k, layer, at] + c2 * f2[k, layer, at]
                before = vp[k, layer, pl.ds(HALO + offset, min(PIECE, length - offset))]
                result[k, layer, at] = before + change
            pltpu.make_async_copy(result.at[k, layer], out.at[k, layer], sem).start()
    pltpu.make_async_copy(result, out, sem).wait()


def per_device(nx, ny, previous, dissipated, material, coolant):
    scen, layers, length, width = previous.shape
    tiers = material.shape[0]
    ext = length + 2 * HALO
    f32 = jnp.float32
    field = pltpu.VMEM((scen, layers + 2, ext + 3 * HALO, width), f32)
    strip = pltpu.VMEM((ext, width), f32)
    letter = pltpu.VMEM((length, width), f32)
    own = pltpu.VMEM(previous.shape, f32)
    matrix = pltpu.VMEM((2 * width, width), jnp.bfloat16)
    shared = pl.pallas_call(
        functools.partial(kernel, nx, ny),
        out_shape=(pltpu.VMEM((1, width), f32), pltpu.VMEM((scen, layers, ext, width), f32), own, own, own),
        in_specs=[pl.BlockSpec(memory_space=pl.ANY)] * 4,
        out_specs=[pl.BlockSpec(memory_space=pltpu.VMEM)] * 5,
        scratch_shapes=[
            pltpu.VMEM((scen, tiers, ext, width), f32),
            pltpu.VMEM((tiers, ext, width), jnp.int32),
            pltpu.VMEM((layers - tiers, ext, width), jnp.int32),
            pltpu.VMEM((2 * scen + 1, ext, width), f32),
            letter, letter, strip, strip,
            pltpu.VMEM((4 * scen + 1, ext, width), f32),
            pltpu.VMEM((4 * scen + 1, ext, width), f32),
            pltpu.VMEM((8 * scen + 2, ext + 2 * HALO, width), f32),
            pltpu.VMEM((layers + 2, ext + 3 * HALO, width), f32),
            pltpu.VMEM((layers, ext, width), f32),
            pltpu.VMEM((layers, ext, width), f32),
            pltpu.VMEM((layers, ext, width), f32),
            pltpu.VMEM((layers, ext, width), f32),
            field, field, field, field,
            pltpu.VMEM((1, width), f32),
            pltpu.VMEM((nx * ny, 1, width), f32),
            matrix, matrix, matrix,
            pltpu.SemaphoreType.REGULAR((max(nx, ny).bit_length(),)),
            pltpu.SemaphoreType.DMA((5,)),
            pltpu.SemaphoreType.DMA((16,)),
            pltpu.SemaphoreType.DMA((16,)),
            pltpu.SemaphoreType.DMA,
            pltpu.SemaphoreType.DMA,
        ],
        compiler_params=pltpu.CompilerParams(
            collective_id=0, has_side_effects=True, vmem_limit_bytes=48 * 1024 * 1024),
    )(*(pltpu.with_memory_space_constraint(part, pltpu.HBM)
        for part in (previous, dissipated, material, coolant)))
    shared = [pltpu.with_memory_space_constraint(part, pltpu.VMEM) for part in shared]
    return pl.pallas_call(
        combine,
        out_shape=jax.ShapeDtypeStruct(previous.shape, f32),
        in_specs=[pl.BlockSpec(memory_space=pltpu.VMEM)] * 5,
        out_specs=pl.BlockSpec(memory_space=pl.ANY),
        scratch_shapes=[own, pltpu.SemaphoreType.DMA],
        compiler_params=pltpu.CompilerParams(vmem_limit_bytes=16 * 1024 * 1024),
    )(*shared)


def solution(mesh):
    return jax.shard_map(
        functools.partial(per_device, mesh.shape["gx"], mesh.shape["gy"]),
        mesh=mesh,
        in_specs=(
            P(None, None, "gx", "gy"),
            P(None, None, "gx", "gy"),
            P(None, "gx", "gy"),
            P(None, "gx", "gy"),
        ),
        out_specs=P(None, None, "gx", "gy"),
        check_vma=False,
    )
```
